32 devices in a mesh: dp: 8 (over y, x, core), tensor: 4 (over z).
Axes of the slice: x: 2, y: 2, z: 4, core: 2. Of those that a mesh axis runs over, the one named last changes fastest.
Arguments:
- hidden_in: bfloat16 [4096, 2048], P('dp', 'tensor'), may hold values from -6 to 6
- cotangent: bfloat16 [4096, 2048], P('dp', 'tensor'), may hold values from -6 to 6
- segment_ids: int32 [4096], P('dp'), may hold values from -1 to 4095, as said below
- positions: int32 [4096], P('dp'), may hold values from 0 to 1023, as said below
- norm_gain: float32 [2048], replicated, may hold values from 0.25 to 1.75
- norm_shift: float32 [2048], replicated, may hold values from -1.5 to 1.5
- qkv_weight: bfloat16 [2048, 3, 2048], P(None, None, 'tensor'), may hold values from -0.53033009 to 0.53033009
- qv_bias: float32 [2, 2048], P(None, 'tensor'), may hold values from -3 to 3
- key_bias: float32 [32, 32], P('tensor'), may hold values from -3 to 3
- dense_weight: bfloat16 [2048, 2048], P('tensor'), may hold values from -1.5 to 1.5
- fc1_weight: bfloat16 [2048, 8192], P(None, 'tensor'), may hold values from -0.125 to 0.125
- fc1_bias: float32 [8192], P('tensor'), may hold values from -3 to 3
- fc2_weight: bfloat16 [8192, 2048], P('tensor'), may hold values from -0.0625 to 0.0625
- out_bias: float32 [2, 2048], replicated, may hold values from -1.5 to 1.5
Outputs:
- block_out: bfloat16 [4096, 2048], P('dp', 'tensor')
- input_grad: float32 [4096, 2048], P('dp', 'tensor')
- norm_grad: float32 [2, 2048], P(None, ('tensor', 'dp'))
- qkv_grad: float32 [2048, 3, 2048], P('dp', None, 'tensor')
- qvbias_grad: float32 [2, 2048], P(None, ('tensor', 'dp'))
- keybias_grad: float32 [32, 32], P('tensor', 'dp')
- dense_grad: float32 [2048, 2048], P(('tensor', 'dp'))
- fc1_grad: float32 [2048, 8192], P('dp', 'tensor')
- fc1bias_grad: float32 [8192], P(('tensor', 'dp'))
- fc2_grad: float32 [8192, 2048], P(('tensor', 'dp'))
- outbias_grad: float32 [2, 2048], P(None, ('tensor', 'dp'))
The draws below stay inside these ranges and needn't reach their ends.
Inputs may be any that keep to these rules, and one draw needn't show every extreme that they name: `segment_ids`: the tokens of one segment id stand in a row inside one block of 512 slots, and different segments have different ids; -1 marks unused slots, which end a block; every block has 256 or more used slots, and some block is a single segment of 512 tokens. Within a segment the positions rise by one from token to token; unused slots have position 0.
All inputs are finite; a program needn't handle non-finite values.
Results may differ from the reference program's by a relative error of at most 0.028.
The reference program's roundings to bfloat16 on the way count: a program that leaves them out, or rounds other values in their place, can miss the bound.
Values may be sent and summed in bfloat16 or wider, within the bound.
A program may use at most 256 MiB of HBM per device.

```python
import math
import jax
import jax.numpy as jnp
from jax import lax

D = 2048
H = 32
HD = 64
ROT = 32
FF = 8192
TOK_DEV = 512
TOKENS = 4096


def packing_layout(key):
    base = jax.random.fold_in(key, 11)
    key_live, key_full, key_begin, key_offset = jax.random.split(base, 4)
    num_devs = TOKENS // TOK_DEV
    dev_ids = jnp.arange(num_devs, dtype=jnp.int32)
    slot_ids = jnp.arange(TOK_DEV, dtype=jnp.int32)
    live_count = jax.random.randint(key_live, (num_devs,), TOK_DEV // 2, TOK_DEV)
    full_dev = jax.random.randint(key_full, (), 0, num_devs)
    is_full = dev_ids == full_dev
    live_count = jnp.where(is_full, TOK_DEV, live_count)
    begins = jax.random.randint(key_begin, (num_devs, TOK_DEV), 0, max(TOK_DEV // 2, 2)) == 0
    begins = begins | (slot_ids[None, :] == 0)
    begins = jnp.where(is_full[:, None], slot_ids[None, :] == 0, begins)
    local_ids = jnp.cumsum(begins.astype(jnp.int32), axis=1) - 1
    seg_ids = dev_ids[:, None] * TOK_DEV + (TOK_DEV - 1) - local_ids
    padded = slot_ids[None, :] >= live_count[:, None]
    seg_ids = jnp.where(padded, -1, seg_ids)
    start_slot = lax.cummax(jnp.where(begins, slot_ids[None, :], 0), axis=1)
    rank_in = slot_ids[None, :] - start_slot
    offsets = jax.random.randint(key_offset, (num_devs, TOK_DEV), 0, TOK_DEV + 1)
    offset_here = jnp.take_along_axis(offsets, start_slot, axis=1)
    offset_here = jnp.where(is_full[:, None], TOK_DEV, offset_here)
    pos_ids = jnp.where(padded, 0, rank_in + offset_here)
    return (seg_ids.reshape(-1).astype(jnp.int32), pos_ids.reshape(-1).astype(jnp.int32))


def draw_segment_ids(key, part):
    return packing_layout(key)[0]


def draw_positions(key, part):
    return packing_layout(key)[1]


def draw_qkv_weight(key, part):
    noise = jax.random.normal(jax.random.fold_in(key, 5), (D, 3, D), jnp.float32)
    noise = jnp.clip(noise, -4.0, 4.0)
    return (noise * (1.0 / math.sqrt(D))).astype(jnp.bfloat16)


def steps_of(rng, dims, cuts, low, top_value):
    def one(position, parts):
        draws = jax.random.uniform(jax.random.fold_in(jax.random.fold_in(rng, 6), position), (parts,), jnp.float32, low / len(cuts), top_value / len(cuts))
        return jnp.repeat(jnp.exp(draws), dims[position] // parts).reshape((-1,) + (1,) * (len(dims) - position - 1))

    gain = one(*cuts[0])
    for cut in cuts[1:]:
        gain = gain * one(*cut)
    return gain


def gaussian(rng, extent, scale, limit, shards=(), kind=jnp.bfloat16):
    entries = jax.random.normal(rng, extent, jnp.float32) * scale
    if len(shards) > 0:
        entries = steps_of(rng, extent, shards, -0.22, 0.18) * entries
    return jnp.clip(entries, min=-limit, max=limit).astype(kind)


def setup_inputs(seed: int = 0) -> dict:
    key_of = jax.random.split(jax.random.key(seed), 15)
    hidden_in = gaussian(key_of[0], (TOKENS, D), 1.0, 6.0, ((0, 8), (1, 4)))
    cotangent = gaussian(key_of[1], (TOKENS, D), 1.0, 6.0, ((0, 8), (1, 4)))
    segment_ids = draw_segment_ids(jax.random.fold_in(key_of[14], 71), 0)
    positions = draw_positions(jax.random.fold_in(key_of[14], 71), 0)
    norm_gain = jnp.clip(1.0 + 0.15 * jax.random.normal(key_of[4], (D,), jnp.float32), 0.25, 1.75)
    norm_shift = gaussian(key_of[5], (D,), 0.3, 1.5, (), jnp.float32)
    qkv_weight = draw_qkv_weight(jax.random.fold_in(key_of[14], 71), 0)
    qv_bias = gaussian(key_of[7], (2, D), 0.5, 3.0, ((1, 4),), jnp.float32)
    key_bias = gaussian(key_of[8], (H, ROT), 0.5, 3.0, ((0, 4),), jnp.float32)
    dense_weight = gaussian(key_of[9], (D, D), (D * 4 // TOK_DEV) ** -0.5, 1.5, ((0, 4),))
    fc1_weight = gaussian(key_of[10], (D, FF), D ** -0.5, 0.125, ((1, 4),))
    fc1_bias = gaussian(key_of[11], (FF,), 0.5, 3.0, ((0, 4),), jnp.float32)
    fc2_weight = gaussian(key_of[12], (FF, D), FF ** -0.5, 0.0625, ((0, 4),))
    out_bias = gaussian(key_of[13], (2, D), 0.3, 1.5, (), jnp.float32)
    return dict(hidden_in=hidden_in, cotangent=cotangent, segment_ids=segment_ids, positions=positions, norm_gain=norm_gain, norm_shift=norm_shift, qkv_weight=qkv_weight, qv_bias=qv_bias, key_bias=key_bias, dense_weight=dense_weight, fc1_weight=fc1_weight, fc1_bias=fc1_bias, fc2_weight=fc2_weight, out_bias=out_bias)


norm_epsilon = 1e-05
gelu_scale = 0.7978845608028654
gelu_cubic = 0.044715
masked_score = -1e+30

def gelu_pair(pre_act):
    tanh_val = jnp.tanh(gelu_scale * (pre_act + gelu_cubic * pre_act * pre_act * pre_act))
    gelu_val = 0.5 * pre_act * (1.0 + tanh_val)
    gelu_slope = 0.5 * (1.0 + tanh_val) + 0.5 * pre_act * (1.0 - tanh_val * tanh_val) * gelu_scale * (1.0 + 3.0 * gelu_cubic * pre_act * pre_act)
    return (gelu_val, gelu_slope)

def rotary_tables(positions, rot_dims):
    half_rot = rot_dims // 2
    exponent = jnp.arange(half_rot, dtype=jnp.float32) * (2.0 / rot_dims)
    inverse = jnp.power(jnp.float32(10000.0), -exponent)
    angles = positions.astype(jnp.float32)[:, None] * inverse[None, :]
    return (jnp.cos(angles)[:, None, :], jnp.sin(angles)[:, None, :])

def rotate_fwd(operand, cosine, sine, rot_dims):
    half_rot = rot_dims // 2
    lower = operand[..., :half_rot]
    upper = operand[..., half_rot:rot_dims]
    return jnp.concatenate([lower * cosine - upper * sine, upper * cosine + lower * sine, operand[..., rot_dims:]], axis=-1)

def rotate_back(operand, cosine, sine, rot_dims):
    half_rot = rot_dims // 2
    lower = operand[..., :half_rot]
    upper = operand[..., half_rot:rot_dims]
    return jnp.concatenate([lower * cosine + upper * sine, upper * cosine - lower * sine, operand[..., rot_dims:]], axis=-1)

def reference(hidden_in, cotangent, segment_ids, positions, norm_gain, norm_shift, qkv_weight, qv_bias, key_bias, dense_weight, fc1_weight, fc1_bias, fc2_weight, out_bias):
    num_blocks = TOKENS // TOK_DEV
    score_scale = HD ** (-0.5)
    qkv_full = qkv_weight.astype(jnp.float32)
    key_pad = jnp.concatenate([key_bias, jnp.zeros((H, HD - ROT), jnp.float32)], axis=1)
    slot_ids = jnp.arange(TOK_DEV, dtype=jnp.int32)
    causal = slot_ids[None, :] <= slot_ids[:, None]
    bias_total = out_bias[0] + out_bias[1]

    def one_block(totals, pieces):
        block_in, block_cot, block_seg, block_pos = pieces
        in_f = block_in.astype(jnp.float32)
        row_mean = lax.optimization_barrier(jnp.mean(in_f, axis=1, keepdims=True))
        centred = in_f - row_mean
        inv_std = lax.rsqrt(lax.optimization_barrier(jnp.mean(centred * centred, axis=1, keepdims=True)) + norm_epsilon)
        normed = centred * inv_std
        hidden = (normed * norm_gain + norm_shift).astype(jnp.bfloat16)
        hidden_f = hidden.astype(jnp.float32)
        projected = jnp.einsum('td,dcn->tcn', hidden_f, qkv_full)
        cosine, sine = rotary_tables(block_pos, ROT)
        queries = rotate_fwd((projected[:, 0] + qv_bias[0]).reshape(TOK_DEV, H, HD), cosine, sine, ROT).astype(jnp.bfloat16)
        keys_rot = rotate_fwd(projected[:, 1].reshape(TOK_DEV, H, HD) + key_pad[None], cosine, sine, ROT).astype(jnp.bfloat16)
        values_b = (projected[:, 2] + qv_bias[1]).reshape(TOK_DEV, H, HD).astype(jnp.bfloat16)
        allowed = (block_seg[:, None] == block_seg[None, :]) & causal
        scores = jnp.einsum('qhd,khd->hqk', queries.astype(jnp.float32), keys_rot.astype(jnp.float32)) * score_scale
        scores = jnp.where(allowed[None], scores, masked_score)
        row_top = lax.optimization_barrier(jnp.max(scores, axis=2, keepdims=True))
        log_total = row_top + jnp.log(lax.optimization_barrier(jnp.sum(jnp.exp(scores - row_top), axis=2, keepdims=True)))
        prob_f = jnp.exp(scores - log_total)
        prob_b = prob_f.astype(jnp.bfloat16)
        attn_mix = jnp.einsum('hqk,khd->qhd', prob_b.astype(jnp.float32), values_b.astype(jnp.float32)).astype(jnp.bfloat16)
        attn_flat = attn_mix.reshape(TOK_DEV, D)
        pre_act = jnp.dot(hidden, fc1_weight, preferred_element_type=jnp.float32) + fc1_bias
        gelu_val, gelu_slope = gelu_pair(pre_act)
        act_b = gelu_val.astype(jnp.bfloat16)
        branches = jnp.dot(attn_flat, dense_weight, preferred_element_type=jnp.float32) + jnp.dot(act_b, fc2_weight, preferred_element_type=jnp.float32)
        block_out = (in_f + branches + bias_total).astype(jnp.bfloat16)
        live_rows = block_seg >= 0
        grad_b = jnp.where(live_rows[:, None], block_cot, jnp.zeros_like(block_cot))
        grad_f = grad_b.astype(jnp.float32)
        fc2_g = jnp.dot(act_b.T, grad_b, preferred_element_type=jnp.float32)
        dense_g = jnp.dot(attn_flat.T, grad_b, preferred_element_type=jnp.float32)
        outb_g = lax.optimization_barrier(jnp.sum(grad_f, axis=0))
        d_pre = jnp.dot(grad_b, fc2_weight.T, preferred_element_type=jnp.float32) * gelu_slope
        d_pre_b = d_pre.astype(jnp.bfloat16)
        fc1_g = jnp.dot(hidden.T, d_pre_b, preferred_element_type=jnp.float32)
        fc1b_g = lax.optimization_barrier(jnp.sum(d_pre, axis=0))
        d_attn = jnp.dot(grad_b, dense_weight.T, preferred_element_type=jnp.float32).astype(jnp.bfloat16).reshape(TOK_DEV, H, HD)
        d_attn_f = d_attn.astype(jnp.float32)
        delta = lax.optimization_barrier(jnp.sum(d_attn_f * attn_mix.astype(jnp.float32), axis=2))
        d_prob = jnp.einsum('qhd,khd->hqk', d_attn_f, values_b.astype(jnp.float32))
        d_score = (prob_f * (d_prob - delta.T[:, :, None]) * score_scale).astype(jnp.bfloat16)
        d_score_f = d_score.astype(jnp.float32)
        d_query = jnp.einsum('hqk,khd->qhd', d_score_f, keys_rot.astype(jnp.float32))
        d_key = jnp.einsum('hqk,qhd->khd', d_score_f, queries.astype(jnp.float32))
        d_value = jnp.einsum('hqk,qhd->khd', prob_b.astype(jnp.float32), d_attn_f)
        d_query = rotate_back(d_query, cosine, sine, ROT).reshape(TOK_DEV, D)
        d_key = rotate_back(d_key, cosine, sine, ROT)
        keyb_g = lax.optimization_barrier(jnp.sum(d_key[:, :, :ROT], axis=0))
        d_key = d_key.reshape(TOK_DEV, D)
        d_value = d_value.reshape(TOK_DEV, D)
        qvb_g = jnp.stack([lax.optimization_barrier(jnp.sum(d_query, axis=0)), lax.optimization_barrier(jnp.sum(d_value, axis=0))])
        d_proj = jnp.stack([d_query, d_key, d_value], axis=1).astype(jnp.bfloat16)
        d_proj_f = d_proj.astype(jnp.float32)
        qkv_g = jnp.einsum('td,tcn->dcn', hidden_f, d_proj_f)
        d_hidden = jnp.einsum('tcn,dcn->td', d_proj_f, qkv_full) + jnp.dot(d_pre_b, fc1_weight.T, preferred_element_type=jnp.float32)
        norm_g = jnp.stack([lax.optimization_barrier(jnp.sum(d_hidden * normed, axis=0)), lax.optimization_barrier(jnp.sum(d_hidden, axis=0))])
        scaled = d_hidden * norm_gain
        block_dx = inv_std * (scaled - lax.optimization_barrier(jnp.mean(scaled, axis=1, keepdims=True)) - normed * lax.optimization_barrier(jnp.mean(scaled * normed, axis=1, keepdims=True))) + grad_f
        updates = (norm_g, qkv_g, qvb_g, keyb_g, dense_g, fc1_g, fc1b_g, fc2_g, outb_g)
        new_totals = tuple((total + update for total, update in zip(totals, updates)))
        return (new_totals, (block_out, block_dx))
    zeros_all = (jnp.zeros((2, D), jnp.float32), jnp.zeros((D, 3, D), jnp.float32), jnp.zeros((2, D), jnp.float32), jnp.zeros((H, ROT), jnp.float32), jnp.zeros((D, D), jnp.float32), jnp.zeros((D, FF), jnp.float32), jnp.zeros((FF,), jnp.float32), jnp.zeros((FF, D), jnp.float32), jnp.zeros((D,), jnp.float32))
    pieces = (hidden_in.reshape(num_blocks, TOK_DEV, D), cotangent.reshape(num_blocks, TOK_DEV, D), segment_ids.reshape(num_blocks, TOK_DEV), positions.reshape(num_blocks, TOK_DEV))
    totals, (outs_all, dx_all) = lax.scan(one_block, zeros_all, pieces)
    norm_g, qkv_g, qvb_g, keyb_g, dense_g, fc1_g, fc1b_g, fc2_g, outb_g = totals
    return (outs_all.reshape(TOKENS, D), dx_all.reshape(TOKENS, D), norm_g, qkv_g, qvb_g, keyb_g, dense_g, fc1_g, fc1b_g, fc2_g, jnp.stack([outb_g, outb_g]))
```

```python
import functools

import jax
import jax.numpy as jnp
from jax import lax
from jax.experimental import pallas as pl
from jax.experimental.pallas import tpu as pltpu
from jax.sharding import PartitionSpec as P

HD = 64
ROT = 32
LANES = 128

norm_epsilon = 1e-05
gelu_scale = 0.7978845608028654
gelu_cubic = 0.044715
masked_score = -1e30

MESH = pl.DeviceIdType.MESH
F32 = jnp.float32
BF16 = jnp.bfloat16
VMEM_BYTES = 67043328


def gelu_pair(pre_act):
    tanh_val = jnp.tanh(gelu_scale * (pre_act + gelu_cubic * pre_act * pre_act * pre_act))
    gelu_val = 0.5 * pre_act * (1.0 + tanh_val)
    gelu_slope = 0.5 * (1.0 + tanh_val) + 0.5 * pre_act * (
        1.0 - tanh_val * tanh_val
    ) * gelu_scale * (1.0 + 3.0 * gelu_cubic * pre_act * pre_act)
    return (gelu_val, gelu_slope)


def rotary_tables(positions, rot_dims):
    half_rot = rot_dims // 2
    exponent = jnp.arange(half_rot, dtype=jnp.float32) * (2.0 / rot_dims)
    inverse = jnp.power(jnp.float32(10000.0), -exponent)
    angles = positions.astype(jnp.float32)[:, None] * inverse[None, :]
    return (jnp.cos(angles)[:, None, :], jnp.sin(angles)[:, None, :])


def rotate_fwd(operand, cosine, sine, rot_dims):
    half_rot = rot_dims // 2
    lower = operand[..., :half_rot]
    upper = operand[..., half_rot:rot_dims]
    return jnp.concatenate(
        [lower * cosine - upper * sine, upper * cosine + lower * sine, operand[..., rot_dims:]],
        axis=-1,
    )


def rotate_back(operand, cosine, sine, rot_dims):
    half_rot = rot_dims // 2
    lower = operand[..., :half_rot]
    upper = operand[..., half_rot:rot_dims]
    return jnp.concatenate(
        [lower * cosine + upper * sine, upper * cosine - lower * sine, operand[..., rot_dims:]],
        axis=-1,
    )


class Place:
    def __init__(self, nd, nt):
        self.nd, self.nt = nd, nt
        self.nch = nd // 2
        self.bits = self.nch.bit_length() - 1
        self.d = lax.axis_index("dp")
        self.t = lax.axis_index("tensor")
        self.c = lax.rem(self.d, 2)
        self.j = self.d // 2

    def pair(self):
        return (self.d + 1 - 2 * self.c, self.t)

    def chip_bit(self, b):
        return lax.rem(self.j // (1 << b), 2)

    def over(self, b):
        step = 2 << b
        return (self.d + step - 2 * step * self.chip_bit(b), self.t)

    def right(self):
        return (self.d, jnp.minimum(self.t + 1, self.nt - 1))

    def left(self):
        return (self.d, jnp.maximum(self.t - 1, 0))


def remote(src, dst, send, recv, device):
    return pltpu.make_async_remote_copy(
        src_ref=src, dst_ref=dst, send_sem=send, recv_sem=recv, device_id=device, device_id_type=MESH
    )


def greet(place, dp_peers):
    barrier = pltpu.get_barrier_semaphore()
    count = 0
    for k in range(1, place.nd if dp_peers == "all" else 1):
        pl.semaphore_signal(
            barrier, inc=1, device_id=(lax.rem(place.d + k, place.nd), place.t), device_id_type=MESH
        )
        count += 1
    if dp_peers == "pair":
        pl.semaphore_signal(barrier, inc=1, device_id=place.pair(), device_id_type=MESH)
        count += 1
    for k in range(1, place.nt):
        pl.semaphore_signal(
            barrier, inc=1, device_id=(place.d, lax.rem(place.t + k, place.nt)), device_id_type=MESH
        )
        count += 1
    pl.semaphore_wait(barrier, count)


def gather_kernel(nd, nt, xc, aux, full, aux_p, send_z, recv_z, send_c, recv_c, aux_sem, own_sem):
    place = Place(nd, nt)
    t = place.t
    wl = xc.shape[2]
    greet(place, "pair")

    def part(a, slot, k):
        return full.at[a, slot, :, pl.ds(pl.multiple_of(k * wl, wl), wl)]

    def own_copy(a):
        return pltpu.make_async_copy(xc.at[a], part(a, 0, t), own_sem.at[a])

    def aux_copy():
        return remote(aux, aux_p, aux_sem.at[0], aux_sem.at[1], place.pair())

    def z_copy(a, k, side):
        return remote(
            part(a, 0, k), part(a, 0, k), send_z.at[side, a, k], recv_z.at[a, k],
            place.right() if side == 0 else place.left(),
        )

    def c_copy(a, k):
        return remote(part(a, 0, k), part(a, 1, k), send_c.at[a, k], recv_c.at[a, k], place.pair())

    own_copy(0).start()
    own_copy(1).start()
    aux_copy().start()
    own_copy(0).wait()
    own_copy(1).wait()

    def item(side, who, i):
        if side == 0:
            first = i <= who
            return jnp.where(first, 0, 1), jnp.where(first, who - i, 2 * who + 1 - i)
        n = nt - who
        first = i < n
        return jnp.where(first, 0, 1), jnp.where(first, who + i, who + i - n)

    for step in range(2 * nt):
        if step == 0:
            c_copy(0, t).start()
            c_copy(1, t).start()
        if step >= 1:
            @pl.when((t > 0) & (step - 1 < 2 * t))
            def _():
                a, k = item(0, t - 1, step - 1)
                z_copy(a, k, 0).wait_recv()
                c_copy(a, k).start()

            @pl.when((t < nt - 1) & (step - 1 < 2 * (nt - 1 - t)))
            def _():
                a, k = item(1, t + 1, step - 1)
                z_copy(a, k, 1).wait_recv()
                c_copy(a, k).start()

        @pl.when((t < nt - 1) & (step < 2 * (t + 1)))
        def _():
            a, k = item(0, t, step)
            z_copy(a, k, 0).start()

        @pl.when((t > 0) & (step < 2 * (nt - t)))
        def _():
            a, k = item(1, t, step)
            z_copy(a, k, 1).start()

    for step in range(2 * nt):
        @pl.when((t < nt - 1) & (step < 2 * (t + 1)))
        def _():
            a, k = item(0, t, step)
            z_copy(a, k, 0).wait_send()

        @pl.when((t > 0) & (step < 2 * (nt - t)))
        def _():
            a, k = item(1, t, step)
            z_copy(a, k, 1).wait_send()

    for a in range(2):
        for k in range(nt):
            c_copy(a, k).wait()
    aux_copy().wait()


def gather(xc, aux, nd, nt):
    _, rows, wl = xc.shape
    return pl.pallas_call(
        functools.partial(gather_kernel, nd, nt),
        out_shape=(
            jax.ShapeDtypeStruct((2, 2, rows, wl * nt), BF16),
            jax.ShapeDtypeStruct(aux.shape, aux.dtype),
        ),
        in_specs=[pl.BlockSpec(memory_space=pltpu.VMEM)] * 2,
        out_specs=[pl.BlockSpec(memory_space=pltpu.VMEM)] * 2,
        scratch_shapes=[
            pltpu.SemaphoreType.DMA((2, 2, nt)),
            pltpu.SemaphoreType.DMA((2, nt)),
            pltpu.SemaphoreType.DMA((2, nt)),
            pltpu.SemaphoreType.DMA((2, nt)),
            pltpu.SemaphoreType.DMA((2,)),
            pltpu.SemaphoreType.DMA((2,)),
        ],
        compiler_params=pltpu.CompilerParams(
            collective_id=0, has_side_effects=True, vmem_limit_bytes=40 << 20
        ),
        name="gather",
    )(xc, aux)


def tiles(rows, size):
    size = min(rows, size)
    assert rows % size == 0
    return size, rows // size


class Halving:
    def __init__(self, place, grad, cols, order, recv, stage, send_sem, recv_sem):
        self.p, self.g, self.cols, self.order = place, grad, cols, order
        self.r, self.s, self.ss, self.rs = recv, stage, send_sem, recv_sem
        self.off = [0]
        for i in range(len(order)):
            self.off.append(self.off[-1] + (place.nch >> (i + 1)))

    def block(self, i, m, mine):
        j = 0
        for b in self.order[:i]:
            j = j + (self.p.chip_bit(b) << b)
        if i < len(self.order):
            b = self.order[i]
            v = self.p.chip_bit(b)
            j = j + ((v if mine else 1 - v) << b)
            for q, b2 in enumerate(self.order[i + 1 :]):
                j = j + (((m >> q) & 1) << b2)
        return j

    def held(self, i, m, mine, before):
        idx = 0
        for r in range(before + 1, min(i, len(self.order))):
            idx = idx + (self.p.chip_bit(self.order[r]) << (r - before - 1))
        if i < len(self.order):
            v = self.p.chip_bit(self.order[i])
            idx = idx + ((v if mine else 1 - v) << (i - before - 1)) + (m << (i - before))
        return self.off[before] + idx

    def copy(self, i, m):
        src = (
            self.g.at[self.block(0, m, False), :, self.cols]
            if i == 0
            else self.s.at[self.off[i] + m - self.off[1]]
        )
        k = self.off[i] + m
        return remote(
            src, self.r.at[k], self.ss.at[k], self.rs.at[k], self.p.over(self.order[i])
        )

    def total(self, i, m, rows):
        blk = self.block(i, m, False)
        acc = self.g[blk, rows, self.cols].astype(F32)
        for before in range(i):
            acc = acc + self.r[self.held(i, m, False, before), rows, :].astype(F32)
        return acc

    def start(self, i):
        for m in range(self.p.nch >> (i + 1)):
            if i > 0:
                size, n = tiles(self.g.shape[1], 64)

                @pl.loop(0, n)
                def _(q):
                    rows = pl.ds(pl.multiple_of(q * size, size), size)
                    self.s[self.off[i] + m - self.off[1], rows, :] = self.total(i, m, rows).astype(BF16)

            self.copy(i, m).start()

    def wait(self, i):
        for m in range(self.p.nch >> (i + 1)):
            self.copy(i, m).wait()


def sum_kernel(nd, nt, names, *refs):
    place = Place(nd, nt)
    n = len(names)
    grads = refs[:n]
    part_o, part_h = refs[n : n + 2]
    outs = refs[n + 2 : 2 * n + 2 + 2]
    sc = list(refs[2 * n + 4 :])
    fin = outs[:n]
    out_o, out_h = outs[n:]
    t = place.t
    greet(place, "all")
    halves = []
    for gi in range(n):
        w = grads[gi].shape[2]
        for h in range(2):
            order = list(range(place.bits))
            if h == 1:
                order = order[::-1]
            recv, stage, ss, rs = sc[:4]
            del sc[:4]
            halves.append(
                (gi, h, Halving(place, grads[gi], pl.ds(h * (w // 2), w // 2), order, recv, stage, ss, rs))
            )
    for _, _, hv in halves:
        hv.start(0)

    lines = []
    for part, out in ((part_o, out_o), (part_h, out_h)):
        pr, rb, sb, sem_c, sem_s, sem_r = sc[:6]
        del sc[:6]
        lines.append((part, out, pr, rb, sb, sem_c, sem_s, sem_r))
    rows_t, wl = lines[0][3].shape[1:]

    def pair_copy(line):
        part, _, pr, _, _, sem_c, _, _ = line
        return remote(part.at[1], pr, sem_c.at[0], sem_c.at[1], place.pair())

    def own(line, k, rows):
        part, _, pr = line[:3]
        cols = pl.ds(pl.multiple_of(k * wl, wl), wl)
        return part[0, rows, cols].astype(F32) + pr[rows, cols].astype(F32)

    def line_copy(line, side, k):
        rb, sb, sem_s, sem_r = line[3], line[4], line[6], line[7]
        if side == 0:
            slot, dev = k, place.right()
        else:
            slot, dev = jnp.where(k == t - 1, nt, k), place.left()
        return remote(sb.at[k], rb.at[slot], sem_s.at[side, k], sem_r.at[slot], dev)

    def line_wait(line, side, k):
        rb, sb, sem_s, sem_r = line[3], line[4], line[6], line[7]
        slot = k if side == 0 else jnp.where(k == t, nt, k)
        remote(sb.at[k], rb.at[slot], sem_s.at[side, k], sem_r.at[slot], place.pair()).wait_recv()

    def line_send(line, side, step):
        me = t if side == 0 else nt - 1 - t

        @pl.when((me <= step) & (me < nt - 1))
        def _():
            k = nt - 1 - step + me
            k = k if side == 0 else nt - 1 - k
            rb, sb = line[3], line[4]

            @pl.when(me > 0)
            def _():
                line_wait(line, side, k)

            size, cnt = tiles(rows_t, 64)

            @pl.loop(0, cnt)
            def _(q):
                rows = pl.ds(pl.multiple_of(q * size, size), size)
                got = rb[k, rows, :].astype(F32)
                sb[k, rows, :] = (own(line, k, rows) + jnp.where(me > 0, got, 0.0)).astype(BF16)

            line_copy(line, side, k).start()

    def line_finish(line):
        @pl.when(t > 0)
        def _():
            line_wait(line, 0, t)

        @pl.when(t < nt - 1)
        def _():
            line_wait(line, 1, t)

        rb, out = line[3], line[1]
        size, cnt = tiles(rows_t, 64)

        @pl.loop(0, cnt)
        def _(q):
            rows = pl.ds(pl.multiple_of(q * size, size), size)
            out[rows, :] = (
                own(line, t, rows)
                + jnp.where(t > 0, rb[t, rows, :].astype(F32), 0.0)
                + jnp.where(t < nt - 1, rb[nt, rows, :].astype(F32), 0.0)
            )

        for side in range(2):
            me = t if side == 0 else nt - 1 - t
            for step in range(nt - 1):
                @pl.when((me <= step) & (me < nt - 1))
                def _():
                    k = nt - 1 - step + me
                    k = k if side == 0 else nt - 1 - k
                    line_copy(line, side, k).wait_send()

    for line in lines:
        pair_copy(line).start()
    for line in lines:
        pair_copy(line).wait()

    def finish_pair(gi):
        send, recv, sem = fin_sc[gi]
        return remote(send, recv, sem.at[0], sem.at[1], place.pair())

    fin_sc = {}
    for gi, name in enumerate(names):
        if name in ("fc1", "qkv"):
            fin_sc[gi] = sc[:3]
            del sc[:3]

    def finish(gi):
        name = names[gi]
        out = fin[gi]
        for gj, h, hv in halves:
            if gj != gi:
                continue
            w2 = grads[gi].shape[2] // 2
            cols = pl.ds(h * w2, w2)
            if gi in fin_sc:
                send = fin_sc[gi][0]
                rn = grads[gi].shape[1] // 2
                size, cnt = tiles(rn, 64)

                @pl.loop(0, cnt)
                def _(q):
                    base = pl.multiple_of(q * size, size)
                    rows = pl.ds(base, size)
                    mine = pl.ds(pl.multiple_of(place.c * rn + base, size), size)
                    other = pl.ds(pl.multiple_of((1 - place.c) * rn + base, size), size)
                    out[0, rows, cols] = hv.total(place.bits, 0, mine)
                    send[rows, cols] = hv.total(place.bits, 0, other).astype(BF16)
            else:
                size, cnt = tiles(grads[gi].shape[1], 64)

                @pl.loop(0, cnt)
                def _(q):
                    rows = pl.ds(pl.multiple_of(q * size, size), size)
                    out[rows, cols] = hv.total(place.bits, 0, rows)
        if gi in fin_sc:
            finish_pair(gi).start()

    for step in range(max(nt - 1, n * place.bits)):
        if step < nt - 1:
            for line in lines:
                line_send(line, 0, step)
                line_send(line, 1, step)
        if step < n * place.bits:
            i = step // n
            gi = step % n
            for gj, h, hv in halves:
                if gj == gi:
                    hv.wait(i)
                    if i + 1 < place.bits:
                        hv.start(i + 1)
            if i + 1 == place.bits:
                finish(gi)
    for line in lines:
        line_finish(line)
    for gi in fin_sc:
        finish_pair(gi).wait()
        recv = fin_sc[gi][1]
        fin[gi][1] = recv[...].astype(F32)


def sum_all(grads, part_o, part_h, nd, nt):
    names = tuple(grads)
    nch = nd // 2
    rows_t, width = part_o.shape[1:]
    wl = width // nt
    out_shape, scratch = [], []
    for name in names:
        _, r, w = grads[name].shape
        shape = (2, r // 2, w) if name in ("fc1", "qkv") else (r, w)
        out_shape.append(jax.ShapeDtypeStruct(shape, F32))
        for h in range(2):
            scratch += [
                pltpu.VMEM((nch - 1, r, w // 2), BF16),
                pltpu.VMEM((max(nch // 2 - 1, 1), r, w // 2), BF16),
                pltpu.SemaphoreType.DMA((nch - 1,)),
                pltpu.SemaphoreType.DMA((nch - 1,)),
            ]
    out_shape += [jax.ShapeDtypeStruct((rows_t, wl), F32)] * 2
    for _ in range(2):
        scratch += [
            pltpu.VMEM((rows_t, width), BF16),
            pltpu.VMEM((nt + 1, rows_t, wl), BF16),
            pltpu.VMEM((nt, rows_t, wl), BF16),
            pltpu.SemaphoreType.DMA((2,)),
            pltpu.SemaphoreType.DMA((2, nt)),
            pltpu.SemaphoreType.DMA((nt + 1,)),
        ]
    for name in names:
        if name in ("fc1", "qkv"):
            _, r, w = grads[name].shape
            scratch += [
                pltpu.VMEM((r // 2, w), BF16),
                pltpu.VMEM((r // 2, w), BF16),
                pltpu.SemaphoreType.DMA((2,)),
            ]
    vm = pl.BlockSpec(memory_space=pltpu.VMEM)
    res = pl.pallas_call(
        functools.partial(sum_kernel, nd, nt, names),
        out_shape=out_shape,
        in_specs=[vm] * (len(names) + 2),
        out_specs=[vm] * len(out_shape),
        scratch_shapes=scratch,
        compiler_params=pltpu.CompilerParams(
            collective_id=1, has_side_effects=True, vmem_limit_bytes=VMEM_BYTES
        ),
        name="sum_all",
    )(*grads.values(), part_o, part_h)
    return dict(zip(names, res)), res[-2], res[-1]


def small_kernel(nd, nt, stat, vec, stat_all, vec_all, ss, rs, sv, rv):
    place = Place(nd, nt)
    greet(place, "all")
    stat_all[place.t] = stat[...]
    vec_all[place.d] = vec[...]

    def s_copy(k):
        peer = lax.rem(place.t + k, nt)
        return remote(stat, stat_all.at[place.t], ss.at[k], rs.at[place.t], (place.d, peer))

    def v_copy(k):
        peer = lax.rem(place.d + k, nd)
        return remote(vec, vec_all.at[place.d], sv.at[k], rv.at[place.d], (peer, place.t))

    for k in range(1, nt):
        s_copy(k).start()
    for k in range(1, nd):
        v_copy(k).start()
    for k in range(1, nt):
        s_copy(k).wait_send()
        frm = lax.rem(place.t + k, nt)
        remote(stat, stat_all.at[frm], ss.at[k], rs.at[frm], place.pair()).wait_recv()
    for k in range(1, nd):
        v_copy(k).wait_send()
        frm = lax.rem(place.d + k, nd)
        remote(vec, vec_all.at[frm], sv.at[k], rv.at[frm], place.pair()).wait_recv()


def small(stat, vec, nd, nt):
    vm = pl.BlockSpec(memory_space=pltpu.VMEM)
    return pl.pallas_call(
        functools.partial(small_kernel, nd, nt),
        out_shape=(
            jax.ShapeDtypeStruct((nt, *stat.shape), F32),
            jax.ShapeDtypeStruct((nd, *vec.shape), F32),
        ),
        in_specs=[vm] * 2,
        out_specs=[vm] * 2,
        scratch_shapes=[
            pltpu.SemaphoreType.DMA((nt,)),
            pltpu.SemaphoreType.DMA((nt,)),
            pltpu.SemaphoreType.DMA((nd,)),
            pltpu.SemaphoreType.DMA((nd,)),
        ],
        compiler_params=pltpu.CompilerParams(collective_id=2, has_side_effects=True),
        name="small",
    )(stat, vec)


def per_device(
    hidden_in,
    cotangent,
    segment_ids,
    positions,
    norm_gain,
    norm_shift,
    qkv_weight,
    qv_bias,
    key_bias,
    dense_weight,
    fc1_weight,
    fc1_bias,
    fc2_weight,
    out_bias,
):
    nd, nt = lax.axis_size("dp"), lax.axis_size("tensor")
    d_idx, t_idx = lax.axis_index("dp"), lax.axis_index("tensor")
    c = lax.rem(d_idx, 2)
    nch = nd // 2
    rows, wl = hidden_in.shape
    width = wl * nt
    heads = key_bias.shape[0] // 2
    hw = heads * HD
    units = fc1_weight.shape[1] // 2
    ub = units // nch
    score_scale = HD ** (-0.5)

    aux = jnp.concatenate([segment_ids.reshape(-1, LANES), positions.reshape(-1, LANES)])
    full, aux_p = gather(jnp.stack([hidden_in, cotangent]), aux, nd, nt)
    seg = jnp.stack([segment_ids, aux_p[: rows // LANES].reshape(rows)])
    pos = jnp.stack([positions, aux_p[rows // LANES :].reshape(rows)])

    def pick(w, axis, blk):
        shape = w.shape
        n = shape[axis] // (2 * blk)
        w = w.reshape(*shape[:axis], n, 2, blk, *shape[axis + 1 :])
        w = lax.dynamic_index_in_dim(w, c, axis + 1, keepdims=False)
        return w.reshape(*shape[:axis], n * blk, *shape[axis + 1 :])

    w1 = pick(fc1_weight, 1, ub)
    b1 = pick(fc1_bias, 0, ub)
    w2 = pick(fc2_weight, 0, ub)
    wq = lax.dynamic_slice_in_dim(qkv_weight, c * hw, hw, 2)
    qvb = lax.dynamic_slice_in_dim(qv_bias, c * hw, hw, 1)
    kb = lax.dynamic_slice_in_dim(key_bias, c * heads, heads, 0)
    wd = lax.dynamic_slice_in_dim(dense_weight, c * hw, hw, 0)

    in_f = full[0].reshape(2 * rows, width).astype(F32)
    row_mean = jnp.mean(in_f, axis=1, keepdims=True)
    centred = in_f - row_mean
    inv_std = lax.rsqrt(jnp.mean(centred * centred, axis=1, keepdims=True) + norm_epsilon)
    hidden = (centred * inv_std * norm_gain + norm_shift).astype(BF16)

    proj = jnp.einsum("td,dcn->ctn", hidden, wq, preferred_element_type=F32)
    cosine, sine = rotary_tables(pos.reshape(-1), ROT)
    cosine, sine = (v.reshape(2, rows, 1, ROT // 2) for v in (cosine, sine))
    kpad = jnp.concatenate([kb, jnp.zeros((heads, HD - ROT), F32)], axis=1)

    def by_head(v):
        return v.reshape(2, rows, heads, HD)

    queries = rotate_fwd(by_head(proj[0] + qvb[0]), cosine, sine, ROT).astype(BF16)
    keys = rotate_fwd(by_head(proj[1]) + kpad, cosine, sine, ROT).astype(BF16)
    values = by_head(proj[2] + qvb[1]).astype(BF16)
    slots = jnp.arange(rows, dtype=jnp.int32)
    allowed = (seg[:, :, None] == seg[:, None, :]) & (slots[None, :] <= slots[:, None])[None]
    scores = jnp.einsum("bqhd,bkhd->bhqk", queries, keys, preferred_element_type=F32) * score_scale
    scores = jnp.where(allowed[:, None], scores, masked_score)
    top = jnp.max(scores, axis=3, keepdims=True)
    log_total = top + jnp.log(jnp.sum(jnp.exp(scores - top), axis=3, keepdims=True))
    prob_f = jnp.exp(scores - log_total)
    prob_b = prob_f.astype(BF16)
    attn = jnp.einsum("bhqk,bkhd->bqhd", prob_b, values, preferred_element_type=F32).astype(BF16)
    attn_flat = attn.reshape(2 * rows, hw)

    pre = jnp.dot(hidden, w1, preferred_element_type=F32) + b1
    gelu_val, gelu_slope = gelu_pair(pre)
    act = gelu_val.astype(BF16)
    part_o = (
        jnp.dot(attn_flat, wd, preferred_element_type=F32)
        + jnp.dot(act, w2, preferred_element_type=F32)
    ).astype(BF16)

    live = (seg >= 0).reshape(2 * rows, 1)
    cot = full[1].reshape(2 * rows, width)
    grad = jnp.where(live, cot, jnp.zeros_like(cot))
    fc2_g = lax.dot_general(act, grad, (((0,), (0,)), ((), ())), preferred_element_type=F32)
    pairs = [(i, i ^ 1) for i in range(nd)]
    attn_p = lax.ppermute(attn_flat, "dp", pairs).reshape(2, rows, hw)[::-1].reshape(2 * rows, hw)
    attn_all = jnp.where(
        c == 0,
        jnp.concatenate([attn_flat, attn_p], axis=1),
        jnp.concatenate([attn_p, attn_flat], axis=1),
    )
    dense_g = lax.dot_general(attn_all, grad, (((0,), (0,)), ((), ())), preferred_element_type=F32)
    dense_g = pick(dense_g, 0, dense_g.shape[0] // nd)
    d_pre = (
        lax.dot_general(grad, w2, (((1,), (1,)), ((), ())), preferred_element_type=F32) * gelu_slope
    )
    d_pre_b = d_pre.astype(BF16)
    fc1_g = lax.dot_general(hidden, d_pre_b, (((0,), (0,)), ((), ())), preferred_element_type=F32)
    fc1b = jnp.sum(d_pre, axis=0)
    d_attn = by_head(
        lax.dot_general(grad, wd, (((1,), (1,)), ((), ())), preferred_element_type=F32).astype(BF16)
    )
    delta = jnp.sum(d_attn.astype(F32) * attn.astype(F32), axis=3)
    d_prob = jnp.einsum("bqhd,bkhd->bhqk", d_attn, values, preferred_element_type=F32)
    d_score = (prob_f * (d_prob - jnp.moveaxis(delta, 2, 1)[..., None]) * score_scale).astype(BF16)
    d_q = jnp.einsum("bhqk,bkhd->bqhd", d_score, keys, preferred_element_type=F32)
    d_k = jnp.einsum("bhqk,bqhd->bkhd", d_score, queries, preferred_element_type=F32)
    d_v = jnp.einsum("bhqk,bqhd->bkhd", prob_b, d_attn, preferred_element_type=F32)
    d_q = rotate_back(d_q, cosine, sine, ROT)
    d_k = rotate_back(d_k, cosine, sine, ROT)
    keyb = jnp.sum(d_k[..., :ROT], axis=(0, 1))
    qb = jnp.sum(d_q, axis=(0, 1)).reshape(hw)
    vb = jnp.sum(d_v, axis=(0, 1)).reshape(hw)
    d_proj = jnp.concatenate([v.reshape(2 * rows, hw) for v in (d_q, d_k, d_v)], axis=1).astype(BF16)
    qkv_g = lax.dot_general(hidden, d_proj, (((0,), (0,)), ((), ())), preferred_element_type=F32)
    part_h = (
        lax.dot_general(
            d_proj, wq.reshape(width, 3 * hw), (((1,), (1,)), ((), ())), preferred_element_type=F32
        )
        + lax.dot_general(d_pre_b, w1, (((1,), (1,)), ((), ())), preferred_element_type=F32)
    ).astype(BF16)

    grads = {
        "fc2": fc2_g.astype(BF16).reshape(nch, ub, width),
        "dense": dense_g.astype(BF16).reshape(nch, -1, width),
        "fc1": fc1_g.astype(BF16).reshape(nch, width // nch, units),
        "qkv": qkv_g.astype(BF16).reshape(nch, width // nch, 3 * hw),
    }
    sums, out_sum, dh = sum_all(
        grads, part_o.reshape(2, rows, width), part_h.reshape(2, rows, width), nd, nt
    )

    def both(own, other, axis):
        first = jnp.where(c == 0, own, other)
        second = jnp.where(c == 0, other, own)
        return jnp.concatenate([first, second], axis=axis)

    r1 = width // nd
    g1 = sums["fc1"].reshape(2, r1, nch, 1, ub)
    fc1_out = both(g1[0], g1[1], 2).reshape(r1, 2 * units)
    gq = sums["qkv"].reshape(2, r1, 3, hw)
    qkv_out = both(gq[0], gq[1], 2)

    col = t_idx * wl
    bias = lax.dynamic_slice_in_dim(out_bias[0] + out_bias[1], col, wl, 0)
    block_out = (hidden_in.astype(F32) + out_sum + bias).astype(BF16)
    mean_own, inv_own = row_mean[:rows], inv_std[:rows]
    normed = (hidden_in.astype(F32) - mean_own) * inv_own
    gain = lax.dynamic_slice_in_dim(norm_gain, col, wl, 0)
    scaled = dh * gain
    stat = jnp.stack([jnp.sum(scaled, axis=1), jnp.sum(scaled * normed, axis=1)]).reshape(-1, LANES)
    norm_g = jnp.stack([jnp.sum(dh * normed, axis=0), jnp.sum(dh, axis=0)])
    own_grad = jnp.where(segment_ids[:, None] >= 0, cotangent, jnp.zeros_like(cotangent)).astype(F32)
    outb = jnp.sum(own_grad, axis=0)
    mine = [v.reshape(-1) for v in (norm_g, outb, fc1b, qb, vb, keyb)]
    sizes = [v.shape[0] for v in mine]
    vec = jnp.concatenate(mine)
    pad = -vec.shape[0] % (8 * LANES)
    vec = jnp.concatenate([vec, jnp.zeros((pad,), F32)]).reshape(-1, LANES)
    stat_all, vec_all = small(stat, vec, nd, nt)
    stat = jnp.sum(stat_all, axis=0).reshape(2, rows, 1) / width
    input_grad = inv_own * (scaled - stat[0] - normed * stat[1]) + own_grad
    vec_all = vec_all.reshape(nd, -1)
    bits, at = [], 0
    for s in sizes:
        bits.append(vec_all[:, at : at + s])
        at += s
    norm_a, outb_a, fc1b_a, qb_a, vb_a, keyb_a = bits
    cw = wl // nd
    norm_sh = lax.dynamic_slice_in_dim(jnp.sum(norm_a, axis=0).reshape(2, wl), d_idx * cw, cw, 1)
    outb_sh = lax.dynamic_slice_in_dim(jnp.sum(outb_a, axis=0), d_idx * cw, cw, 0)
    outb_sh = jnp.stack([outb_sh, outb_sh])
    fc1b_sum = jnp.sum(fc1b_a.reshape(nch, 2, units), axis=0).reshape(2, nch, ub)
    fc1b_sh = fc1b_sum.transpose(1, 0, 2).reshape(nd, ub)
    fc1b_sh = lax.dynamic_index_in_dim(fc1b_sh, d_idx, 0, keepdims=False)
    qv_sum = jnp.stack([jnp.sum(v.reshape(nch, 2 * hw), axis=0) for v in (qb_a, vb_a)])
    qvb_sh = lax.dynamic_slice_in_dim(qv_sum, d_idx * (2 * hw // nd), 2 * hw // nd, 1)
    kb_sum = jnp.sum(keyb_a.reshape(nch, 2 * heads, ROT), axis=0)
    keyb_sh = lax.dynamic_slice_in_dim(kb_sum, d_idx * (ROT // nd), ROT // nd, 1)
    return (
        block_out,
        input_grad,
        norm_sh,
        qkv_out,
        qvb_sh,
        keyb_sh,
        sums["dense"],
        fc1_out,
        fc1b_sh,
        sums["fc2"],
        outb_sh,
    )


def solution(mesh):
    placed = (
        P("dp", "tensor"),
        P("dp", "tensor"),
        P("dp"),
        P("dp"),
        P(),
        P(),
        P(None, None, "tensor"),
        P(None, "tensor"),
        P("tensor", None),
        P("tensor", None),
        P(None, "tensor"),
        P("tensor"),
        P("tensor", None),
        P(),
    )
    return jax.shard_map(
        per_device,
        mesh=mesh,
        in_specs=placed,
        out_specs=(
            P("dp", "tensor"),
            P("dp", "tensor"),
            P(None, ("tensor", "dp")),
            P("dp", None, "tensor"),
            P(None, ("tensor", "dp")),
            P("tensor", "dp"),
            P(("tensor", "dp"), None),
            P("dp", "tensor"),
            P(("tensor", "dp")),
            P(("tensor", "dp"), None),
            P(None, ("tensor", "dp")),
        ),
        check_vma=False,
    )
```

```python
import functools

import jax
import jax.numpy as jnp
from jax import lax
from jax.experimental import pallas as pl
from jax.experimental.pallas import tpu as pltpu
from jax.sharding import PartitionSpec as P

HD = 64
ROT = 32
LANES = 128

norm_epsilon = 1e-05
gelu_scale = 0.7978845608028654
gelu_cubic = 0.044715
masked_score = -1e30

MESH = pl.DeviceIdType.MESH
F32 = jnp.float32
BF16 = jnp.bfloat16
VMEM_BYTES = 67043328


def gelu_pair(pre_act):
    tanh_val = jnp.tanh(gelu_scale * (pre_act + gelu_cubic * pre_act * pre_act * pre_act))
    gelu_val = 0.5 * pre_act * (1.0 + tanh_val)
    gelu_slope = 0.5 * (1.0 + tanh_val) + 0.5 * pre_act * (
        1.0 - tanh_val * tanh_val
    ) * gelu_scale * (1.0 + 3.0 * gelu_cubic * pre_act * pre_act)
    return (gelu_val, gelu_slope)


class Place:
    def __init__(self, nd, nt):
        self.nd, self.nt = nd, nt
        self.nch = nd // 2
        self.bits = self.nch.bit_length() - 1
        self.d = lax.axis_index("dp")
        self.t = lax.axis_index("tensor")
        self.c = lax.rem(self.d, 2)
        self.j = self.d // 2

    def pair(self):
        return (self.d + 1 - 2 * self.c, self.t)

    def chip_bit(self, b):
        return lax.rem(self.j // (1 << b), 2)

    def over(self, b):
        step = 2 << b
        return (self.d + step - 2 * step * self.chip_bit(b), self.t)

    def right(self):
        return (self.d, jnp.minimum(self.t + 1, self.nt - 1))

    def left(self):
        return (self.d, jnp.maximum(self.t - 1, 0))


def remote(src, dst, send, recv, device):
    return pltpu.make_async_remote_copy(
        src_ref=src, dst_ref=dst, send_sem=send, recv_sem=recv, device_id=device, device_id_type=MESH
    )


def greet(place, dp_peers):
    barrier = pltpu.get_barrier_semaphore()
    count = 0
    for k in range(1, place.nd if dp_peers == "all" else 1):
        pl.semaphore_signal(
            barrier, inc=1, device_id=(lax.rem(place.d + k, place.nd), place.t), device_id_type=MESH
        )
        count += 1
    if dp_peers == "pair":
        pl.semaphore_signal(barrier, inc=1, device_id=place.pair(), device_id_type=MESH)
        count += 1
    for k in range(1, place.nt):
        pl.semaphore_signal(
            barrier, inc=1, device_id=(place.d, lax.rem(place.t + k, place.nt)), device_id_type=MESH
        )
        count += 1
    pl.semaphore_wait(barrier, count)


BK = 512
TW = 256


def mm(a, b, ca=1, cb=0):
    return lax.dot_general(a, b, (((ca,), (cb,)), ((), ())), preferred_element_type=F32)


def at256(i):
    return pl.ds(pl.multiple_of(i * TW, TW), TW)


class Plan:
    def __init__(self, nd, nt, units, heads, ub):
        self.nd, self.nt = nd, nt
        self.nch = nd // 2
        self.bits = self.nch.bit_length() - 1
        self.units, self.heads, self.ub = units, heads, ub
        self.hw = heads * HD
        self.nu = units // BK
        self.width = nt * BK
        self.rb = self.width // nd
        self.rd = 2 * self.hw // nd
        n = 0
        for name, size in (
            ("xb", 2 * nt),
            ("cb", 2 * nt),
            ("hb", 2 * nt),
            ("w1b", 2 * nt + 1),
            ("w2b", 2 * nt + 1),
            ("f2b", self.nu * nt),
            ("f1b", self.nu * nt),
            ("xo", 1),
            ("co", 1),
        ):
            setattr(self, name, n)
            n += size
        self.blocks = n
        self.n2 = 2 * nt
        self.n1 = 2 * (units // TW)
        self.n3 = 2 * 3
        self.pieces = self.n2 + self.n1 + self.n3 + 2


class Piece:
    def __init__(self, place, order, view, recv, ss, rs):
        self.p, self.order, self.view, self.r, self.ss, self.rs = place, order, view, recv, ss, rs
        self.off = [0]
        for i in range(len(order)):
            self.off.append(self.off[-1] + (place.nch >> (i + 1)))

    def block(self, i, m, mine):
        j = 0
        for b in self.order[:i]:
            j = j + self.p.chip_bit(b) * (1 << b)
        if i < len(self.order):
            b = self.order[i]
            v = self.p.chip_bit(b)
            j = j + (v if mine else 1 - v) * (1 << b)
            for q, b2 in enumerate(self.order[i + 1 :]):
                j = j + ((m >> q) & 1) * (1 << b2)
        return j

    def held(self, i, m, before):
        idx = 0
        for r in range(before + 1, min(i, len(self.order))):
            idx = idx + self.p.chip_bit(self.order[r]) * (1 << (r - before - 1))
        if i < len(self.order):
            v = self.p.chip_bit(self.order[i])
            idx = idx + (1 - v) * (1 << (i - before - 1)) + m * (1 << (i - before))
        return self.off[before] + idx

    def copy(self, i, m):
        k = self.off[i] + m
        return remote(
            self.view(self.block(i, m, False)),
            self.r.at[k],
            self.ss.at[k],
            self.rs.at[k],
            self.p.over(self.order[i]),
        )

    def total(self, i, m):
        acc = self.view(self.block(i, m, False))[...].astype(F32)
        for before in range(i):
            acc = acc + self.r[self.held(i, m, before)].astype(F32)
        return acc

    def start(self, i):
        for m in range(self.p.nch >> (i + 1)):
            if i > 0:
                self.view(self.block(i, m, False))[...] = self.total(i, m).astype(BF16)
            self.copy(i, m).start()

    def wait(self, i):
        for m in range(self.p.nch >> (i + 1)):
            self.copy(i, m).wait()

    def final(self):
        return self.total(len(self.order), 0)


def block_kernel(pn, direct, *refs):
    (
        x_in, c_in, tab_in, segr_in, gain, shift, w1, w2, wq, wd, b1, qvb, kb, obias,
        block_out, input_grad, norm_out, qkv_out, qvb_out, keyb_out, dense_out, fc1_out, fc1b_out,
        fc2_out, outb_out,
        pool, wq_v, wd_v, tab, segr, act, buf, slope, qkv, attn, attn_p, dl, at_tmp, dg, dr, rp, fs, fr,
        ostage, mean_v, inv_v, bias3, fb, ob, ng, sv, rv, stc, stt, sr,
        s_load, s_z, r_z, s_c, r_c, s_tab, s_p, r_p, s_d, r_d, s_f, s_os, s_a, s_oc, r_oc, s_ol, r_ol,
        s_hc, r_hc, s_hl, r_hl, s_v, r_v, s_s, r_s, credit,
    ) = refs
    nd, nt, nch, nu = pn.nd, pn.nt, pn.nch, pn.nu
    hw, ub, rb, rd = pn.hw, pn.ub, pn.rb, pn.rd
    place = Place(nd, nt)
    t, c, d = place.t, place.c, place.d
    nq = pn.units // TW

    def load(i, src, dst):
        return pltpu.make_async_copy(src, dst, s_load.at[i])

    loads = {
        "x": [load(0, x_in, pool.at[pn.xb + t])],
        "c": [load(1, c_in, pool.at[pn.cb + t])],
        "tab": [load(2, tab_in, tab.at[0]), load(3, segr_in, segr.at[0])],
        "wd": [load(4, wd.at[pl.ds(pl.multiple_of(c * hw, hw), hw), :], wd_v)],
        "wq": [
            load(5, wq, wq_v)
        ],
        "xo": [load(8, x_in, pool.at[pn.xo]), load(9, c_in, pool.at[pn.co])],
        "w1": [],
        "w2": [],
        "w1r": [],
    }
    n = 10
    for q in range(nq):
        col = (2 * q + c if direct else q) * TW
        src = w1.at[:, :, pl.ds(pl.multiple_of(col, TW), TW)]
        half = pl.ds((q % 2) * TW, TW)
        loads["w1"].append(load(n, src, pool.at[pl.ds(pn.w1b + (q // 2) * nt, nt), :, half]))
        loads["w1r"].append(load(n + 1, src, pool.at[pl.ds(pn.cb + (q // 2) * nt, nt), :, half]))
        n += 2
        for k in range(nt):
            src = w2.at[pl.ds(pl.multiple_of(col, TW), TW), pl.ds(k * BK, BK)]
            loads["w2"].append(load(n, src, pool.at[pn.w2b + (q // 2) * nt + k, half, :]))
            n += 1

    def begin(*names):
        for name in names:
            for cp in loads[name]:
                cp.start()

    def arrive(*names):
        for name in names:
            for cp in loads[name]:
                cp.wait()

    begin("x", "c", "tab", "w1", "wq", "wd", "w2", "xo")
    greet(place, "all")

    def blk(a, s, k):
        return pool.at[a * (pn.cb - pn.xb) + pn.xb + s * nt + k]

    def z_copy(a, k, side):
        return remote(
            blk(a, 0, k), blk(a, 0, k), s_z.at[side, a, k], r_z.at[a, k],
            place.right() if side == 0 else place.left(),
        )

    def c_copy(a, k):
        return remote(blk(a, 0, k), blk(a, 1, k), s_c.at[a, k], r_c.at[a, k], place.pair())

    def tab_copies():
        return (
            remote(tab.at[0], tab.at[1], s_tab.at[0], s_tab.at[1], place.pair()),
            remote(segr.at[0], segr.at[1], s_tab.at[2], s_tab.at[3], place.pair()),
        )

    def item(side, who, i):
        if side == 0:
            first = i <= who
            return jnp.where(first, 0, 1), jnp.where(first, who - i, 2 * who + 1 - i)
        m = nt - who
        first = i < m
        return jnp.where(first, 0, 1), jnp.where(first, who + i, who + i - m)

    def progress(step):
        if step >= 1:
            @pl.when((t > 0) & (step - 1 < 2 * t))
            def _():
                a, k = item(0, t - 1, step - 1)
                z_copy(a, k, 0).wait_recv()
                c_copy(a, k).start()

            @pl.when((t < nt - 1) & (step - 1 < 2 * (nt - 1 - t)))
            def _():
                a, k = item(1, t + 1, step - 1)
                z_copy(a, k, 1).wait_recv()
                c_copy(a, k).start()

        for side in range(2):
            me = t if side == 0 else nt - 1 - t

            @pl.when((me < nt - 1) & (step <= me))
            def _():
                z_copy(0, me - step if side == 0 else nt - 1 - me + step, side).start()

            @pl.when((me < nt - 1) & (step >= me) & (step <= 2 * me))
            def _():
                k = 2 * me - step
                z_copy(1, k if side == 0 else nt - 1 - k, side).start()

    def z_sent(a):
        for m in range(nt):
            for side in range(2):
                me = t if side == 0 else nt - 1 - t

                @pl.when((me < nt - 1) & (m <= me))
                def _():
                    k = me - m
                    z_copy(a, k if side == 0 else nt - 1 - k, side).wait_send()

        for k in range(nt):
            c_copy(a, k).wait_send()

    def arrival(tt, k):
        if k == tt:
            return -1
        return 2 * tt - 1 - k if k < tt else (nt - 1 - tt) + (k - tt - 1)

    orders = [sorted(range(nt), key=lambda k, tt=tt: (arrival(tt, k), k)) for tt in range(nt)]
    needed = [max(arrival(tt, orders[tt][i]) for tt in range(nt)) + 1 for i in range(nt)]

    def chunk(i):
        k = orders[0][i]
        for tt in range(1, nt):
            k = jnp.where(t == tt, orders[tt][i], k)
        return k

    arrive("x", "c", "tab")
    progress(0)
    c_copy(0, t).start()
    c_copy(1, t).start()
    for cp in tab_copies():
        cp.start()
    fb[...] = jnp.zeros_like(fb)
    bias3[...] = jnp.zeros_like(bias3)
    ng[...] = jnp.zeros_like(ng)
    for step in range(1, nt):
        progress(step)
    for k in range(nt):
        c_copy(0, k).wait_recv()

    lr = 32

    @pl.loop(0, 2 * BK // lr)
    def _(q):
        s = q // (BK // lr)
        rows = pl.ds(pl.multiple_of(lax.rem(q, BK // lr) * lr, lr), lr)
        xs = [pool[pn.xb + s * nt + k, rows, :].astype(F32) for k in range(nt)]
        mean = sum(jnp.sum(v, axis=1, keepdims=True) for v in xs) / pn.width
        xs = [v - mean for v in xs]
        var = sum(jnp.sum(v * v, axis=1, keepdims=True) for v in xs) / pn.width
        inv = lax.rsqrt(var + norm_epsilon)
        for k in range(nt):
            cols = pl.ds(k * BK, BK)
            pool[pn.hb + s * nt + k, rows, :] = (xs[k] * inv * gain[:, cols] + shift[:, cols]).astype(BF16)

        @pl.when(s == 0)
        def _():
            mean_v[rows, :] = jnp.broadcast_to(mean, (lr, LANES))
            inv_v[rows, :] = jnp.broadcast_to(inv, (lr, LANES))

    for cp in tab_copies():
        cp.wait()
    arrive("w1")

    def live(s):
        return tab[s, :, pl.ds(2 * LANES, 1)] >= 0.0

    @pl.loop(0, 2 * nq)
    def _(i):
        s, q = i // nq, lax.rem(i, nq)
        half = at256(lax.rem(q, 2))
        pre = sum(
            mm(pool[pn.hb + s * nt + k], pool[pn.w1b + (q // 2) * nt + k, :, half]) for k in range(nt)
        )
        col = (2 * q + c if direct else q) * TW
        pre = pre + b1[:, pl.ds(pl.multiple_of(col, TW), TW)]
        val, slo = gelu_pair(pre)
        val = val.astype(BF16)
        act[s, :, at256(q)] = val
        slope[s, :, at256(q)] = slo
        val = jnp.where(live(s), val, jnp.zeros_like(val))
        buf[at256(q), pl.ds(pl.multiple_of(s * BK, BK), BK)] = val.T

    def tell(i):
        def signal(n, device):
            pl.semaphore_signal(credit.at[3 * i + n], inc=1, device_id=device, device_id_type=MESH)

        signal(0, place.pair())
        pl.when(t > 0)(lambda: signal(2, place.left()))
        pl.when(t < nt - 1)(lambda: signal(1, place.right()))

    def told(i):
        pl.semaphore_wait(credit.at[3 * i], 1)
        pl.when(t > 0)(lambda: pl.semaphore_wait(credit.at[3 * i + 1], 1))
        pl.when(t < nt - 1)(lambda: pl.semaphore_wait(credit.at[3 * i + 2], 1))

    tell(0)

    orders_ab = [list(range(pn.bits)), list(range(pn.bits))[::-1]]

    def piece(index, half, view, recv):
        return Piece(place, orders_ab[half], view, recv, s_p.at[index], r_p.at[index])

    per2 = BK // ub

    def view2(i, h):
        def view(j):
            return pool.at[
                pn.f2b + nu * i + j // per2,
                pl.ds(pl.multiple_of(lax.rem(j, per2) * ub, ub), ub),
                pl.ds(h * TW, TW),
            ]

        return view

    def view1(q, h):
        def view(j):
            r = 2 * j * rb + h * rb
            return pool.at[
                pn.f1b + nu * (r // BK) + q // 2,
                pl.ds(pl.multiple_of(lax.rem(r, BK), rb), rb),
                pl.ds((q % 2) * TW, TW),
            ]

        return view

    def view3(i, h):
        def view(j):
            r = 2 * j * rb + h * rb
            if i < 2:
                b, col = pn.f2b + r // BK, i * TW
            else:
                b, col = pn.f2b + nt + r // (2 * BK), pl.multiple_of(lax.rem(r // BK, 2) * TW, TW)
            return pool.at[b, pl.ds(pl.multiple_of(lax.rem(r, BK), rb), rb), pl.ds(col, TW)]

        return view

    def view_d(h):
        w = pn.width // 2

        def view(j):
            return dg.at[pl.ds(pl.multiple_of(j * rd, rd), rd), pl.ds(h * w, w)]

        return view

    fc2_p = [[piece(2 * i + h, h, view2(i, h), rp.at[2 * i + h]) for h in range(2)] for i in range(nt)]
    fc1_p = [
        [piece(pn.n2 + 2 * q + h, h, view1(q, h), rp.at[pn.n2 + 2 * q + h]) for h in range(2)]
        for q in range(nq)
    ]
    qkv_p = [
        [piece(pn.n2 + pn.n1 + 2 * i + h, h, view3(i, h), rp.at[2 * i + h]) for h in range(2)]
        for i in range(3)
    ]
    den_p = [piece(pn.n2 + pn.n1 + pn.n3 + h, h, view_d(h), dr.at[h]) for h in range(2)]

    os_used = []

    def stage_out(value_to, dst):
        n = len(os_used)
        slot = n % ostage.shape[0]
        if n >= ostage.shape[0]:
            os_used[n - ostage.shape[0]].wait()
        value_to(ostage.at[slot])
        cp = pltpu.make_async_copy(ostage.at[slot, pl.ds(0, dst.shape[0]), :], dst, s_os.at[slot])
        cp.start()
        os_used.append(cp)

    def fin2(i):
        for h in range(2):
            p = fc2_p[i][h]
            p.wait(pn.bits - 1)

            def put(ref, p=p):
                ref[pl.ds(0, ub), :] = p.final()

            col = chunk(i) * BK + h * TW
            stage_out(put, fc2_out.at[:, pl.ds(pl.multiple_of(col, TW), TW)])

    def send_pair(slot):
        return remote(fs.at[slot], fr.at[slot], s_f.at[0, slot], s_f.at[1, slot], place.pair())

    def fin_pair(pieces, slot, dst):
        for h in range(2):
            pieces[h].wait(pn.bits - 1)

        def put(ref):
            for h in range(2):
                @pl.when(c == h)
                def _():
                    ref[pl.ds(0, rb), :] = pieces[h].final()

                @pl.when(c != h)
                def _():
                    fs[slot] = pieces[h].final().astype(BF16)

        stage_out(put, dst)
        send_pair(slot).start()

    def dst1(q, core):
        col = (2 * q + core) * TW if direct else core * pn.units + q * TW
        return fc1_out.at[:, pl.ds(pl.multiple_of(col, TW), TW)]

    def dst3(i, core):
        return qkv_out.at[i, :, pl.ds(pl.multiple_of(core * hw, hw), hw)]

    def fin1(q):
        fin_pair(fc1_p[q], q, dst1(q, c))

    def fin3(i):
        fin_pair(qkv_p[i], nq + i, dst3(i, c))

    def fin_d():
        for h in range(2):
            den_p[h].wait(pn.bits - 1)
            for w in range(pn.width // 2 // TW):

                def put(ref, h=h, w=w):
                    p = den_p[h]
                    cols = pl.ds(w * TW, TW)
                    blk_me = p.block(len(p.order), 0, True)
                    acc = dg[pl.ds(pl.multiple_of(blk_me * rd, rd), rd), pl.ds(h * (pn.width // 2) + w * TW, TW)].astype(F32)
                    for before in range(len(p.order)):
                        acc = acc + p.r[p.held(len(p.order), 0, before), :, cols].astype(F32)
                    ref[pl.ds(0, rd), :] = acc

                stage_out(put, dense_out.at[:, pl.ds(h * (pn.width // 2) + w * TW, TW)])

    def mids(pieces, i):
        for p in pieces:
            p.wait(i - 1)
            p.start(i)

    def mid(pieces):
        for i in range(1, pn.bits):
            mids(pieces, i)

    def fc2_chunk(i):
        k = chunk(i)
        c_copy(1, k).wait_recv()

        @pl.loop(0, 2 * nu)
        def _(q):
            u, h = q // 2, lax.rem(q, 2)
            rows = pl.ds(pl.multiple_of(u * BK, BK), BK)
            out = mm(buf[rows, pl.ds(0, BK)], pool[pn.cb + k, :, at256(h)]) + mm(
                buf[rows, pl.ds(BK, BK)], pool[pn.cb + nt + k, :, at256(h)]
            )
            pool[pn.f2b + nu * i + u, :, at256(h)] = out.astype(BF16)

        for p in fc2_p[i]:
            p.start(0)

    done_steps = [nt - 1]

    def upto(step):
        while done_steps[0] < min(step, 2 * nt - 2):
            done_steps[0] += 1
            progress(done_steps[0])

    fc2_chunk(0)
    upto(needed[1])
    fc2_chunk(1)

    arrive("wq")
    lane = lax.broadcasted_iota(jnp.int32, (BK, TW), 1)
    low = lax.rem(lane, ROT) < ROT // 2

    def swap(v):
        return jnp.where(low, pltpu.roll(v, TW - ROT // 2, 1), pltpu.roll(v, ROT // 2, 1))

    def table(s, i):
        v = tab[s, :, pl.ds(i * LANES, LANES)]
        return jnp.concatenate([v, v], axis=1)

    @pl.loop(0, 2)
    def _(s):
        for i in range(3):
            v = sum(mm(pool[pn.hb + s * nt + k], wq_v[i, pl.ds(k * BK, BK), :]) for k in range(nt))
            cols = pl.ds(pl.multiple_of(c * hw, hw), hw)
            if i == 1:
                v = v + kb[:, cols]
            else:
                v = v + qvb[pl.ds(i // 2, 1), cols]
            if i < 2:
                v = v * table(s, 0) + swap(v) * table(s, 1)
            qkv[i, s] = v.astype(BF16)

    mid(fc2_p[0])
    z_sent(0)

    @pl.loop(0, 2 * nt)
    def _(i):
        for h in range(2):
            pool[pn.xb + i, :, pl.ds(h * TW, TW)] = pool[pn.hb + i, pl.ds(h * TW, TW), :].T

    upto(needed[2])
    fc2_chunk(2)
    mid(fc2_p[1])

    lane1 = lax.broadcasted_iota(jnp.int32, (1, LANES), 1)
    heads2 = [lane1 < HD, lane1 >= HD]
    score_scale = HD ** (-0.5)

    def only(v, h):
        return jnp.where(heads2[h], v, jnp.zeros_like(v))

    def bias_of(s, qt):
        nk = (qt + 1) * TW
        col = lax.broadcasted_iota(jnp.int32, (TW, nk), 1)
        row = lax.broadcasted_iota(jnp.int32, (TW, nk), 0) + qt * TW
        same = tab[s, pl.ds(qt * TW, TW), pl.ds(2 * LANES, 1)] == segr[s, pl.ds(0, 1), pl.ds(0, nk)]
        return jnp.where(same & (col <= row), 0.0, masked_score)

    def probs(qh, keys, bias):
        sc = mm(qh, keys, 1, 1) * score_scale + bias
        top = jnp.max(sc, axis=1, keepdims=True)
        ex = jnp.exp(sc - top)
        return ex * (1.0 / jnp.sum(ex, axis=1, keepdims=True))

    npair = hw // LANES

    @pl.loop(0, 2 * npair)
    def _(i):
        s, hp = i // npair, lax.rem(i, npair)
        cols = pl.ds(pl.multiple_of(hp * LANES, LANES), LANES)
        for qt in range(2):
            rows, kr = pl.ds(qt * TW, TW), pl.ds(0, (qt + 1) * TW)
            bias = bias_of(s, qt)
            out = []
            for h in range(2):
                pb = probs(only(qkv[0, s, rows, cols], h), qkv[1, s, kr, cols], bias).astype(BF16)
                out.append(mm(pb, qkv[2, s, kr, cols]))
            attn[s, rows, cols] = jnp.where(heads2[0], out[0], out[1]).astype(BF16)

    def attn_copy(s):
        return remote(attn.at[s], attn_p.at[1 - s], s_a.at[0, s], s_a.at[1, s], place.pair())

    attn_copy(0).start()
    attn_copy(1).start()
    arrive("wd", "w2")

    @pl.loop(0, 2 * nt * 2)
    def _(i):
        b, h = i // 2, lax.rem(i, 2)
        s, k = b // nt, lax.rem(b, nt)
        half = at256(h)
        out = mm(attn[s], wd_v[:, pl.ds(pl.multiple_of(k * BK + h * TW, TW), TW)])
        for u in range(nu):
            out = out + mm(act[s, :, pl.ds(u * BK, BK)], pool[pn.w2b + u * nt + k, :, half])
        pool[pn.hb + b, :, half] = out.astype(BF16)

    class Line:
        def __init__(self, pr, rbase, sp, rp_, sl, rl):
            self.pr, self.rbase, self.sp, self.rp, self.sl, self.rl = pr, rbase, sp, rp_, sl, rl

        def pair(self, k):
            return remote(
                pool.at[pn.hb + nt + k], pool.at[self.pr + k], self.sp.at[k], self.rp.at[k], place.pair()
            )

        def copy(self, side, k, dev):
            if side == 0:
                slot = k
            else:
                slot = jnp.where(k == t - 1, nt, k)
            return remote(
                pool.at[pn.hb + k], pool.at[self.rbase + slot], self.sl.at[side, k], self.rl.at[slot], dev
            )

        def got(self, slot):
            remote(
                pool.at[pn.hb], pool.at[self.rbase + slot], self.sl.at[0, 0], self.rl.at[slot], place.pair()
            ).wait_recv()

        def send(self, side, step):
            me = t if side == 0 else nt - 1 - t

            @pl.when((me <= step) & (me < nt - 1))
            def _():
                k = nt - 1 - step + me
                k = k if side == 0 else nt - 1 - k

                @pl.when(me > 0)
                def _():
                    self.got(k)

                @pl.loop(0, BK // 64)
                def _(q):
                    rows = pl.ds(pl.multiple_of(q * 64, 64), 64)
                    v = pool[pn.hb + k, rows, :].astype(F32) + pool[self.pr + k, rows, :].astype(F32)
                    r = pool[self.rbase + k, rows, :].astype(F32)
                    pool[pn.hb + k, rows, :] = (v + jnp.where(me > 0, r, 0.0)).astype(BF16)

                self.copy(side, k, place.right() if side == 0 else place.left()).start()

        def sent(self):
            for side in range(2):
                me = t if side == 0 else nt - 1 - t
                for step in range(nt - 1):
                    @pl.when((me <= step) & (me < nt - 1))
                    def _():
                        k = nt - 1 - step + me
                        k = k if side == 0 else nt - 1 - k
                        self.copy(side, k, place.pair()).wait_send()

        def finish(self):
            @pl.when(t > 0)
            def _():
                self.got(t)

            @pl.when(t < nt - 1)
            def _():
                self.got(nt)

        def value(self, rows):
            v = pool[pn.hb + t, rows, :].astype(F32) + pool[self.pr + t, rows, :].astype(F32)
            v = v + jnp.where(t > 0, pool[self.rbase + t, rows, :].astype(F32), 0.0)
            return v + jnp.where(t < nt - 1, pool[self.rbase + nt, rows, :].astype(F32), 0.0)

    line_o = Line(pn.w1b, pn.w1b + nt, s_oc, r_oc, s_ol, r_ol)
    line_h = Line(pn.w2b, pn.w2b + nt, s_hc, r_hc, s_hl, r_hl)
    told(0)
    for k in range(nt):
        line_o.pair(k).start()

    upto(needed[3])
    fc2_chunk(3) if nt > 3 else None
    mid(fc2_p[2])

    @pl.loop(0, 2 * nq)
    def _(i):
        s, q = i // nq, lax.rem(i, nq)
        rows = at256(lax.rem(q, 2))
        v = sum(
            mm(pool[pn.cb + s * nt + k], pool[pn.w2b + (q // 2) * nt + k, rows, :], 1, 1) for k in range(nt)
        )
        v = jnp.where(live(s), v * slope[s, :, at256(q)], 0.0)
        act[s, :, at256(q)] = v.astype(BF16)
        fb[pl.ds(0, 1), at256(q)] += jnp.sum(v, axis=0, keepdims=True)

    tell(1)
    for k in range(nt):
        line_o.pair(k).wait()
    line_o.send(0, 0)
    line_o.send(1, 0)

    def fc1_chunk(q):
        @pl.loop(0, nt)
        def _(k):
            cols = pl.ds(q * TW, TW)
            out = mm(pool[pn.xb + k], act[0, :, cols]) + mm(pool[pn.xb + nt + k], act[1, :, cols])
            pool[pn.f1b + nu * k + q // 2, :, pl.ds((q % 2) * TW, TW)] = out.astype(BF16)

        for p in fc1_p[q]:
            p.start(0)

    fc1_chunk(0)
    mid(fc2_p[3])
    fc1_chunk(1)
    fin2(0)
    fin2(1)
    line_o.send(0, 1)
    line_o.send(1, 1)

    def dcols(i):
        return pl.ds(i * hw, hw)

    @pl.loop(0, 2)
    def _(s):
        v = sum(mm(pool[pn.cb + s * nt + k], wd_v[:, pl.ds(k * BK, BK)], 1, 1) for k in range(nt))
        v = jnp.where(live(s), v, 0.0)
        buf[pl.ds(pl.multiple_of(s * BK, BK), BK), dcols(3)] = v.astype(BF16)

    ob[...] = jnp.broadcast_to(
        jnp.sum(jnp.where(live(0), pool[pn.cb + t].astype(F32), 0.0), axis=0, keepdims=True), ob.shape
    )
    for s in range(2):
        attn_copy(s).wait()
    for core in range(2):
        for s in range(2):
            mine = attn if core == 0 else attn_p
            v = jnp.where(live(s), mine[s], jnp.zeros((BK, hw), BF16))
            at_tmp[...] = v.T
            who = c if core == 0 else 1 - c
            for j in range(nch // 2):
                off = lax.rem((2 * j + c) * rd, hw)
                dst = (who * (nch // 2) + j) * rd
                dl[pl.ds(pl.multiple_of(dst, rd), rd), pl.ds(s * BK, BK)] = at_tmp[
                    pl.ds(pl.multiple_of(off, rd), rd), :
                ]

    @pl.loop(0, 2 * nt)
    def _(i):
        k, h = i // 2, lax.rem(i, 2)
        out = mm(dl[:, pl.ds(0, BK)], pool[pn.cb + k, :, at256(h)]) + mm(
            dl[:, pl.ds(BK, BK)], pool[pn.cb + nt + k, :, at256(h)]
        )
        dg[:, pl.ds(pl.multiple_of(i * TW, TW), TW)] = out.astype(BF16)

    z_sent(1)
    begin("w1r")
    fc1_chunk(2)
    mid(fc1_p[0])
    fin2(2)
    fc1_chunk(3) if nq > 3 else None
    mid(fc1_p[1])
    for p in den_p:
        p.start(0)
    fin2(3) if nt > 3 else None
    for b in range(pn.bits):
        pl.semaphore_signal(credit.at[6 + b], inc=1, device_id=place.over(b), device_id_type=MESH)
    line_o.send(0, 2) if nt > 3 else None
    line_o.send(1, 2) if nt > 3 else None

    @pl.loop(0, 2 * npair)
    def _(i):
        s, hp = i // npair, lax.rem(i, npair)
        cols = pl.ds(pl.multiple_of(hp * LANES, LANES), LANES)
        base = pl.multiple_of(s * BK, BK)
        dq, dk, dv = [], [None, None], [None, None]
        for qt in range(2):
            rows, kr, nk = pl.ds(qt * TW, TW), pl.ds(0, (qt + 1) * TW), (qt + 1) * TW
            bias = bias_of(s, qt)
            da = buf[pl.ds(base + qt * TW, TW), pl.ds(pl.multiple_of(3 * hw + hp * LANES, LANES), LANES)]
            prod = da.astype(F32) * attn[s, rows, cols].astype(F32)
            qs, ks, vs = qkv[0, s, rows, cols], qkv[1, s, kr, cols], qkv[2, s, kr, cols]
            got = []
            for h in range(2):
                pf = probs(only(qs, h), ks, bias)
                pb = pf.astype(BF16)
                delta = jnp.sum(only(prod, h), axis=1, keepdims=True)
                dp = mm(only(da, h), vs, 1, 1)
                ds = (pf * (dp - delta) * score_scale).astype(BF16)
                got.append((mm(ds, ks), mm(ds, qs, 0, 0), mm(pb, da, 0, 0)))
            pick = [jnp.where(heads2[0], a, b) for a, b in zip(*got)]
            dq.append(pick[0])
            for lst, v in ((dk, pick[1]), (dv, pick[2])):
                lst[0] = v[:TW] if lst[0] is None else lst[0] + v[:TW]
                if qt:
                    lst[1] = v[TW:]
        low1 = lax.rem(lane1, ROT) < ROT // 2
        for i3, parts in enumerate((dq, dk, dv)):
            for qt in range(2):
                rows = pl.ds(qt * TW, TW)
                v = parts[qt]
                if i3 < 2:
                    sw = jnp.where(
                        low1, pltpu.roll(v, LANES - ROT // 2, 1), pltpu.roll(v, ROT // 2, 1)
                    )
                    v = v * tab[s, rows, pl.ds(0, LANES)] - sw * tab[s, rows, pl.ds(LANES, LANES)]
                bias3[i3, pl.ds(0, 1), cols] += jnp.sum(v, axis=0, keepdims=True)
                buf[
                    pl.ds(base + qt * TW, TW), pl.ds(pl.multiple_of(i3 * hw + hp * LANES, LANES), LANES)
                ] = v.astype(BF16)

    mid(fc1_p[2])
    mid(den_p)
    for b in range(pn.bits):
        pl.semaphore_wait(credit.at[6 + b], 1)

    def qkv_chunk(i):
        @pl.loop(0, nt)
        def _(k):
            out = mm(pool[pn.xb + k], buf[pl.ds(0, BK), dcols(i)]) + mm(
                pool[pn.xb + nt + k], buf[pl.ds(BK, BK), dcols(i)]
            )
            if i < 2:
                pool[pn.f2b + k, :, pl.ds(i * TW, TW)] = out.astype(BF16)
            else:
                pool[pn.f2b + nt + k // 2, :, at256(lax.rem(k, 2))] = out.astype(BF16)

        for p in qkv_p[i]:
            p.start(0)

    qkv_chunk(0)
    mid(fc1_p[3]) if nq > 3 else None
    fin1(0)
    qkv_chunk(1)
    fin1(1)
    qkv_chunk(2)

    arrive("xo")
    line_o.finish()

    @pl.loop(0, BK // 64)
    def _(q):
        rows = pl.ds(pl.multiple_of(q * 64, 64), 64)
        ocol = pl.ds(pl.multiple_of(t * BK, BK), BK)
        v = pool[pn.xo, rows, :].astype(F32) + line_o.value(rows)
        v = v + (obias[pl.ds(0, 1), ocol] + obias[pl.ds(1, 1), ocol])
        block_out[rows, :] = v.astype(BF16)

    line_o.sent()

    arrive("w1r")

    def dh_chunk(b):
        s, k = b // nt, lax.rem(b, nt)

        @pl.loop(0, 2)
        def _(h):
            rows = at256(h)
            base = pl.multiple_of(s * BK, BK)
            out = 0.0
            for i in range(3):
                out = out + mm(
                    buf[pl.ds(base, BK), dcols(i)],
                    wq_v[i, pl.ds(pl.multiple_of(k * BK + h * TW, TW), TW), :], 1, 1,
                )
            for u in range(nu):
                out = out + mm(act[s, :, pl.ds(u * BK, BK)], pool[pn.cb + u * nt + k, rows, :], 1, 1)
            pool[pn.hb + b, :, rows] = out.astype(BF16)

    told(1)

    @pl.loop(0, nt)
    def _(k):
        dh_chunk(nt + k)
        line_h.pair(k).start()

    mid(qkv_p[0])
    fin1(2)

    @pl.loop(0, nt)
    def _(k):
        dh_chunk(k)

    for k in range(nt):
        line_h.pair(k).wait()
    line_h.send(0, 0)
    line_h.send(1, 0)
    fin1(3) if nq > 3 else None
    fin_d()
    mid(qkv_p[1])
    line_h.send(0, 1)
    line_h.send(1, 1)
    mid(qkv_p[2])
    fin3(0)
    if nt > 3:
        line_h.send(0, 2)
        line_h.send(1, 2)
    fin3(1)

    line_h.finish()
    gcol = pl.ds(pl.multiple_of(t * BK, BK), BK)

    def tail(rows):
        dh = line_h.value(rows)
        normed = (pool[pn.xo, rows, :].astype(F32) - mean_v[rows, pl.ds(0, 1)]) * inv_v[rows, pl.ds(0, 1)]
        return dh, normed, dh * gain[:, gcol]

    first = lax.broadcasted_iota(jnp.int32, (64, LANES), 1) == 0

    @pl.loop(0, BK // 64)
    def _(q):
        rows = pl.ds(pl.multiple_of(q * 64, 64), 64)
        dh, normed, scaled = tail(rows)
        s1 = jnp.sum(scaled, axis=1, keepdims=True)
        s2 = jnp.sum(scaled * normed, axis=1, keepdims=True)
        stc[rows, :] = jnp.where(first, s1, s2)
        ng[pl.ds(0, 1), :] += jnp.sum(dh * normed, axis=0, keepdims=True)
        ng[pl.ds(1, 1), :] += jnp.sum(dh, axis=0, keepdims=True)

    stt[...] = stc[...].T[:8]

    def s_copy(k):
        return remote(stt, sr.at[t], s_s.at[k], r_s.at[t], (d, lax.rem(t + k, nt)))

    def v_copy(k):
        peer = lax.rem(d + k, nd)
        return remote(sv.at[peer], rv.at[d], s_v.at[k], r_v.at[d], (peer, t))

    for k in range(1, nt):
        s_copy(k).start()
    cw, hwd = BK // nd, 2 * hw // nd
    sv[...] = jnp.zeros_like(sv)
    for dd in range(nd):
        mine = c == dd % 2
        sv[dd, pl.ds(0, 1), pl.ds(0, ub)] = jnp.where(mine, fb[pl.ds(0, 1), pl.ds((dd // 2) * ub, ub)], 0.0)
        sv[dd, pl.ds(1, 2), pl.ds(0, cw)] = ng[pl.ds(0, 2), pl.ds(dd * cw, cw)]
        sv[dd, pl.ds(3, 1), pl.ds(0, cw)] = ob[pl.ds(0, 1), pl.ds(dd * cw, cw)]
        here = c == (dd * hwd) // hw
        src = pl.ds((dd * hwd) % hw, hwd)
        sv[dd, pl.ds(4, 1), pl.ds(0, hwd)] = jnp.where(here, bias3[0, pl.ds(0, 1), src], 0.0)
        sv[dd, pl.ds(5, 1), pl.ds(0, hwd)] = jnp.where(here, bias3[2, pl.ds(0, 1), src], 0.0)
        for core in range(2):
            sv[dd, pl.ds(6 + core, 1), :] = jnp.where(c == core, bias3[1, pl.ds(0, 1), :], 0.0)
    for k in range(1, nd):
        v_copy(k).start()
    rv[d] = sv[d]
    sr[t] = stt[...]
    fin3(2)
    for slot in range(nq + 3):
        send_pair(slot).wait()

        def put(ref, slot=slot):
            ref[pl.ds(0, rb), :] = fr[slot].astype(F32)

        stage_out(put, dst1(slot, 1 - c) if slot < nq else dst3(slot - nq, 1 - c))
    for k in range(1, nt):
        s_copy(k).wait_send()
        frm = lax.rem(t + k, nt)
        remote(stt, sr.at[frm], s_s.at[k], r_s.at[frm], place.pair()).wait_recv()
    tot = sr[0]
    for k in range(1, nt):
        tot = tot + sr[k]
    stc[...] = jnp.concatenate([tot / pn.width, jnp.zeros((LANES - 8, BK), F32)], axis=0).T

    @pl.loop(0, BK // 64)
    def _(q):
        rows = pl.ds(pl.multiple_of(q * 64, 64), 64)
        dh, normed, scaled = tail(rows)
        v = inv_v[rows, pl.ds(0, 1)] * (scaled - stc[rows, pl.ds(0, 1)] - normed * stc[rows, pl.ds(1, 1)])
        keep = tab[0, rows, pl.ds(2 * LANES, 1)] >= 0.0
        input_grad[rows, :] = v + jnp.where(keep, pool[pn.co, rows, :].astype(F32), 0.0)

    line_h.sent()
    for k in range(1, nd):
        v_copy(k).wait_send()
        frm = lax.rem(d + k, nd)
        remote(sv.at[0], rv.at[frm], s_v.at[k], r_v.at[frm], place.pair()).wait_recv()
    res = rv[0]
    for k in range(1, nd):
        res = res + rv[k]
    fc1b_out[...] = res[0:1, :ub]
    norm_out[...] = res[1:3, :cw]
    outb_out[...] = jnp.concatenate([res[3:4, :cw], res[3:4, :cw]], axis=0)
    qvb_out[...] = res[4:6, :hwd]
    rk = ROT // nd
    turned = pltpu.roll(res, lax.rem(TW - d * rk, TW), 1)
    for core in range(2):
        for h in range(pn.heads):
            keyb_out[pl.ds(core * pn.heads + h, 1), :] = turned[6 + core : 7 + core, h * HD : h * HD + rk]
    for cp in os_used[-ostage.shape[0] :]:
        cp.wait()

def per_device(
    hidden_in,
    cotangent,
    segment_ids,
    positions,
    norm_gain,
    norm_shift,
    qkv_weight,
    qv_bias,
    key_bias,
    dense_weight,
    fc1_weight,
    fc1_bias,
    fc2_weight,
    out_bias,
):
    nd, nt = lax.axis_size("dp"), lax.axis_size("tensor")
    c = lax.rem(lax.axis_index("dp"), 2)
    nch = nd // 2
    rows, wl = hidden_in.shape
    width = wl * nt
    heads = key_bias.shape[0] // 2
    units = fc1_weight.shape[1] // 2
    ub = units // nch
    pn = Plan(nd, nt, units, heads, ub)
    hw, rb, rd, nq = pn.hw, pn.rb, pn.rd, units // TW
    assert rows == BK and wl == BK and nt == 4 and nq == 4 and hw == TW and rb == ub
    direct = ub == TW

    half = ROT // 2
    lane = jnp.arange(LANES, dtype=jnp.int32) % HD
    rotary = lane < ROT
    inverse = jnp.power(jnp.float32(10000.0), -((lane % half).astype(F32) * (2.0 / ROT)))
    angles = positions.astype(F32)[:, None] * inverse[None, :]
    sign = jnp.where(lane < half, -1.0, 1.0)
    seg = segment_ids.astype(F32)
    tab = jnp.concatenate(
        [
            jnp.where(rotary, jnp.cos(angles), 1.0),
            jnp.where(rotary, jnp.sin(angles) * sign, 0.0),
            jnp.broadcast_to(seg[:, None], (rows, LANES)),
        ],
        axis=1,
    )
    segr = jnp.broadcast_to(seg[None, :], (8, rows))
    kb = jnp.concatenate([key_bias, jnp.zeros((2 * heads, HD - ROT), F32)], axis=1).reshape(1, 2 * hw)

    def pick(w, axis):
        shape = w.shape
        w = w.reshape(*shape[:axis], nch, 2, ub, *shape[axis + 1 :])
        w = lax.dynamic_index_in_dim(w, c, axis + 1, keepdims=False)
        return w.reshape(*shape[:axis], units, *shape[axis + 1 :])

    w1, w2, b1 = fc1_weight, fc2_weight, fc1_bias
    if not direct:
        w1, w2, b1 = pick(w1, 1), pick(w2, 0), pick(b1, 0)
    w1 = w1.reshape(nt, BK, w1.shape[1])
    wq = lax.dynamic_slice_in_dim(qkv_weight, c * hw, hw, 2).transpose(1, 0, 2)
    b1 = b1.reshape(1, -1)

    vm = pl.BlockSpec(memory_space=pltpu.VMEM)
    anyw = pl.BlockSpec(memory_space=pl.ANY)
    shapes = [
        ((rows, wl), BF16, vm),
        ((rows, wl), F32, vm),
        ((2, wl // nd), F32, vm),
        ((3, rb, 2 * hw), F32, anyw),
        ((2, 2 * hw // nd), F32, vm),
        ((2 * heads, ROT // nd), F32, vm),
        ((rd, width), F32, anyw),
        ((rb, 2 * units), F32, anyw),
        ((1, ub), F32, vm),
        ((ub, width), F32, anyw),
        ((2, wl // nd), F32, vm),
    ]
    dma = pltpu.SemaphoreType.DMA
    nos = 4
    scratch = [
        pltpu.VMEM((pn.blocks, BK, BK), BF16),
        pltpu.VMEM((3, width, hw), BF16),
        pltpu.VMEM((hw, width), BF16),
        pltpu.VMEM((2, rows, 3 * LANES), F32),
        pltpu.VMEM((2, 8, rows), F32),
        pltpu.VMEM((2, rows, units), BF16),
        pltpu.VMEM((units, 2 * rows), BF16),
        pltpu.VMEM((2, rows, units), F32),
        pltpu.VMEM((3, 2, rows, hw), BF16),
        pltpu.VMEM((2, rows, hw), BF16),
        pltpu.VMEM((2, rows, hw), BF16),
        pltpu.VMEM((nch * rd, 2 * rows), BF16),
        pltpu.VMEM((hw, rows), BF16),
        pltpu.VMEM((nch * rd, width), BF16),
        pltpu.VMEM((2, nch - 1, rd, width // 2), BF16),
        pltpu.VMEM((pn.n2 + pn.n1, nch - 1, rb, TW), BF16),
        pltpu.VMEM((nq + 3, rb, TW), BF16),
        pltpu.VMEM((nq + 3, rb, TW), BF16),
        pltpu.VMEM((nos, max(rb, rd), TW), F32),
        pltpu.VMEM((rows, LANES), F32),
        pltpu.VMEM((rows, LANES), F32),
        pltpu.VMEM((3, 8, hw), F32),
        pltpu.VMEM((8, units), F32),
        pltpu.VMEM((8, wl), F32),
        pltpu.VMEM((8, wl), F32),
        pltpu.VMEM((nd, 8, TW), F32),
        pltpu.VMEM((nd, 8, TW), F32),
        pltpu.VMEM((rows, LANES), F32),
        pltpu.VMEM((8, rows), F32),
        pltpu.VMEM((nt, 8, rows), F32),
        dma((10 + nq * (2 + nt),)),
        dma((2, 2, nt)),
        dma((2, nt)),
        dma((2, nt)),
        dma((2, nt)),
        dma((4,)),
        dma((pn.pieces, nch - 1)),
        dma((pn.pieces, nch - 1)),
        dma((2,)),
        dma((2,)),
        dma((2, nq + 3)),
        dma((nos,)),
        dma((2, 2)),
        dma((nt,)),
        dma((nt,)),
        dma((2, nt)),
        dma((nt + 1,)),
        dma((nt,)),
        dma((nt,)),
        dma((2, nt)),
        dma((nt + 1,)),
        dma((nd,)),
        dma((nd,)),
        dma((nt,)),
        dma((nt,)),
        pltpu.SemaphoreType.REGULAR((6 + pn.bits,)),
    ]
    res = pl.pallas_call(
        functools.partial(block_kernel, pn, direct),
        out_shape=[jax.ShapeDtypeStruct(s, dt) for s, dt, _ in shapes],
        in_specs=[anyw, anyw, anyw, anyw, vm, vm, anyw, anyw, anyw, anyw, vm, vm, vm, vm],
        out_specs=[sp for _, _, sp in shapes],
        scratch_shapes=scratch,
        compiler_params=pltpu.CompilerParams(
            collective_id=0, has_side_effects=True, vmem_limit_bytes=VMEM_BYTES
        ),
        name="block",
    )(
        hidden_in, cotangent, tab, segr, norm_gain.reshape(1, width), norm_shift.reshape(1, width),
        w1, w2, wq, dense_weight, b1, qv_bias, kb, out_bias,
    )
    res = list(res)
    res[3] = res[3].transpose(1, 0, 2)
    if not direct:
        res[7] = res[7].reshape(rb, 2, nch, ub).transpose(0, 2, 1, 3).reshape(rb, 2 * units)
    res[8] = res[8].reshape(ub)
    return tuple(res)


def solution(mesh):
    placed = (
        P("dp", "tensor"),
        P("dp", "tensor"),
        P("dp"),
        P("dp"),
        P(),
        P(),
        P(None, None, "tensor"),
        P(None, "tensor"),
        P("tensor", None),
        P("tensor", None),
        P(None, "tensor"),
        P("tensor"),
        P("tensor", None),
        P(),
    )
    return jax.shard_map(
        per_device,
        mesh=mesh,
        in_specs=placed,
        out_specs=(
            P("dp", "tensor"),
            P("dp", "tensor"),
            P(None, ("tensor", "dp")),
            P("dp", None, "tensor"),
            P(None, ("tensor", "dp")),
            P("tensor", "dp"),
            P(("tensor", "dp"), None),
            P("dp", "tensor"),
            P(("tensor", "dp")),
            P(("tensor", "dp"), None),
            P(None, ("tensor", "dp")),
        ),
        check_vma=False,
    )
```

```python
import functools

import jax
import jax.numpy as jnp
from jax import lax
from jax.experimental import pallas as pl
from jax.experimental.pallas import tpu as pltpu
from jax.sharding import PartitionSpec as P

HD = 64
ROT = 32
LANES = 128

norm_epsilon = 1e-05
gelu_scale = 0.7978845608028654
gelu_cubic = 0.044715
masked_score = -1e30

MESH = pl.DeviceIdType.MESH
F32 = jnp.float32
BF16 = jnp.bfloat16
VMEM_BYTES = 67043328


def gelu_tanh(u):
    return jnp.tanh(u * (gelu_scale + (gelu_scale * gelu_cubic) * (u * u)))


def gelu_slope(u):
    tanh_val = gelu_tanh(u)
    return 0.5 * (1.0 + tanh_val) + (0.5 * u) * (1.0 - tanh_val * tanh_val) * (
        gelu_scale + (3.0 * gelu_scale * gelu_cubic) * (u * u)
    )


class Place:
    def __init__(self, nd, nt):
        self.nd, self.nt = nd, nt
        self.nch = nd // 2
        self.bits = self.nch.bit_length() - 1
        self.d = lax.axis_index("dp")
        self.t = lax.axis_index("tensor")
        self.c = lax.rem(self.d, 2)
        self.j = self.d // 2

    def pair(self):
        return (self.d + 1 - 2 * self.c, self.t)

    def chip_bit(self, b):
        return lax.rem(self.j // (1 << b), 2)

    def over(self, b):
        step = 2 << b
        return (self.d + step - 2 * step * self.chip_bit(b), self.t)

    def right(self):
        return (self.d, jnp.minimum(self.t + 1, self.nt - 1))

    def left(self):
        return (self.d, jnp.maximum(self.t - 1, 0))


def remote(src, dst, send, recv, device):
    return pltpu.make_async_remote_copy(
        src_ref=src, dst_ref=dst, send_sem=send, recv_sem=recv, device_id=device, device_id_type=MESH
    )


def greet(place):
    barrier = pltpu.get_barrier_semaphore()

    def signal(d, t):
        pl.semaphore_signal(barrier, inc=1, device_id=(d, t), device_id_type=MESH)

    for k in range(1, place.nd):
        signal(lax.rem(place.d + k, place.nd), place.t)
    for k in range(1, place.nt):
        signal(place.d, lax.rem(place.t + k, place.nt))
        signal(place.pair()[0], lax.rem(place.t + k, place.nt))


def greeted(place):
    pl.semaphore_wait(pltpu.get_barrier_semaphore(), place.nd - 1 + 2 * (place.nt - 1))


BK = 512
TW = 256


def mm(a, b, ca=1, cb=0):
    return lax.dot_general(a, b, (((ca,), (cb,)), ((), ())), preferred_element_type=F32)


def cat(parts, axis):
    return jnp.concatenate(parts, axis=axis)


def at512(i):
    return pl.ds(pl.multiple_of(i * BK, BK), BK)


def at256(i):
    return pl.ds(pl.multiple_of(i * TW, TW), TW)


class Plan:
    def __init__(self, nd, nt, units, heads, ub):
        self.nd, self.nt = nd, nt
        self.nch = nd // 2
        self.bits = self.nch.bit_length() - 1
        self.units, self.heads, self.ub = units, heads, ub
        self.hw = heads * HD
        self.nu = units // BK
        self.width = nt * BK
        self.rb = self.width // nd
        self.rd = 2 * self.hw // nd
        n = 0
        for name, size in (
            ("xb", 2 * nt),
            ("cb", 2 * nt),
            ("hb", 2 * nt),
            ("w1b", 2 * nt + 1),
            ("w2b", 2 * nt + 1),
            ("f2b", self.nu * nt),
            ("f1b", self.nu * nt),
            ("xo", 1),
            ("co", 1),
        ):
            setattr(self, name, n)
            n += size
        self.blocks = n
        self.n2 = 2 * nt
        self.n1 = 2 * (units // TW)
        self.n3 = 2 * 3
        self.pieces = self.n2 + self.n1 + self.n3 + nt


class Piece:
    def __init__(self, place, order, view, recv, ss, rs):
        self.p, self.order, self.view, self.r, self.ss, self.rs = place, order, view, recv, ss, rs
        self.off = [0]
        for i in range(len(order)):
            self.off.append(self.off[-1] + (place.nch >> (i + 1)))

    def block(self, i, m, mine):
        j = 0
        for b in self.order[:i]:
            j = j + self.p.chip_bit(b) * (1 << b)
        if i < len(self.order):
            b = self.order[i]
            v = self.p.chip_bit(b)
            j = j + (v if mine else 1 - v) * (1 << b)
            for q, b2 in enumerate(self.order[i + 1 :]):
                j = j + ((m >> q) & 1) * (1 << b2)
        return j

    def held(self, i, m, before):
        idx = 0
        for r in range(before + 1, min(i, len(self.order))):
            idx = idx + self.p.chip_bit(self.order[r]) * (1 << (r - before - 1))
        if i < len(self.order):
            v = self.p.chip_bit(self.order[i])
            idx = idx + (1 - v) * (1 << (i - before - 1)) + m * (1 << (i - before))
        return self.off[before] + idx

    def copy(self, i, m):
        k = self.off[i] + m
        return remote(
            self.view(self.block(i, m, False)),
            self.r.at[k],
            self.ss.at[k],
            self.rs.at[k],
            self.p.over(self.order[i]),
        )

    def total(self, i, m):
        acc = self.view(self.block(i, m, False))[...].astype(F32)
        for before in range(i):
            acc = acc + self.r[self.held(i, m, before)].astype(F32)
        return acc

    def start(self, i):
        for m in range(self.p.nch >> (i + 1)):
            if i > 0:
                self.view(self.block(i, m, False))[...] = self.total(i, m).astype(BF16)
            self.copy(i, m).start()

    def wait(self, i):
        for m in range(self.p.nch >> (i + 1)):
            self.copy(i, m).wait()

    def final(self):
        return self.total(len(self.order), 0)


def block_kernel(pn, direct, *refs):
    (
        x_in, c_in, tab_in, segr_in, gain, shift, w1, w2, wq, wd, b1, qvb, kb, obias,
        block_out, input_grad, norm_out, qkv_out, qvb_out, keyb_out, dense_out, fc1_out, fc1b_out,
        fc2_out, outb_out,
        pool, wq_v, wd_v, tab, segr, act, buf, pre_v, qkv, attn, attn_p, dl, at_tmp, dg, dr, rp, fs, fr,
        ostage, mi, bias3, fb, ob, ng, sv, rv, stc, stt, sr, st,
        s_load, s_z, r_z, s_c, r_c, s_tab, s_p, r_p, s_d, r_d, s_f, s_os, s_a, s_oc, r_oc, s_ol, r_ol,
        s_hc, r_hc, s_hl, r_hl, s_v, r_v, s_s, r_s, s_st, r_st, credit,
    ) = refs
    nd, nt, nch, nu = pn.nd, pn.nt, pn.nch, pn.nu
    hw, ub, rb, rd = pn.hw, pn.ub, pn.rb, pn.rd
    place = Place(nd, nt)
    t, c, d = place.t, place.c, place.d
    nq = pn.units // TW

    def load(i, src, dst):
        return pltpu.make_async_copy(src, dst, s_load.at[i])

    loads = {
        "x": [load(0, x_in, pool.at[pn.xb + t])],
        "c": [load(1, c_in, pool.at[pn.cb + t])],
        "tab": [load(2, tab_in, tab.at[0]), load(3, segr_in, segr.at[0])],
        "wd": [load(4, wd.at[pl.ds(pl.multiple_of(c * hw, hw), hw), :], wd_v)],
        "wq": [
            load(5, wq, wq_v)
        ],
        "xo": [load(8, x_in, pool.at[pn.xo]), load(9, c_in, pool.at[pn.co])],
        "w1": [],
        "w2": [],
        "w1r": [],
    }
    n = 10
    for q in range(nq):
        col = (2 * q + c if direct else q) * TW
        src = w1.at[:, :, pl.ds(pl.multiple_of(col, TW), TW)]
        half = pl.ds((q % 2) * TW, TW)
        loads["w1"].append(load(n, src, pool.at[pl.ds(pn.w1b + (q // 2) * nt, nt), :, half]))
        loads["w1r"].append(load(n + 1, src, pool.at[pl.ds(pn.cb + (q // 2) * nt, nt), :, half]))
        n += 2
        for k in range(nt):
            src = w2.at[pl.ds(pl.multiple_of(col, TW), TW), pl.ds(k * BK, BK)]
            loads["w2"].append(load(n, src, pool.at[pn.w2b + (q // 2) * nt + k, half, :]))
            n += 1

    def begin(*names):
        for name in names:
            for cp in loads[name]:
                cp.start()

    def arrive(*names):
        for name in names:
            for cp in loads[name]:
                cp.wait()

    begin("x", "c", "tab", "w1", "wq", "wd", "w2", "xo")
    greet(place)
    arrive("x")

    first = lax.broadcasted_iota(jnp.int32, (64, LANES), 1) == 0

    @pl.loop(0, BK // 64)
    def _(q):
        rows = pl.ds(pl.multiple_of(q * 64, 64), 64)
        v = pool[pn.xb + t, rows, :].astype(F32)
        m = jnp.sum(v, axis=1, keepdims=True) / BK
        v = v - m
        stc[rows, :] = jnp.where(first, m, jnp.sum(v * v, axis=1, keepdims=True))

    stt[...] = stc[...].T[:8]
    greeted(place)

    def blk(a, s, k, f):
        return pool.at[a * (pn.cb - pn.xb) + pn.xb + s * nt + k, at256(f), :]

    def z_dev(side):
        return place.right() if side == 0 else place.left()

    def z_copy(a, k, side, f):
        return remote(blk(a, 0, k, f), blk(a, 0, k, f), s_z.at[side, a, k, f], r_z.at[a, k, f], z_dev(side))

    def c_copy(a, k, f):
        return remote(blk(a, 0, k, f), blk(a, 1, k, f), s_c.at[a, k, f], r_c.at[a, k, f], place.pair())

    def own_z(a, side, f):
        src = (x_in, c_in)[a].at[at256(f), :]
        return remote(src, blk(a, 0, t, f), s_z.at[side, a, t, f], r_z.at[a, t, f], z_dev(side))

    def own_c(a, f):
        src = (x_in, c_in)[a].at[at256(f), :]
        return remote(src, blk(a, 1, t, f), s_c.at[a, t, f], r_c.at[a, t, f], place.pair())

    def tab_copies():
        return (
            remote(tab.at[0], tab.at[1], s_tab.at[0], s_tab.at[1], place.pair()),
            remote(segr.at[0], segr.at[1], s_tab.at[2], s_tab.at[3], place.pair()),
        )

    def item(side, who, i):
        if side == 0:
            first = i <= who
            return jnp.where(first, 0, 1), jnp.where(first, who - i, 2 * who + 1 - i)
        m = nt - who
        first = i < m
        return jnp.where(first, 0, 1), jnp.where(first, who + i, who + i - m)

    def progress(step, halves=(0, 1)):
        for f in halves:
            if step >= 1:
                @pl.when((t > 0) & (step - 1 < 2 * t))
                def _():
                    a, k = item(0, t - 1, step - 1)
                    z_copy(a, k, 0, f).wait_recv()
                    c_copy(a, k, f).start()

                @pl.when((t < nt - 1) & (step - 1 < 2 * (nt - 1 - t)))
                def _():
                    a, k = item(1, t + 1, step - 1)
                    z_copy(a, k, 1, f).wait_recv()
                    c_copy(a, k, f).start()

            for side in range(2):
                me = t if side == 0 else nt - 1 - t
                if step == 0:
                    pl.when(me < nt - 1)(lambda side=side: own_z(0, side, f).start())
                else:
                    @pl.when((me < nt - 1) & (step <= me))
                    def _():
                        z_copy(0, me - step if side == 0 else nt - 1 - me + step, side, f).start()

                @pl.when((me < nt - 1) & (step > me) & (step <= 2 * me))
                def _():
                    k = 2 * me - step
                    z_copy(1, k if side == 0 else nt - 1 - k, side, f).start()

        for side in range(2 if 1 in halves else 0):
            me = t if side == 0 else nt - 1 - t

            @pl.when((me < nt - 1) & (step == me))
            def _():
                own_z(1, side, 0).start()
                own_z(1, side, 1).start()

    def z_sent(a):
        for f in range(2):
            for m in range(nt):
                for side in range(2):
                    me = t if side == 0 else nt - 1 - t

                    @pl.when((me < nt - 1) & (m <= me))
                    def _():
                        k = me - m
                        z_copy(a, k if side == 0 else nt - 1 - k, side, f).wait_send()

            for k in range(nt):
                c_copy(a, k, f).wait_send()

    def arrival(tt, k):
        if k == tt:
            return -1
        return 2 * tt - 1 - k if k < tt else (nt - 1 - tt) + (k - tt - 1)

    orders = [sorted(range(nt), key=lambda k, tt=tt: (arrival(tt, k), k)) for tt in range(nt)]
    needed = [max(arrival(tt, orders[tt][i]) for tt in range(nt)) + 1 for i in range(nt)]

    def chunk(i):
        k = orders[0][i]
        for tt in range(1, nt):
            k = jnp.where(t == tt, orders[tt][i], k)
        return k

    def st_copy(s, k):
        peer = lax.rem(t + k, nt)
        dev = (d, peer) if s == 0 else (place.pair()[0], peer)
        return remote(stt, st.at[s, t], s_st.at[s, k], r_st.at[s, t], dev)

    for k in range(nt):
        for s in range(2):
            if k or s:
                st_copy(s, k).start()
    progress(0)
    for f in range(2):
        own_c(0, f).start()
    st[0, t] = stt[...]
    arrive("c", "tab")
    for f in range(2):
        own_c(1, f).start()
    for cp in tab_copies():
        cp.start()
    fb[...] = jnp.zeros_like(fb)
    bias3[...] = jnp.zeros_like(bias3)
    ng[...] = jnp.zeros_like(ng)
    for k in range(nt):
        for s in range(2):
            if k or s:
                frm = lax.rem(t + k, nt)
                st_copy(s, k).wait_send()
                remote(stt, st.at[s, frm], s_st.at[s, k], r_st.at[s, frm], place.pair()).wait_recv()
    for s in range(2):
        mean = sum(st[s, k, pl.ds(0, 1), :] for k in range(nt)) / nt
        dev = 0.0
        for k in range(nt):
            off = st[s, k, pl.ds(0, 1), :] - mean
            dev = dev + st[s, k, pl.ds(1, 1), :] + BK * off * off
        inv = lax.rsqrt(dev / pn.width + norm_epsilon)
        both = jnp.concatenate([mean, inv, jnp.zeros((LANES - 2, BK), F32)], axis=0)
        mi[s] = both.T
    arrive("w1")

    def take(k, start):
        cols = pl.ds(pl.multiple_of(k * BK, BK), BK)
        for s in range(2):
            if s == 1:
                for f in range(2):
                    c_copy(0, k, f).wait_recv()

            @pl.loop(0, BK // 64)
            def _(q):
                rows = pl.ds(pl.multiple_of(q * 64, 64), 64)
                v = pool[pn.xb + s * nt + k, rows, :].astype(F32)
                v = (v - mi[s, rows, pl.ds(0, 1)]) * mi[s, rows, pl.ds(1, 1)]
                pool[pn.hb + s * nt + k, rows, :] = (v * gain[:, cols] + shift[:, cols]).astype(BF16)

            @pl.loop(0, nu)
            def _(u):
                out = mm(pool[pn.hb + s * nt + k], pool[pn.w1b + u * nt + k])
                if start:
                    pre_v[s, :, at512(u)] = out
                else:
                    pre_v[s, :, at512(u)] += out

    take(t, True)
    progress(1)
    pl.when(t >= 1)(lambda: take(t - 1, False))
    progress(2, (0,))
    pl.when(t + 1 < nt)(lambda: take(t + 1, False))
    progress(2, (1,))
    pl.when(t >= 2)(lambda: take(t - 2, False))
    progress(3, (0,))
    pl.when(t + 2 < nt)(lambda: take(t + 2, False))
    progress(3, (1,))
    pl.when(t >= 3)(lambda: take(t - 3, False))
    pl.when(t + 3 < nt)(lambda: take(t + 3, False))

    for cp in tab_copies():
        cp.wait()

    def live(s):
        return tab[s, :, pl.ds(2 * LANES, 1)] >= 0.0

    def biased(s, q):
        col = (2 * q + c if direct else q) * TW
        return pre_v[s, :, at256(q)] + b1[:, pl.ds(pl.multiple_of(col, TW), TW)]

    @pl.loop(0, 2 * nq)
    def _(i):
        s, q = i // nq, lax.rem(i, nq)
        pre = biased(s, q)
        val = (0.5 * pre * (1.0 + gelu_tanh(pre))).astype(BF16)
        act[s, :, at256(q)] = val
        val = jnp.where(live(s), val, jnp.zeros_like(val))
        buf[at256(q), pl.ds(pl.multiple_of(s * BK, BK), BK)] = val.T

    def tell(i):
        def signal(n, device):
            pl.semaphore_signal(credit.at[3 * i + n], inc=1, device_id=device, device_id_type=MESH)

        signal(0, place.pair())
        pl.when(t > 0)(lambda: signal(2, place.left()))
        pl.when(t < nt - 1)(lambda: signal(1, place.right()))

    def told(i):
        pl.semaphore_wait(credit.at[3 * i], 1)
        pl.when(t > 0)(lambda: pl.semaphore_wait(credit.at[3 * i + 1], 1))
        pl.when(t < nt - 1)(lambda: pl.semaphore_wait(credit.at[3 * i + 2], 1))

    tell(0)

    orders_ab = [list(range(pn.bits)), list(range(pn.bits))[::-1]]

    def piece(index, half, view, recv):
        return Piece(place, orders_ab[half], view, recv, s_p.at[index], r_p.at[index])

    per2 = BK // ub

    def view2(i, h):
        def view(j):
            return pool.at[
                pn.f2b + nu * i + j // per2,
                pl.ds(pl.multiple_of(lax.rem(j, per2) * ub, ub), ub),
                pl.ds(h * TW, TW),
            ]

        return view

    def view1(q, h):
        def view(j):
            r = 2 * j * rb + h * rb
            return pool.at[
                pn.f1b + nu * (r // BK) + q // 2,
                pl.ds(pl.multiple_of(lax.rem(r, BK), rb), rb),
                pl.ds((q % 2) * TW, TW),
            ]

        return view

    def view3(i, h):
        def view(j):
            r = 2 * j * rb + h * rb
            if i < 2:
                b, col = pn.f2b + r // BK, i * TW
            else:
                b, col = pn.f2b + nt + r // (2 * BK), pl.multiple_of(lax.rem(r // BK, 2) * TW, TW)
            return pool.at[b, pl.ds(pl.multiple_of(lax.rem(r, BK), rb), rb), pl.ds(col, TW)]

        return view

    def view_d(i):
        def view(j):
            return dg.at[pl.ds(pl.multiple_of(j * rd, rd), rd), pl.ds(i * BK, BK)]

        return view

    fc2_p = [[piece(2 * i + h, h, view2(i, h), rp.at[2 * i + h]) for h in range(2)] for i in range(nt)]
    fc1_p = [
        [piece(pn.n2 + 2 * q + h, h, view1(q, h), rp.at[pn.n2 + 2 * q + h]) for h in range(2)]
        for q in range(nq)
    ]
    qkv_p = [
        [piece(pn.n2 + pn.n1 + 2 * i + h, h, view3(i, h), rp.at[2 * i + h]) for h in range(2)]
        for i in range(3)
    ]
    den_p = [piece(pn.n2 + pn.n1 + pn.n3 + i, i % 2, view_d(i), dr.at[i]) for i in range(nt)]

    os_used = []

    def stage_out(value_to, dst):
        n = len(os_used)
        slot = n % ostage.shape[0]
        if n >= ostage.shape[0]:
            os_used[n - ostage.shape[0]].wait()
        value_to(ostage.at[slot])
        cp = pltpu.make_async_copy(ostage.at[slot, pl.ds(0, dst.shape[0]), :], dst, s_os.at[slot])
        cp.start()
        os_used.append(cp)

    def fin2(i):
        for h in range(2):
            p = fc2_p[i][h]
            p.wait(pn.bits - 1)

            def put(ref, p=p):
                ref[pl.ds(0, ub), :] = p.final()

            col = chunk(i) * BK + h * TW
            stage_out(put, fc2_out.at[:, pl.ds(pl.multiple_of(col, TW), TW)])

    def send_pair(slot):
        return remote(fs.at[slot], fr.at[slot], s_f.at[0, slot], s_f.at[1, slot], place.pair())

    def fin_pair(pieces, slot, dst):
        for h in range(2):
            pieces[h].wait(pn.bits - 1)

        def put(ref):
            for h in range(2):
                @pl.when(c == h)
                def _():
                    ref[pl.ds(0, rb), :] = pieces[h].final()

                @pl.when(c != h)
                def _():
                    fs[slot] = pieces[h].final().astype(BF16)

        stage_out(put, dst)
        send_pair(slot).start()

    def dst1(q, core):
        col = (2 * q + core) * TW if direct else core * pn.units + q * TW
        return fc1_out.at[:, pl.ds(pl.multiple_of(col, TW), TW)]

    def dst3(i, core):
        return qkv_out.at[i, :, pl.ds(pl.multiple_of(core * hw, hw), hw)]

    def fin1(q):
        fin_pair(fc1_p[q], q, dst1(q, c))

    def fin3(i):
        fin_pair(qkv_p[i], nq + i, dst3(i, c))

    def fin_d():
        for i in range(nt):
            p = den_p[i]
            p.wait(pn.bits - 1)
            for h in range(2):

                def put(ref, p=p, i=i, h=h):
                    half = pl.ds(h * TW, TW)
                    me = p.block(len(p.order), 0, True)
                    acc = dg[pl.ds(pl.multiple_of(me * rd, rd), rd), pl.ds(i * BK + h * TW, TW)].astype(F32)
                    for before in range(len(p.order)):
                        acc = acc + p.r[p.held(len(p.order), 0, before), :, half].astype(F32)
                    ref[pl.ds(0, rd), :] = acc

                col = chunk(i) * BK + h * TW
                stage_out(put, dense_out.at[:, pl.ds(pl.multiple_of(col, TW), TW)])

    def mids(pieces, i):
        for p in pieces:
            p.wait(i - 1)
            p.start(i)

    def mid(pieces):
        for i in range(1, pn.bits):
            mids(pieces, i)

    def fc2_chunk(i):
        k = chunk(i)
        for f in range(2):
            c_copy(1, k, f).wait_recv()
        for h in range(2):

            half = pl.ds(h * TW, TW)
            out = mm(buf[...], cat([pool[pn.cb + k, :, half], pool[pn.cb + nt + k, :, half]], 0)).astype(BF16)
            for u in range(nu):
                pool[pn.f2b + nu * i + u, :, half] = out[u * BK : (u + 1) * BK]
            fc2_p[i][h].start(0)

    done_steps = [nt - 1]

    def upto(step):
        while done_steps[0] < min(step, 2 * nt - 2):
            done_steps[0] += 1
            progress(done_steps[0])

    fc2_chunk(0)

    arrive("wq")
    lane = lax.broadcasted_iota(jnp.int32, (BK, TW), 1)
    low = lax.rem(lane, ROT) < ROT // 2

    def swap(v):
        return jnp.where(low, pltpu.roll(v, TW - ROT // 2, 1), pltpu.roll(v, ROT // 2, 1))

    def table(s, i):
        v = tab[s, :, pl.ds(i * LANES, LANES)]
        return jnp.concatenate([v, v], axis=1)

    @pl.loop(0, 2)
    def _(s):
        all_v = mm(cat([pool[pn.hb + s * nt + k] for k in range(nt)], 1), cat([wq_v[i] for i in range(3)], 1))
        for i in range(3):
            v = all_v[:, i * hw : (i + 1) * hw]
            cols = pl.ds(pl.multiple_of(c * hw, hw), hw)
            if i == 1:
                v = v + kb[:, cols]
            else:
                v = v + qvb[pl.ds(i // 2, 1), cols]
            if i < 2:
                v = v * table(s, 0) + swap(v) * table(s, 1)
            qkv[i, s] = v.astype(BF16)

    upto(needed[1])
    fc2_chunk(1)
    z_sent(0)

    @pl.loop(0, 2 * nt)
    def _(i):
        for h in range(2):
            pool[pn.xb + i, :, pl.ds(h * TW, TW)] = pool[pn.hb + i, pl.ds(h * TW, TW), :].T

    mid(fc2_p[0])

    lane1 = lax.broadcasted_iota(jnp.int32, (1, LANES), 1)
    heads2 = [lane1 < HD, lane1 >= HD]
    score_scale = HD ** (-0.5)

    def only(v, h):
        return jnp.where(heads2[h], v, jnp.zeros_like(v))

    def bias_of(s, qt):
        nk = (qt + 1) * TW
        col = lax.broadcasted_iota(jnp.int32, (TW, nk), 1)
        row = lax.broadcasted_iota(jnp.int32, (TW, nk), 0) + qt * TW
        same = tab[s, pl.ds(qt * TW, TW), pl.ds(2 * LANES, 1)] == segr[s, pl.ds(0, 1), pl.ds(0, nk)]
        return jnp.where(same & (col <= row), 0.0, masked_score)

    def probs(qh, keys, bias):
        sc = mm(qh, keys, 1, 1) * score_scale + bias
        top = jnp.max(sc, axis=1, keepdims=True)
        ex = jnp.exp(sc - top)
        return ex * (1.0 / jnp.sum(ex, axis=1, keepdims=True))

    npair = hw // LANES

    def attention(s):
        @pl.loop(0, npair)
        def _(hp):
            cols = pl.ds(pl.multiple_of(hp * LANES, LANES), LANES)
            for qt in range(2):
                rows, kr = pl.ds(qt * TW, TW), pl.ds(0, (qt + 1) * TW)
                bias = bias_of(s, qt)
                out = []
                for h in range(2):
                    pb = probs(only(qkv[0, s, rows, cols], h), qkv[1, s, kr, cols], bias).astype(BF16)
                    out.append(mm(pb, qkv[2, s, kr, cols]))
                attn[s, rows, cols] = jnp.where(heads2[0], out[0], out[1]).astype(BF16)

    def attn_copy(s):
        return remote(attn.at[s], attn_p.at[1 - s], s_a.at[0, s], s_a.at[1, s], place.pair())

    attention(0)
    attn_copy(0).start()
    upto(needed[2])
    fc2_chunk(2)
    mid(fc2_p[1])
    attention(1)
    attn_copy(1).start()
    arrive("wd", "w2")

    class Line:
        def __init__(self, part, pr, rbase, sp, rp_, sl, rl):
            self.part, self.pr, self.rbase, self.sp, self.rp, self.sl, self.rl = part, pr, rbase, sp, rp_, sl, rl

        def pair(self, k):
            return remote(
                pool.at[self.part + nt + k], pool.at[self.pr + k], self.sp.at[k], self.rp.at[k], place.pair()
            )

        def copy(self, side, k, f, dev):
            slot = k if side == 0 else jnp.where(k == t - 1, nt, k)
            return remote(
                pool.at[self.part + k, at256(f), :],
                pool.at[self.rbase + slot, at256(f), :],
                self.sl.at[side, k, f],
                self.rl.at[slot, f],
                dev,
            )

        def got(self, slot, f):
            remote(
                pool.at[self.part, at256(f), :],
                pool.at[self.rbase + slot, at256(f), :],
                self.sl.at[0, 0, f],
                self.rl.at[slot, f],
                place.pair(),
            ).wait_recv()

        def each(self, side, step, do, which="all"):
            me = t if side == 0 else nt - 1 - t
            here = {"all": me <= step, "end": me == 0, "mid": (me > 0) & (me <= step)}[which]

            @pl.when(here & (me < nt - 1))
            def _():
                k = nt - 1 - step + me
                do(k if side == 0 else nt - 1 - k)

        def send(self, step, which):
            for side in range(2):

                def do(k, side=side):
                    for f in range(2):
                        if which == "mid":
                            self.got(k, f)

                        @pl.loop(0, TW // 64)
                        def _(q):
                            rows = pl.ds(pl.multiple_of(f * TW + q * 64, 64), 64)
                            v = pool[self.part + k, rows, :].astype(F32) + pool[self.pr + k, rows, :].astype(F32)
                            if which == "mid":
                                v = v + pool[self.rbase + k, rows, :].astype(F32)
                            pool[self.part + k, rows, :] = v.astype(BF16)

                        self.copy(side, k, f, z_dev(side)).start()

                self.each(side, step, do, which)

        def sent(self):
            for side in range(2):
                for step in range(nt - 1):
                    for f in range(2):
                        self.each(
                            side, step, lambda k, side=side, f=f: self.copy(side, k, f, place.pair()).wait_send()
                        )

        def finish(self, halves=(0, 1)):
            for f in halves:
                pl.when(t > 0)(lambda: self.got(t, f))
                pl.when(t < nt - 1)(lambda: self.got(nt, f))

        def value(self, rows):
            v = pool[self.part + t, rows, :].astype(F32) + pool[self.pr + t, rows, :].astype(F32)
            v = v + jnp.where(t > 0, pool[self.rbase + t, rows, :].astype(F32), 0.0)
            return v + jnp.where(t < nt - 1, pool[self.rbase + nt, rows, :].astype(F32), 0.0)

    line_o = Line(pn.hb, pn.w1b, pn.w1b + nt, s_oc, r_oc, s_ol, r_ol)
    line_h = Line(pn.hb, pn.w2b, pn.w2b + nt, s_hc, r_hc, s_hl, r_hl)
    def out_rows(s):
        @pl.loop(0, nt)
        def _(k):
            rhs = cat([wd_v[:, at512(k)]] + [pool[pn.w2b + u * nt + k] for u in range(nu)], 0)
            pool[pn.hb + s * nt + k] = mm(cat([attn[s], act[s]], 1), rhs).astype(BF16)

    out_rows(1)
    told(0)
    for k in range(nt):
        line_o.pair(k).start()
    out_rows(0)

    for s in range(2):
        attn_copy(s).wait()
    for core in range(2):
        for s in range(2):
            mine = attn if core == 0 else attn_p
            v = jnp.where(live(s), mine[s], jnp.zeros((BK, hw), BF16))
            at_tmp[...] = v.T
            who = c if core == 0 else 1 - c
            for j in range(nch // 2):
                off = lax.rem((2 * j + c) * rd, hw)
                dst = (who * (nch // 2) + j) * rd
                dl[pl.ds(pl.multiple_of(dst, rd), rd), pl.ds(s * BK, BK)] = at_tmp[
                    pl.ds(pl.multiple_of(off, rd), rd), :
                ]

    def dense_chunk(i):
        k = chunk(i)
        out = mm(dl[...], cat([pool[pn.cb + k], pool[pn.cb + nt + k]], 0))
        dg[:, pl.ds(i * BK, BK)] = out.astype(BF16)
        den_p[i].start(0)

    mid(fc2_p[2])
    for i in range(nt - 1):
        dense_chunk(i)
    upto(needed[3])
    for k in range(nt):
        line_o.pair(k).wait()
    for step in range(nt - 1):
        line_o.send(step, "end")
    fc2_chunk(3)
    dense_chunk(3)

    def dpre_block(u):
        @pl.loop(0, 2)
        def _(s):
            v = mm(
                cat([pool[pn.cb + s * nt + k] for k in range(nt)], 1),
                cat([pool[pn.w2b + u * nt + k] for k in range(nt)], 1),
                1,
                1,
            )
            for h in range(2):
                q = 2 * u + h
                w = v[:, h * TW : (h + 1) * TW]
                w = jnp.where(live(s), w * gelu_slope(biased(s, q)), 0.0)
                buf[pl.ds(pl.multiple_of(s * BK, BK), BK), pl.ds(q * TW, TW)] = w.astype(BF16)
                fb[pl.ds(0, 1), pl.ds(q * TW, TW)] += jnp.sum(w, axis=0, keepdims=True)

    def fc1_block(u):
        @pl.loop(0, nt)
        def _(k):
            out = mm(cat([pool[pn.xb + k], pool[pn.xb + nt + k]], 1), buf[:, pl.ds(u * BK, BK)])
            pool[pn.f1b + nu * k + u] = out.astype(BF16)

        for q in (2 * u, 2 * u + 1):
            for p in fc1_p[q]:
                p.start(0)

    dpre_block(0)
    fc1_block(0)
    dpre_block(1)
    tell(1)
    line_o.send(1, "mid")
    fc1_block(1)
    mid(fc2_p[3])
    mid(den_p)

    def dcols(i):
        return pl.ds(i * hw, hw)

    @pl.loop(0, 2)
    def _(s):
        v = mm(cat([pool[pn.cb + s * nt + k] for k in range(nt)], 1), wd_v[...], 1, 1)
        v = jnp.where(live(s), v, 0.0)
        act[s, :, dcols(3)] = v.astype(BF16)

    ob[...] = jnp.broadcast_to(
        jnp.sum(jnp.where(live(0), pool[pn.cb + t].astype(F32), 0.0), axis=0, keepdims=True), ob.shape
    )
    z_sent(1)
    begin("w1r")
    fin2(0)
    fin2(1)
    line_o.send(2, "mid")

    @pl.loop(0, 2 * npair)
    def _(i):
        s, hp = i // npair, lax.rem(i, npair)
        cols = pl.ds(pl.multiple_of(hp * LANES, LANES), LANES)
        dq, dk, dv = [], [None, None], [None, None]
        for qt in range(2):
            rows, kr, nk = pl.ds(qt * TW, TW), pl.ds(0, (qt + 1) * TW), (qt + 1) * TW
            bias = bias_of(s, qt)
            da = act[s, rows, pl.ds(pl.multiple_of(3 * hw + hp * LANES, LANES), LANES)]
            prod = da.astype(F32) * attn[s, rows, cols].astype(F32)
            qs, ks, vs = qkv[0, s, rows, cols], qkv[1, s, kr, cols], qkv[2, s, kr, cols]
            got = []
            for h in range(2):
                pf = probs(only(qs, h), ks, bias)
                pb = pf.astype(BF16)
                delta = jnp.sum(only(prod, h), axis=1, keepdims=True)
                dp = mm(only(da, h), vs, 1, 1)
                ds = (pf * (dp - delta) * score_scale).astype(BF16)
                got.append((mm(ds, ks), mm(ds, qs, 0, 0), mm(pb, da, 0, 0)))
            pick = [jnp.where(heads2[0], a, b) for a, b in zip(*got)]
            dq.append(pick[0])
            for lst, v in ((dk, pick[1]), (dv, pick[2])):
                lst[0] = v[:TW] if lst[0] is None else lst[0] + v[:TW]
                if qt:
                    lst[1] = v[TW:]
        low1 = lax.rem(lane1, ROT) < ROT // 2
        for i3, parts in enumerate((dq, dk, dv)):
            for qt in range(2):
                rows = pl.ds(qt * TW, TW)
                v = parts[qt]
                if i3 < 2:
                    sw = jnp.where(
                        low1, pltpu.roll(v, LANES - ROT // 2, 1), pltpu.roll(v, ROT // 2, 1)
                    )
                    v = v * tab[s, rows, pl.ds(0, LANES)] - sw * tab[s, rows, pl.ds(LANES, LANES)]
                bias3[i3, pl.ds(0, 1), cols] += jnp.sum(v, axis=0, keepdims=True)
                act[s, rows, pl.ds(pl.multiple_of(i3 * hw + hp * LANES, LANES), LANES)] = v.astype(BF16)

    mid(fc1_p[0])
    mid(fc1_p[1])

    def dh_chunk(s, k):
        rhs = cat([wq_v[i, at512(k), :] for i in range(3)] + [pool[pn.cb + u * nt + k] for u in range(nu)], 1)
        lhs = cat([act[s, :, pl.ds(0, 3 * hw)], buf[pl.ds(s * BK, BK), :]], 1)
        pool[pn.hb + s * nt + k] = mm(lhs, rhs, 1, 1).astype(BF16)

    def step_of(tt, k):
        if k == tt:
            return nt
        return nt - 1 - k + tt if k > tt else k + nt - 1 - tt

    far = [sorted(range(nt), key=lambda k, tt=tt: (step_of(tt, k), k)) for tt in range(nt)]

    def far_chunk(i):
        k = far[0][i]
        for tt in range(1, nt):
            k = jnp.where(t == tt, far[tt][i], k)
        return k

    def dh_far(s, i):
        dh_chunk(s, far_chunk(i))
        if s == 1:
            line_h.pair(far_chunk(i)).start()

    def qkv_blocks():
        @pl.loop(0, nt)
        def _(k):
            out = mm(
                cat([pool[pn.xb + k], pool[pn.xb + nt + k]], 1),
                cat([act[0, :, pl.ds(0, 3 * hw)], act[1, :, pl.ds(0, 3 * hw)]], 0),
            ).astype(BF16)
            pool[pn.f2b + k] = out[:, :BK]
            pool[pn.f2b + nt + k // 2, :, at256(lax.rem(k, 2))] = out[:, BK:]

        for i in range(3):
            for p in qkv_p[i]:
                p.start(0)

    told(1)
    arrive("w1r")
    dh_far(1, 0)
    dh_far(1, 1)

    arrive("xo")
    line_o.finish()

    @pl.loop(0, BK // 64)
    def _(q):
        rows = pl.ds(pl.multiple_of(q * 64, 64), 64)
        ocol = pl.ds(pl.multiple_of(t * BK, BK), BK)
        v = pool[pn.xo, rows, :].astype(F32) + line_o.value(rows)
        v = v + (obias[pl.ds(0, 1), ocol] + obias[pl.ds(1, 1), ocol])
        block_out[rows, :] = v.astype(BF16)

    line_o.sent()
    dh_far(0, 0)
    line_h.pair(far_chunk(0)).wait()
    line_h.send(0, "end")
    dh_far(0, 1)
    line_h.pair(far_chunk(1)).wait()
    line_h.send(1, "end")
    dh_far(1, 2)
    dh_far(0, 2)
    line_h.pair(far_chunk(2)).wait()
    line_h.send(2, "end")
    fin2(2)
    fin2(3)
    for b in range(pn.bits):
        pl.semaphore_signal(credit.at[6 + b], inc=1, device_id=place.over(b), device_id_type=MESH)
    mid(fc1_p[2])
    for b in range(pn.bits):
        pl.semaphore_wait(credit.at[6 + b], 1)
    qkv_blocks()
    mid(fc1_p[3])
    dh_far(1, 3)
    dh_far(0, 3)
    line_h.pair(far_chunk(3)).wait()
    line_h.send(1, "mid")
    fin1(0)
    mid(qkv_p[0])
    line_h.send(2, "mid")
    mid(qkv_p[1])
    mid(qkv_p[2])
    fin1(1)
    fin1(2)
    fin1(3)
    fin_d()
    fin3(0)
    fin3(1)

    gcol = pl.ds(pl.multiple_of(t * BK, BK), BK)

    def tail(rows):
        dh = line_h.value(rows)
        normed = (pool[pn.xo, rows, :].astype(F32) - mi[0, rows, pl.ds(0, 1)]) * mi[0, rows, pl.ds(1, 1)]
        return dh, normed, dh * gain[:, gcol]

    def s_copy(k, f):
        src = stt.at[:, pl.ds(f * TW, TW)]
        return remote(src, sr.at[t, :, pl.ds(f * TW, TW)], s_s.at[k, f], r_s.at[t, f], (d, lax.rem(t + k, nt)))

    def tail_one(f):
        line_h.finish((f,))

        @pl.loop(0, TW // 64)
        def _(q):
            rows = pl.ds(pl.multiple_of(f * TW + q * 64, 64), 64)
            dh, normed, scaled = tail(rows)
            s1 = jnp.sum(scaled, axis=1, keepdims=True)
            s2 = jnp.sum(scaled * normed, axis=1, keepdims=True)
            stc[rows, :] = jnp.where(first, s1, s2)
            ng[pl.ds(0, 1), :] += jnp.sum(dh * normed, axis=0, keepdims=True)
            ng[pl.ds(1, 1), :] += jnp.sum(dh, axis=0, keepdims=True)

        half = pl.ds(f * TW, TW)
        stt[:, half] = stc[half, :].T[:8]
        sr[t, :, half] = stt[:, half]
        for k in range(1, nt):
            s_copy(k, f).start()

    def tail_two(f):
        half = pl.ds(f * TW, TW)
        for k in range(1, nt):
            s_copy(k, f).wait_send()
            frm = lax.rem(t + k, nt)
            remote(
                stt.at[:, half], sr.at[frm, :, half], s_s.at[k, f], r_s.at[frm, f], place.pair()
            ).wait_recv()
        tot = sr[0, :, half]
        for k in range(1, nt):
            tot = tot + sr[k, :, half]
        stc[half, :] = jnp.concatenate([tot / pn.width, jnp.zeros((LANES - 8, TW), F32)], axis=0).T

        @pl.loop(0, TW // 64)
        def _(q):
            rows = pl.ds(pl.multiple_of(f * TW + q * 64, 64), 64)
            dh, normed, scaled = tail(rows)
            v = mi[0, rows, pl.ds(1, 1)] * (scaled - stc[rows, pl.ds(0, 1)] - normed * stc[rows, pl.ds(1, 1)])
            keep = tab[0, rows, pl.ds(2 * LANES, 1)] >= 0.0
            input_grad[rows, :] = v + jnp.where(keep, pool[pn.co, rows, :].astype(F32), 0.0)

    tail_one(0)
    tail_one(1)

    def v_copy(k):
        peer = lax.rem(d + k, nd)
        return remote(sv.at[peer], rv.at[d], s_v.at[k], r_v.at[d], (peer, t))

    cw, hwd = BK // nd, 2 * hw // nd
    sv[...] = jnp.zeros_like(sv)
    for dd in range(nd):
        mine = c == dd % 2
        sv[dd, pl.ds(0, 1), pl.ds(0, ub)] = jnp.where(mine, fb[pl.ds(0, 1), pl.ds((dd // 2) * ub, ub)], 0.0)
        sv[dd, pl.ds(1, 2), pl.ds(0, cw)] = ng[pl.ds(0, 2), pl.ds(dd * cw, cw)]
        sv[dd, pl.ds(3, 1), pl.ds(0, cw)] = ob[pl.ds(0, 1), pl.ds(dd * cw, cw)]
        here = c == (dd * hwd) // hw
        src = pl.ds((dd * hwd) % hw, hwd)
        sv[dd, pl.ds(4, 1), pl.ds(0, hwd)] = jnp.where(here, bias3[0, pl.ds(0, 1), src], 0.0)
        sv[dd, pl.ds(5, 1), pl.ds(0, hwd)] = jnp.where(here, bias3[2, pl.ds(0, 1), src], 0.0)
        for core in range(2):
            sv[dd, pl.ds(6 + core, 1), :] = jnp.where(c == core, bias3[1, pl.ds(0, 1), :], 0.0)
    for k in range(1, nd):
        v_copy(k).start()
    rv[d] = sv[d]
    tail_two(0)
    fin3(2)
    for slot in range(nq + 3):
        send_pair(slot).wait()

        def put(ref, slot=slot):
            ref[pl.ds(0, rb), :] = fr[slot].astype(F32)

        stage_out(put, dst1(slot, 1 - c) if slot < nq else dst3(slot - nq, 1 - c))
    tail_two(1)
    line_h.sent()
    for k in range(1, nd):
        v_copy(k).wait_send()
        frm = lax.rem(d + k, nd)
        remote(sv.at[0], rv.at[frm], s_v.at[k], r_v.at[frm], place.pair()).wait_recv()
    res = rv[0]
    for k in range(1, nd):
        res = res + rv[k]
    fc1b_out[...] = res[0:1, :ub]
    norm_out[...] = res[1:3, :cw]
    outb_out[...] = jnp.concatenate([res[3:4, :cw], res[3:4, :cw]], axis=0)
    qvb_out[...] = res[4:6, :hwd]
    rk = ROT // nd
    turned = pltpu.roll(res, lax.rem(TW - d * rk, TW), 1)
    for core in range(2):
        for h in range(pn.heads):
            keyb_out[pl.ds(core * pn.heads + h, 1), :] = turned[6 + core : 7 + core, h * HD : h * HD + rk]
    for cp in os_used[-ostage.shape[0] :]:
        cp.wait()

def per_device(
    hidden_in,
    cotangent,
    segment_ids,
    positions,
    norm_gain,
    norm_shift,
    qkv_weight,
    qv_bias,
    key_bias,
    dense_weight,
    fc1_weight,
    fc1_bias,
    fc2_weight,
    out_bias,
):
    nd, nt = lax.axis_size("dp"), lax.axis_size("tensor")
    c = lax.rem(lax.axis_index("dp"), 2)
    nch = nd // 2
    rows, wl = hidden_in.shape
    width = wl * nt
    heads = key_bias.shape[0] // 2
    units = fc1_weight.shape[1] // 2
    ub = units // nch
    pn = Plan(nd, nt, units, heads, ub)
    hw, rb, rd, nq = pn.hw, pn.rb, pn.rd, units // TW
    assert rows == BK and wl == BK and nt == 4 and nq == 4 and hw == TW and rb == ub
    direct = ub == TW

    half = ROT // 2
    lane = jnp.arange(LANES, dtype=jnp.int32) % HD
    rotary = lane < ROT
    inverse = jnp.power(jnp.float32(10000.0), -((lane % half).astype(F32) * (2.0 / ROT)))
    angles = positions.astype(F32)[:, None] * inverse[None, :]
    sign = jnp.where(lane < half, -1.0, 1.0)
    seg = segment_ids.astype(F32)
    tab = jnp.concatenate(
        [
            jnp.where(rotary, jnp.cos(angles), 1.0),
            jnp.where(rotary, jnp.sin(angles) * sign, 0.0),
            jnp.broadcast_to(seg[:, None], (rows, LANES)),
        ],
        axis=1,
    )
    segr = jnp.broadcast_to(seg[None, :], (8, rows))
    kb = jnp.concatenate([key_bias, jnp.zeros((2 * heads, HD - ROT), F32)], axis=1).reshape(1, 2 * hw)

    def pick(w, axis):
        shape = w.shape
        w = w.reshape(*shape[:axis], nch, 2, ub, *shape[axis + 1 :])
        w = lax.dynamic_index_in_dim(w, c, axis + 1, keepdims=False)
        return w.reshape(*shape[:axis], units, *shape[axis + 1 :])

    w1, w2, b1 = fc1_weight, fc2_weight, fc1_bias
    if not direct:
        w1, w2, b1 = pick(w1, 1), pick(w2, 0), pick(b1, 0)
    w1 = w1.reshape(nt, BK, w1.shape[1])
    wq = lax.dynamic_slice_in_dim(qkv_weight, c * hw, hw, 2).transpose(1, 0, 2)
    b1 = b1.reshape(1, -1)

    vm = pl.BlockSpec(memory_space=pltpu.VMEM)
    anyw = pl.BlockSpec(memory_space=pl.ANY)
    shapes = [
        ((rows, wl), BF16, vm),
        ((rows, wl), F32, vm),
        ((2, wl // nd), F32, vm),
        ((3, rb, 2 * hw), F32, anyw),
        ((2, 2 * hw // nd), F32, vm),
        ((2 * heads, ROT // nd), F32, vm),
        ((rd, width), F32, anyw),
        ((rb, 2 * units), F32, anyw),
        ((1, ub), F32, vm),
        ((ub, width), F32, anyw),
        ((2, wl // nd), F32, vm),
    ]
    dma = pltpu.SemaphoreType.DMA
    nos = 4
    scratch = [
        pltpu.VMEM((pn.blocks, BK, BK), BF16),
        pltpu.VMEM((3, width, hw), BF16),
        pltpu.VMEM((hw, width), BF16),
        pltpu.VMEM((2, rows, 3 * LANES), F32),
        pltpu.VMEM((2, 8, rows), F32),
        pltpu.VMEM((2, rows, units), BF16),
        pltpu.VMEM((units, 2 * rows), BF16),
        pltpu.VMEM((2, rows, units), F32),
        pltpu.VMEM((3, 2, rows, hw), BF16),
        pltpu.VMEM((2, rows, hw), BF16),
        pltpu.VMEM((2, rows, hw), BF16),
        pltpu.VMEM((nch * rd, 2 * rows), BF16),
        pltpu.VMEM((hw, rows), BF16),
        pltpu.VMEM((nch * rd, width), BF16),
        pltpu.VMEM((nt, nch - 1, rd, BK), BF16),
        pltpu.VMEM((pn.n2 + pn.n1, nch - 1, rb, TW), BF16),
        pltpu.VMEM((nq + 3, rb, TW), BF16),
        pltpu.VMEM((nq + 3, rb, TW), BF16),
        pltpu.VMEM((nos, max(rb, rd), TW), F32),
        pltpu.VMEM((2, rows, LANES), F32),
        pltpu.VMEM((3, 8, hw), F32),
        pltpu.VMEM((8, units), F32),
        pltpu.VMEM((8, wl), F32),
        pltpu.VMEM((8, wl), F32),
        pltpu.VMEM((nd, 8, TW), F32),
        pltpu.VMEM((nd, 8, TW), F32),
        pltpu.VMEM((rows, LANES), F32),
        pltpu.VMEM((8, rows), F32),
        pltpu.VMEM((nt, 8, rows), F32),
        pltpu.VMEM((2, nt, 8, rows), F32),
        dma((10 + nq * (2 + nt),)),
        dma((2, 2, nt, 2)),
        dma((2, nt, 2)),
        dma((2, nt, 2)),
        dma((2, nt, 2)),
        dma((4,)),
        dma((pn.pieces, nch - 1)),
        dma((pn.pieces, nch - 1)),
        dma((2,)),
        dma((2,)),
        dma((2, nq + 3)),
        dma((nos,)),
        dma((2, 2)),
        dma((nt,)),
        dma((nt,)),
        dma((2, nt, 2)),
        dma((nt + 1, 2)),
        dma((nt,)),
        dma((nt,)),
        dma((2, nt, 2)),
        dma((nt + 1, 2)),
        dma((nd,)),
        dma((nd,)),
        dma((nt, 2)),
        dma((nt, 2)),
        dma((2, nt)),
        dma((2, nt)),
        pltpu.SemaphoreType.REGULAR((6 + pn.bits,)),
    ]
    res = pl.pallas_call(
        functools.partial(block_kernel, pn, direct),
        out_shape=[jax.ShapeDtypeStruct(s, dt) for s, dt, _ in shapes],
        in_specs=[anyw, anyw, anyw, anyw, vm, vm, anyw, anyw, anyw, anyw, vm, vm, vm, vm],
        out_specs=[sp for _, _, sp in shapes],
        scratch_shapes=scratch,
        compiler_params=pltpu.CompilerParams(
            collective_id=0, has_side_effects=True, vmem_limit_bytes=VMEM_BYTES
        ),
        name="block",
    )(
        hidden_in, cotangent, tab, segr, norm_gain.reshape(1, width), norm_shift.reshape(1, width),
        w1, w2, wq, dense_weight, b1, qv_bias, kb, out_bias,
    )
    res = list(res)
    res[3] = res[3].transpose(1, 0, 2)
    if not direct:
        res[7] = res[7].reshape(rb, 2, nch, ub).transpose(0, 2, 1, 3).reshape(rb, 2 * units)
    res[8] = res[8].reshape(ub)
    return tuple(res)


def solution(mesh):
    placed = (
        P("dp", "tensor"),
        P("dp", "tensor"),
        P("dp"),
        P("dp"),
        P(),
        P(),
        P(None, None, "tensor"),
        P(None, "tensor"),
        P("tensor", None),
        P("tensor", None),
        P(None, "tensor"),
        P("tensor"),
        P("tensor", None),
        P(),
    )
    return jax.shard_map(
        per_device,
        mesh=mesh,
        in_specs=placed,
        out_specs=(
            P("dp", "tensor"),
            P("dp", "tensor"),
            P(None, ("tensor", "dp")),
            P("dp", None, "tensor"),
            P(None, ("tensor", "dp")),
            P("tensor", "dp"),
            P(("tensor", "dp"), None),
            P("dp", "tensor"),
            P(("tensor", "dp")),
            P(("tensor", "dp"), None),
            P(None, ("tensor", "dp")),
        ),
        check_vma=False,
    )
```

```python
import functools

import jax
import jax.numpy as jnp
import numpy as np
from jax import lax
from jax.experimental import pallas as pl
from jax.experimental.pallas import tpu as pltpu
from jax.sharding import PartitionSpec as P

HD = 64
ROT = 32
LANES = 128

norm_epsilon = 1e-05
gelu_scale = 0.7978845608028654
gelu_cubic = 0.044715
masked_score = -1e30

MESH = pl.DeviceIdType.MESH
F32 = jnp.float32
BF16 = jnp.bfloat16
VMEM_BYTES = 67043328


def gelu_tanh(u):
    return jnp.tanh(u * (gelu_scale + (gelu_scale * gelu_cubic) * (u * u)))


def gelu_slope(u):
    tanh_val = gelu_tanh(u)
    return 0.5 * (1.0 + tanh_val) + (0.5 * u) * (1.0 - tanh_val * tanh_val) * (
        gelu_scale + (3.0 * gelu_scale * gelu_cubic) * (u * u)
    )


class Place:
    def __init__(self, nd, nt):
        self.nd, self.nt = nd, nt
        self.nch = nd // 2
        self.bits = self.nch.bit_length() - 1
        self.d = lax.axis_index("dp")
        self.t = lax.axis_index("tensor")
        self.c = lax.rem(self.d, 2)
        self.j = self.d // 2

    def pair(self):
        return (self.d + 1 - 2 * self.c, self.t)

    def chip_bit(self, b):
        return lax.rem(self.j // (1 << b), 2)

    def over(self, b):
        step = 2 << b
        return (self.d + step - 2 * step * self.chip_bit(b), self.t)

    def right(self):
        return (self.d, jnp.minimum(self.t + 1, self.nt - 1))

    def left(self):
        return (self.d, jnp.maximum(self.t - 1, 0))


def remote(src, dst, send, recv, device):
    return pltpu.make_async_remote_copy(
        src_ref=src, dst_ref=dst, send_sem=send, recv_sem=recv, device_id=device, device_id_type=MESH
    )


def greet(place):
    barrier = pltpu.get_barrier_semaphore()

    def signal(d, t):
        pl.semaphore_signal(barrier, inc=1, device_id=(d, t), device_id_type=MESH)

    for k in range(1, place.nd):
        signal(lax.rem(place.d + k, place.nd), place.t)
    for k in range(1, place.nt):
        signal(place.d, lax.rem(place.t + k, place.nt))
        signal(place.pair()[0], lax.rem(place.t + k, place.nt))


def greeted(place):
    pl.semaphore_wait(pltpu.get_barrier_semaphore(), place.nd - 1 + 2 * (place.nt - 1))


BK = 512
TW = 256


def mm(a, b, ca=1, cb=0):
    return lax.dot_general(a, b, (((ca,), (cb,)), ((), ())), preferred_element_type=F32)


def cat(parts, axis):
    return jnp.concatenate(parts, axis=axis)


def at512(i):
    return pl.ds(pl.multiple_of(i * BK, BK), BK)


def at256(i):
    return pl.ds(pl.multiple_of(i * TW, TW), TW)


class Plan:
    def __init__(self, nd, nt, units, heads, ub):
        self.nd, self.nt = nd, nt
        self.nch = nd // 2
        self.bits = self.nch.bit_length() - 1
        self.units, self.heads, self.ub = units, heads, ub
        self.hw = heads * HD
        self.nu = units // BK
        self.width = nt * BK
        self.rb = self.width // nd
        self.rd = 2 * self.hw // nd
        n = 0
        for name, size in (
            ("xb", 2 * nt),
            ("cb", 2 * nt),
            ("hb", 2 * nt),
            ("w1b", 2 * nt + 1),
            ("w2b", 2 * nt + 1),
            ("f2b", self.nu * nt),
            ("f1b", self.nu * nt),
            ("xo", 1),
            ("co", 1),
        ):
            setattr(self, name, n)
            n += size
        self.blocks = n
        self.n2 = 2 * nt
        self.n1 = 2 * (units // TW)
        self.n3 = 2 * 3
        self.pieces = self.n2 + self.n1 + self.n3 + nt


class Piece:
    def __init__(self, place, order, view, recv, ss, rs):
        self.p, self.order, self.view, self.r, self.ss, self.rs = place, order, view, recv, ss, rs
        self.off = [0]
        for i in range(len(order)):
            self.off.append(self.off[-1] + (place.nch >> (i + 1)))

    def block(self, i, m, mine):
        j = 0
        for b in self.order[:i]:
            j = j + self.p.chip_bit(b) * (1 << b)
        if i < len(self.order):
            b = self.order[i]
            v = self.p.chip_bit(b)
            j = j + (v if mine else 1 - v) * (1 << b)
            for q, b2 in enumerate(self.order[i + 1 :]):
                j = j + ((m >> q) & 1) * (1 << b2)
        return j

    def held(self, i, m, before):
        idx = 0
        for r in range(before + 1, min(i, len(self.order))):
            idx = idx + self.p.chip_bit(self.order[r]) * (1 << (r - before - 1))
        if i < len(self.order):
            v = self.p.chip_bit(self.order[i])
            idx = idx + (1 - v) * (1 << (i - before - 1)) + m * (1 << (i - before))
        return self.off[before] + idx

    def copy(self, i, m):
        k = self.off[i] + m
        return remote(
            self.view(self.block(i, m, False)),
            self.r.at[k],
            self.ss.at[k],
            self.rs.at[k],
            self.p.over(self.order[i]),
        )

    def total(self, i, m, rows):
        acc = self.view(self.block(i, m, False))[rows, :].astype(F32)
        for before in range(i):
            acc = acc + self.r[self.held(i, m, before), rows, :].astype(F32)
        return acc

    def each(self, do):
        rows = self.view(0).shape[0]
        size = min(rows, 64)

        @pl.loop(0, rows // size)
        def _(q):
            do(pl.ds(pl.multiple_of(q * size, size), size))

    def start(self, i):
        for m in range(self.p.nch >> (i + 1)):
            if i > 0:
                dst = self.view(self.block(i, m, False))

                def put(rows, dst=dst, m=m):
                    dst[rows, :] = self.total(i, m, rows).astype(BF16)

                self.each(put)
            self.copy(i, m).start()

    def wait(self, i):
        for m in range(self.p.nch >> (i + 1)):
            self.copy(i, m).wait()

    def final(self, to):
        def put(rows):
            to[rows, :] = self.total(len(self.order), 0, rows).astype(to.dtype)

        self.each(put)


def block_kernel(pn, direct, *refs):
    (
        x_in, c_in, seg_in, pos_in, freq, gain, shift, w1, w2, wq, wd, b1, qvb, kb, obias,
        block_out, input_grad, norm_out, qkv_out, qvb_out, keyb_out, dense_out, fc1_out, fc1b_out,
        fc2_out, outb_out,
        pool, wq_v, wd_v, tab, segr, act, buf, pre_v, qkv, attn, attn_p, dl, at_tmp, dg, dr, rp, fs, fr,
        ostage, mi, bias3, fb, ob, ng, sv, rv, stc, stt, sr, st, kbv,
        s_load, s_z, r_z, s_c, r_c, s_tab, s_p, r_p, s_d, r_d, s_f, s_os, s_a, s_oc, r_oc, s_ol, r_ol,
        s_hc, r_hc, s_hl, r_hl, s_v, r_v, s_s, r_s, s_st, r_st, credit,
    ) = refs
    nd, nt, nch, nu = pn.nd, pn.nt, pn.nch, pn.nu
    hw, ub, rb, rd = pn.hw, pn.ub, pn.rb, pn.rd
    place = Place(nd, nt)
    t, c, d = place.t, place.c, place.d
    nq = pn.units // TW

    def load(i, src, dst):
        return pltpu.make_async_copy(src, dst, s_load.at[i])

    loads = {
        "x": [load(0, x_in, pool.at[pn.xb + t])],
        "c": [load(1, c_in, pool.at[pn.cb + t])],
        "wd": [load(4, wd.at[pl.ds(pl.multiple_of(c * hw, hw), hw), :], wd_v)],
        "wq": [
            load(5, wq.at[:, :, pl.ds(pl.multiple_of(c * hw, hw), hw)], wq_v)
        ],
        "xo": [load(8, x_in, pool.at[pn.xo]), load(9, c_in, pool.at[pn.co])],
        "w1": [],
        "w2": [],
        "w1r": [],
    }
    n = 10
    for q in range(nq):
        col = (2 * q + c if direct else q) * TW
        src = w1.at[:, :, pl.ds(pl.multiple_of(col, TW), TW)]
        half = pl.ds((q % 2) * TW, TW)
        loads["w1"].append(load(n, src, pool.at[pl.ds(pn.w1b + (q // 2) * nt, nt), :, half]))
        loads["w1r"].append(load(n + 1, src, pool.at[pl.ds(pn.cb + (q // 2) * nt, nt), :, half]))
        n += 2
        for k in range(nt):
            src = w2.at[pl.ds(pl.multiple_of(col, TW), TW), pl.ds(k * BK, BK)]
            loads["w2"].append(load(n, src, pool.at[pn.w2b + (q // 2) * nt + k, half, :]))
            n += 1

    def begin(*names):
        for name in names:
            for cp in loads[name]:
                cp.start()

    def arrive(*names):
        for name in names:
            for cp in loads[name]:
                cp.wait()

    begin("x", "c", "w1", "wq", "wd", "w2", "xo")
    greet(place)
    arrive("x")

    first = lax.broadcasted_iota(jnp.int32, (64, LANES), 1) == 0

    @pl.loop(0, BK // 64)
    def _(q):
        rows = pl.ds(pl.multiple_of(q * 64, 64), 64)
        v = pool[pn.xb + t, rows, :].astype(F32)
        m = jnp.sum(v, axis=1, keepdims=True) / BK
        v = v - m
        stc[rows, :] = jnp.where(first, m, jnp.sum(v * v, axis=1, keepdims=True))

    stt[...] = stc[...].T[:8]
    greeted(place)

    def blk(a, s, k, f):
        return pool.at[a * (pn.cb - pn.xb) + pn.xb + s * nt + k, at256(f), :]

    def z_dev(side):
        return place.right() if side == 0 else place.left()

    def z_copy(a, k, side, f):
        return remote(blk(a, 0, k, f), blk(a, 0, k, f), s_z.at[side, a, k, f], r_z.at[a, k, f], z_dev(side))

    def c_copy(a, k, f):
        return remote(blk(a, 0, k, f), blk(a, 1, k, f), s_c.at[a, k, f], r_c.at[a, k, f], place.pair())

    def own_z(a, side, f):
        src = (x_in, c_in)[a].at[at256(f), :]
        return remote(src, blk(a, 0, t, f), s_z.at[side, a, t, f], r_z.at[a, t, f], z_dev(side))

    def own_c(a, f):
        src = (x_in, c_in)[a].at[at256(f), :]
        return remote(src, blk(a, 1, t, f), s_c.at[a, t, f], r_c.at[a, t, f], place.pair())

    def tab_copies():
        return (
            remote(tab.at[0], tab.at[1], s_tab.at[0], s_tab.at[1], place.pair()),
            remote(segr.at[0], segr.at[1], s_tab.at[2], s_tab.at[3], place.pair()),
        )

    def item(side, who, i):
        if side == 0:
            first = i <= who
            return jnp.where(first, 0, 1), jnp.where(first, who - i, 2 * who + 1 - i)
        m = nt - who
        first = i < m
        return jnp.where(first, 0, 1), jnp.where(first, who + i, who + i - m)

    def progress(step, halves=(0, 1)):
        for f in halves:
            if step >= 1:
                @pl.when((t > 0) & (step - 1 < 2 * t))
                def _():
                    a, k = item(0, t - 1, step - 1)
                    z_copy(a, k, 0, f).wait_recv()
                    c_copy(a, k, f).start()

                @pl.when((t < nt - 1) & (step - 1 < 2 * (nt - 1 - t)))
                def _():
                    a, k = item(1, t + 1, step - 1)
                    z_copy(a, k, 1, f).wait_recv()
                    c_copy(a, k, f).start()

            for side in range(2):
                me = t if side == 0 else nt - 1 - t
                if step == 0:
                    pl.when(me < nt - 1)(lambda side=side: own_z(0, side, f).start())
                else:
                    @pl.when((me < nt - 1) & (step <= me))
                    def _():
                        z_copy(0, me - step if side == 0 else nt - 1 - me + step, side, f).start()

                @pl.when((me < nt - 1) & (step > me) & (step <= 2 * me))
                def _():
                    k = 2 * me - step
                    z_copy(1, k if side == 0 else nt - 1 - k, side, f).start()

        for side in range(2 if 1 in halves else 0):
            me = t if side == 0 else nt - 1 - t

            @pl.when((me < nt - 1) & (step == me))
            def _():
                own_z(1, side, 0).start()
                own_z(1, side, 1).start()

    def z_sent(a):
        for f in range(2):
            for m in range(nt):
                for side in range(2):
                    me = t if side == 0 else nt - 1 - t

                    @pl.when((me < nt - 1) & (m <= me))
                    def _():
                        k = me - m
                        z_copy(a, k if side == 0 else nt - 1 - k, side, f).wait_send()

            for k in range(nt):
                c_copy(a, k, f).wait_send()

    def arrival(tt, k):
        if k == tt:
            return -1
        return 2 * tt - 1 - k if k < tt else (nt - 1 - tt) + (k - tt - 1)

    orders = [sorted(range(nt), key=lambda k, tt=tt: (arrival(tt, k), k)) for tt in range(nt)]
    needed = [max(arrival(tt, orders[tt][i]) for tt in range(nt)) + 1 for i in range(nt)]

    def chunk(i):
        k = orders[0][i]
        for tt in range(1, nt):
            k = jnp.where(t == tt, orders[tt][i], k)
        return k

    def st_copy(s, k):
        peer = lax.rem(t + k, nt)
        dev = (d, peer) if s == 0 else (place.pair()[0], peer)
        return remote(stt, st.at[s, t], s_st.at[s, k], r_st.at[s, t], dev)

    for k in range(nt):
        for s in range(2):
            if k or s:
                st_copy(s, k).start()
    progress(0)
    for f in range(2):
        own_c(0, f).start()
    st[0, t] = stt[...]

    def column(row):
        return jnp.broadcast_to(row.astype(F32), (LANES, BK)).T

    lane1 = lax.broadcasted_iota(jnp.int32, (1, LANES), 1)
    dim1 = lax.rem(lane1, HD)
    angles = column(pos_in[...]) * freq[...]
    tab[0, :, pl.ds(0, LANES)] = jnp.where(dim1 < ROT, jnp.cos(angles), 1.0)
    sine = jnp.sin(angles)
    sine = jnp.where(dim1 < ROT // 2, -sine, sine)
    tab[0, :, pl.ds(LANES, LANES)] = jnp.where(dim1 < ROT, sine, 0.0)
    tab[0, :, pl.ds(2 * LANES, LANES)] = column(seg_in[...])
    segr[0] = jnp.broadcast_to(seg_in[...].astype(F32), (8, BK))
    kbv[...] = jnp.zeros_like(kbv)
    for h in range(pn.heads):
        kbv[pl.ds(0, 1), pl.ds(h * HD, ROT)] = kb[pl.ds(c * pn.heads + h, 1), :]
    arrive("c")
    for f in range(2):
        own_c(1, f).start()
    for cp in tab_copies():
        cp.start()
    fb[...] = jnp.zeros_like(fb)
    bias3[...] = jnp.zeros_like(bias3)
    ng[...] = jnp.zeros_like(ng)
    for k in range(nt):
        for s in range(2):
            if k or s:
                frm = lax.rem(t + k, nt)
                st_copy(s, k).wait_send()
                remote(stt, st.at[s, frm], s_st.at[s, k], r_st.at[s, frm], place.pair()).wait_recv()
    for s in range(2):
        mean = sum(st[s, k, pl.ds(0, 1), :] for k in range(nt)) / nt
        dev = 0.0
        for k in range(nt):
            off = st[s, k, pl.ds(0, 1), :] - mean
            dev = dev + st[s, k, pl.ds(1, 1), :] + BK * off * off
        inv = lax.rsqrt(dev / pn.width + norm_epsilon)
        both = jnp.concatenate([mean, inv, jnp.zeros((LANES - 2, BK), F32)], axis=0)
        mi[s] = both.T
    arrive("w1")

    def live(s):
        return tab[s, :, pl.ds(2 * LANES, 1)] >= 0.0

    def gelu_block(s, u, pre):
        bias = []
        for q in range(2):
            col = (2 * (2 * u + q) + c if direct else 2 * u + q) * TW
            bias.append(b1[:, pl.ds(pl.multiple_of(col, TW), TW)])
        pre = pre + cat(bias, 1)
        val = (0.5 * pre * (1.0 + gelu_tanh(pre))).astype(BF16)
        act[s, :, at512(u)] = val
        val = jnp.where(live(s), val, jnp.zeros_like(val))
        buf[at512(u), at512(s)] = val.T

    def take(k, start, last=False):
        cols = pl.ds(pl.multiple_of(k * BK, BK), BK)

        @pl.loop(0, 2)
        def _(s):
            @pl.when(s == 1)
            def _():
                for f in range(2):
                    c_copy(0, k, f).wait_recv()

            @pl.loop(0, BK // 64)
            def _(q):
                rows = pl.ds(pl.multiple_of(q * 64, 64), 64)
                v = pool[pn.xb + s * nt + k, rows, :].astype(F32)
                v = (v - mi[s, rows, pl.ds(0, 1)]) * mi[s, rows, pl.ds(1, 1)]
                pool[pn.hb + s * nt + k, rows, :] = (v * gain[:, cols] + shift[:, cols]).astype(BF16)

            @pl.loop(0, nu)
            def _(u):
                out = mm(pool[pn.hb + s * nt + k], pool[pn.w1b + u * nt + k])
                if not start:
                    out = out + pre_v[s, :, at512(u)]
                pre_v[s, :, at512(u)] = out
                if last:
                    gelu_block(s, u, out)

    take(t, True)
    progress(1)
    pl.when(t >= 1)(lambda: take(t - 1, False))
    progress(2, (0,))
    pl.when(t + 1 < nt)(lambda: take(t + 1, False))
    progress(2, (1,))
    take(jnp.where(t >= 2, t - 2, t + 2), False)
    progress(3)
    for cp in tab_copies():
        cp.wait()

    @pl.when((t == 0) | (t == nt - 1))
    def _():
        take(nt - 1 - t, False, True)

    @pl.when((t > 0) & (t < nt - 1))
    def _():
        @pl.loop(0, 2 * nu)
        def _(i):
            s, u = i // nu, lax.rem(i, nu)
            gelu_block(s, u, pre_v[s, :, at512(u)])


    def biased(s, q):
        col = (2 * q + c if direct else q) * TW
        return pre_v[s, :, at256(q)] + b1[:, pl.ds(pl.multiple_of(col, TW), TW)]

    def tell(i):
        def signal(n, device):
            pl.semaphore_signal(credit.at[3 * i + n], inc=1, device_id=device, device_id_type=MESH)

        signal(0, place.pair())
        pl.when(t > 0)(lambda: signal(2, place.left()))
        pl.when(t < nt - 1)(lambda: signal(1, place.right()))

    def told(i):
        pl.semaphore_wait(credit.at[3 * i], 1)
        pl.when(t > 0)(lambda: pl.semaphore_wait(credit.at[3 * i + 1], 1))
        pl.when(t < nt - 1)(lambda: pl.semaphore_wait(credit.at[3 * i + 2], 1))

    tell(0)

    orders_ab = [list(range(pn.bits)), list(range(pn.bits))[::-1]]

    def piece(index, half, view, recv):
        return Piece(place, orders_ab[half], view, recv, s_p.at[index], r_p.at[index])

    per2 = BK // ub

    def view2(i, h):
        def view(j):
            return pool.at[
                pn.f2b + nu * i + j // per2,
                pl.ds(pl.multiple_of(lax.rem(j, per2) * ub, ub), ub),
                pl.ds(h * TW, TW),
            ]

        return view

    def view1(q, h):
        def view(j):
            r = 2 * j * rb + h * rb
            return pool.at[
                pn.f1b + nu * (r // BK) + q // 2,
                pl.ds(pl.multiple_of(lax.rem(r, BK), rb), rb),
                pl.ds((q % 2) * TW, TW),
            ]

        return view

    def view3(i, h):
        def view(j):
            r = 2 * j * rb + h * rb
            if i < 2:
                b, col = pn.f2b + r // BK, i * TW
            else:
                b, col = pn.f2b + nt + r // (2 * BK), pl.multiple_of(lax.rem(r // BK, 2) * TW, TW)
            return pool.at[b, pl.ds(pl.multiple_of(lax.rem(r, BK), rb), rb), pl.ds(col, TW)]

        return view

    def view_d(i):
        def view(j):
            return dg.at[pl.ds(pl.multiple_of(j * rd, rd), rd), pl.ds(i * BK, BK)]

        return view

    fc2_p = [[piece(2 * i + h, h, view2(i, h), rp.at[2 * i + h]) for h in range(2)] for i in range(nt)]
    fc1_p = [
        [piece(pn.n2 + 2 * q + h, h, view1(q, h), rp.at[pn.n2 + 2 * q + h]) for h in range(2)]
        for q in range(nq)
    ]
    qkv_p = [
        [piece(pn.n2 + pn.n1 + 2 * i + h, h, view3(i, h), rp.at[2 * i + h]) for h in range(2)]
        for i in range(3)
    ]
    den_p = [piece(pn.n2 + pn.n1 + pn.n3 + i, i % 2, view_d(i), dr.at[i]) for i in range(nt)]

    os_used = []

    def stage_out(value_to, dst):
        n = len(os_used)
        slot = n % ostage.shape[0]
        if n >= ostage.shape[0]:
            os_used[n - ostage.shape[0]].wait()
        value_to(ostage.at[slot])
        cp = pltpu.make_async_copy(ostage.at[slot, pl.ds(0, dst.shape[0]), :], dst, s_os.at[slot])
        cp.start()
        os_used.append(cp)

    def fin2(i):
        for h in range(2):
            p = fc2_p[i][h]
            p.wait(pn.bits - 1)

            def put(ref, p=p):
                p.final(ref)

            col = chunk(i) * BK + h * TW
            stage_out(put, fc2_out.at[:, pl.ds(pl.multiple_of(col, TW), TW)])

    def send_pair(slot):
        return remote(fs.at[slot], fr.at[slot], s_f.at[0, slot], s_f.at[1, slot], place.pair())

    def fin_pair(pieces, slot, dst):
        for h in range(2):
            pieces[h].wait(pn.bits - 1)

        def put(ref):
            for h in range(2):
                @pl.when(c == h)
                def _():
                    pieces[h].final(ref)

                @pl.when(c != h)
                def _():
                    pieces[h].final(fs.at[slot])

        stage_out(put, dst)
        send_pair(slot).start()

    def dst1(q, core):
        col = (2 * q + core) * TW if direct else core * pn.units + q * TW
        return fc1_out.at[:, pl.ds(pl.multiple_of(col, TW), TW)]

    def dst3(i, core):
        return qkv_out.at[i, :, pl.ds(pl.multiple_of(core * hw, hw), hw)]

    def fin1(q):
        fin_pair(fc1_p[q], q, dst1(q, c))

    def fin3(i):
        fin_pair(qkv_p[i], nq + i, dst3(i, c))

    def fin_d():
        for i in range(nt):
            p = den_p[i]
            p.wait(pn.bits - 1)
            for h in range(2):

                def put(ref, p=p, i=i, h=h):
                    half = pl.ds(h * TW, TW)
                    me = p.block(len(p.order), 0, True)
                    acc = dg[pl.ds(pl.multiple_of(me * rd, rd), rd), pl.ds(i * BK + h * TW, TW)].astype(F32)
                    for before in range(len(p.order)):
                        acc = acc + p.r[p.held(len(p.order), 0, before), :, half].astype(F32)
                    ref[pl.ds(0, rd), :] = acc

                col = chunk(i) * BK + h * TW
                stage_out(put, dense_out.at[:, pl.ds(pl.multiple_of(col, TW), TW)])

    def mids(pieces, i):
        for p in pieces:
            p.wait(i - 1)
            p.start(i)

    def mid(pieces):
        for i in range(1, pn.bits):
            mids(pieces, i)

    def fc2_chunk(i):
        k = chunk(i)
        for f in range(2):
            c_copy(1, k, f).wait_recv()
        for h in range(2):

            half = pl.ds(h * TW, TW)
            out = mm(buf[...], cat([pool[pn.cb + k, :, half], pool[pn.cb + nt + k, :, half]], 0)).astype(BF16)
            for u in range(nu):
                pool[pn.f2b + nu * i + u, :, half] = out[u * BK : (u + 1) * BK]
            fc2_p[i][h].start(0)

    done_steps = [nt - 1]

    def upto(step):
        while done_steps[0] < min(step, 2 * nt - 2):
            done_steps[0] += 1
            progress(done_steps[0])

    fc2_chunk(0)

    arrive("wq")
    lane = lax.broadcasted_iota(jnp.int32, (BK, TW), 1)
    low = lax.rem(lane, ROT) < ROT // 2

    def swap(v):
        return jnp.where(low, pltpu.roll(v, TW - ROT // 2, 1), pltpu.roll(v, ROT // 2, 1))

    def table(s, i):
        v = tab[s, :, pl.ds(i * LANES, LANES)]
        return jnp.concatenate([v, v], axis=1)

    @pl.loop(0, 2)
    def _(s):
        all_v = mm(cat([pool[pn.hb + s * nt + k] for k in range(nt)], 1), cat([wq_v[i] for i in range(3)], 1))
        for i in range(3):
            v = all_v[:, i * hw : (i + 1) * hw]
            cols = pl.ds(pl.multiple_of(c * hw, hw), hw)
            if i == 1:
                v = v + kbv[pl.ds(0, 1), :]
            else:
                v = v + qvb[pl.ds(i // 2, 1), cols]
            if i < 2:
                v = v * table(s, 0) + swap(v) * table(s, 1)
            qkv[i, s] = v.astype(BF16)

    upto(needed[1])
    fc2_chunk(1)
    z_sent(0)

    @pl.loop(0, 2 * nt)
    def _(i):
        for h in range(2):
            pool[pn.xb + i, :, pl.ds(h * TW, TW)] = pool[pn.hb + i, pl.ds(h * TW, TW), :].T

    mid(fc2_p[0])

    heads2 = [lane1 < HD, lane1 >= HD]
    score_scale = HD ** (-0.5)

    def only(v, h):
        return jnp.where(heads2[h], v, jnp.zeros_like(v))

    def bias_of(s, qt):
        nk = (qt + 1) * TW
        col = lax.broadcasted_iota(jnp.int32, (TW, nk), 1)
        row = lax.broadcasted_iota(jnp.int32, (TW, nk), 0) + qt * TW
        same = tab[s, pl.ds(qt * TW, TW), pl.ds(2 * LANES, 1)] == segr[s, pl.ds(0, 1), pl.ds(0, nk)]
        return jnp.where(same & (col <= row), 0.0, masked_score)

    def probs(qh, keys, bias):
        sc = mm(qh, keys, 1, 1) * score_scale + bias
        top = jnp.max(sc, axis=1, keepdims=True)
        ex = jnp.exp(sc - top)
        return ex * (1.0 / jnp.sum(ex, axis=1, keepdims=True))

    npair = hw // LANES

    def attention(s):
        @pl.loop(0, npair)
        def _(hp):
            cols = pl.ds(pl.multiple_of(hp * LANES, LANES), LANES)
            for qt in range(2):
                rows, kr = pl.ds(qt * TW, TW), pl.ds(0, (qt + 1) * TW)
                bias = bias_of(s, qt)
                out = []
                for h in range(2):
                    pb = probs(only(qkv[0, s, rows, cols], h), qkv[1, s, kr, cols], bias).astype(BF16)
                    out.append(mm(pb, qkv[2, s, kr, cols]))
                attn[s, rows, cols] = jnp.where(heads2[0], out[0], out[1]).astype(BF16)

    def attn_copy(s):
        return remote(attn.at[s], attn_p.at[1 - s], s_a.at[0, s], s_a.at[1, s], place.pair())

    attention(0)
    attn_copy(0).start()
    upto(needed[2])
    fc2_chunk(2)
    mid(fc2_p[1])
    attention(1)
    attn_copy(1).start()
    arrive("wd", "w2")

    class Line:
        def __init__(self, part, pr, rbase, sp, rp_, sl, rl):
            self.part, self.pr, self.rbase, self.sp, self.rp, self.sl, self.rl = part, pr, rbase, sp, rp_, sl, rl

        def pair(self, k):
            return remote(
                pool.at[self.part + nt + k], pool.at[self.pr + k], self.sp.at[k], self.rp.at[k], place.pair()
            )

        def copy(self, side, k, f, dev):
            slot = k if side == 0 else jnp.where(k == t - 1, nt, k)
            return remote(
                pool.at[self.part + k, at256(f), :],
                pool.at[self.rbase + slot, at256(f), :],
                self.sl.at[side, k, f],
                self.rl.at[slot, f],
                dev,
            )

        def got(self, slot, f):
            remote(
                pool.at[self.part, at256(f), :],
                pool.at[self.rbase + slot, at256(f), :],
                self.sl.at[0, 0, f],
                self.rl.at[slot, f],
                place.pair(),
            ).wait_recv()

        def each(self, side, step, do, which="all"):
            me = t if side == 0 else nt - 1 - t
            here = {"all": me <= step, "end": me == 0, "mid": (me > 0) & (me <= step)}[which]

            @pl.when(here & (me < nt - 1))
            def _():
                k = nt - 1 - step + me
                do(k if side == 0 else nt - 1 - k)

        def send(self, step, which):
            for side in range(2):

                def do(k, side=side):
                    for f in range(2):
                        if which == "mid":
                            self.got(k, f)

                        @pl.loop(0, TW // 64)
                        def _(q):
                            rows = pl.ds(pl.multiple_of(f * TW + q * 64, 64), 64)
                            v = pool[self.part + k, rows, :].astype(F32) + pool[self.pr + k, rows, :].astype(F32)
                            if which == "mid":
                                v = v + pool[self.rbase + k, rows, :].astype(F32)
                            pool[self.part + k, rows, :] = v.astype(BF16)

                        self.copy(side, k, f, z_dev(side)).start()

                self.each(side, step, do, which)

        def sent(self):
            for side in range(2):
                for step in range(nt - 1):
                    for f in range(2):
                        self.each(
                            side, step, lambda k, side=side, f=f: self.copy(side, k, f, place.pair()).wait_send()
                        )

        def finish(self, halves=(0, 1)):
            for f in halves:
                pl.when(t > 0)(lambda: self.got(t, f))
                pl.when(t < nt - 1)(lambda: self.got(nt, f))

        def value(self, rows):
            v = pool[self.part + t, rows, :].astype(F32) + pool[self.pr + t, rows, :].astype(F32)
            v = v + jnp.where(t > 0, pool[self.rbase + t, rows, :].astype(F32), 0.0)
            return v + jnp.where(t < nt - 1, pool[self.rbase + nt, rows, :].astype(F32), 0.0)

    line_o = Line(pn.hb, pn.w1b, pn.w1b + nt, s_oc, r_oc, s_ol, r_ol)
    line_h = Line(pn.hb, pn.w2b, pn.w2b + nt, s_hc, r_hc, s_hl, r_hl)
    def out_rows(s):
        @pl.loop(0, nt)
        def _(k):
            rhs = cat([wd_v[:, at512(k)]] + [pool[pn.w2b + u * nt + k] for u in range(nu)], 0)
            pool[pn.hb + s * nt + k] = mm(cat([attn[s], act[s]], 1), rhs).astype(BF16)

    out_rows(1)
    told(0)
    for k in range(nt):
        line_o.pair(k).start()

    for s in range(2):
        attn_copy(s).wait()
    for core in range(2):
        for s in range(2):
            mine = attn if core == 0 else attn_p
            v = jnp.where(live(s), mine[s], jnp.zeros((BK, hw), BF16))
            at_tmp[...] = v.T
            who = c if core == 0 else 1 - c
            for j in range(nch // 2):
                off = lax.rem((2 * j + c) * rd, hw)
                dst = (who * (nch // 2) + j) * rd
                dl[pl.ds(pl.multiple_of(dst, rd), rd), pl.ds(s * BK, BK)] = at_tmp[
                    pl.ds(pl.multiple_of(off, rd), rd), :
                ]

    def dense_chunk(i):
        k = chunk(i)
        out = mm(dl[...], cat([pool[pn.cb + k], pool[pn.cb + nt + k]], 0))
        dg[:, pl.ds(i * BK, BK)] = out.astype(BF16)
        den_p[i].start(0)

    mid(fc2_p[2])
    for i in range(nt - 1):
        dense_chunk(i)
    out_rows(0)
    upto(needed[3])
    for k in range(nt):
        line_o.pair(k).wait()
    @pl.loop(0, nt - 1)
    def _(step):
        line_o.send(step, "end")

    fc2_chunk(3)
    dense_chunk(3)

    def dpre_block(u):
        @pl.loop(0, 2)
        def _(s):
            v = mm(
                cat([pool[pn.cb + s * nt + k] for k in range(nt)], 1),
                cat([pool[pn.w2b + u * nt + k] for k in range(nt)], 1),
                1,
                1,
            )
            for h in range(2):
                q = 2 * u + h
                w = v[:, h * TW : (h + 1) * TW]
                w = jnp.where(live(s), w * gelu_slope(biased(s, q)), 0.0)
                buf[pl.ds(pl.multiple_of(s * BK, BK), BK), pl.ds(q * TW, TW)] = w.astype(BF16)
                fb[pl.ds(0, 1), pl.ds(q * TW, TW)] += jnp.sum(w, axis=0, keepdims=True)

    def fc1_block(u):
        @pl.loop(0, nt)
        def _(k):
            out = mm(cat([pool[pn.xb + k], pool[pn.xb + nt + k]], 1), buf[:, pl.ds(u * BK, BK)])
            pool[pn.f1b + nu * k + u] = out.astype(BF16)

        for q in (2 * u, 2 * u + 1):
            for p in fc1_p[q]:
                p.start(0)

    dpre_block(0)
    fc1_block(0)
    dpre_block(1)
    tell(1)
    fc1_block(1)
    line_o.send(1, "mid")
    mid(fc2_p[3])
    mid(den_p)

    def dcols(i):
        return pl.ds(i * hw, hw)

    @pl.loop(0, 2)
    def _(s):
        v = mm(cat([pool[pn.cb + s * nt + k] for k in range(nt)], 1), wd_v[...], 1, 1)
        v = jnp.where(live(s), v, 0.0)
        act[s, :, dcols(3)] = v.astype(BF16)

    ob[...] = jnp.broadcast_to(
        jnp.sum(jnp.where(live(0), pool[pn.cb + t].astype(F32), 0.0), axis=0, keepdims=True), ob.shape
    )
    z_sent(1)
    begin("w1r")
    fin2(0)
    fin2(1)
    @pl.loop(0, 2 * npair)
    def _(i):
        pl.when(i == npair)(lambda: line_o.send(2, "mid"))
        s, hp = i // npair, lax.rem(i, npair)
        cols = pl.ds(pl.multiple_of(hp * LANES, LANES), LANES)
        dq, dk, dv = [], [None, None], [None, None]
        for qt in range(2):
            rows, kr, nk = pl.ds(qt * TW, TW), pl.ds(0, (qt + 1) * TW), (qt + 1) * TW
            bias = bias_of(s, qt)
            da = act[s, rows, pl.ds(pl.multiple_of(3 * hw + hp * LANES, LANES), LANES)]
            prod = da.astype(F32) * attn[s, rows, cols].astype(F32)
            qs, ks, vs = qkv[0, s, rows, cols], qkv[1, s, kr, cols], qkv[2, s, kr, cols]
            got = []
            for h in range(2):
                pf = probs(only(qs, h), ks, bias)
                pb = pf.astype(BF16)
                delta = jnp.sum(only(prod, h), axis=1, keepdims=True)
                dp = mm(only(da, h), vs, 1, 1)
                ds = (pf * (dp - delta) * score_scale).astype(BF16)
                got.append((mm(ds, ks), mm(ds, qs, 0, 0), mm(pb, da, 0, 0)))
            pick = [jnp.where(heads2[0], a, b) for a, b in zip(*got)]
            dq.append(pick[0])
            for lst, v in ((dk, pick[1]), (dv, pick[2])):
                lst[0] = v[:TW] if lst[0] is None else lst[0] + v[:TW]
                if qt:
                    lst[1] = v[TW:]
        low1 = lax.rem(lane1, ROT) < ROT // 2
        for i3, parts in enumerate((dq, dk, dv)):
            for qt in range(2):
                rows = pl.ds(qt * TW, TW)
                v = parts[qt]
                if i3 < 2:
                    sw = jnp.where(
                        low1, pltpu.roll(v, LANES - ROT // 2, 1), pltpu.roll(v, ROT // 2, 1)
                    )
                    v = v * tab[s, rows, pl.ds(0, LANES)] - sw * tab[s, rows, pl.ds(LANES, LANES)]
                bias3[i3, pl.ds(0, 1), cols] += jnp.sum(v, axis=0, keepdims=True)
                act[s, rows, pl.ds(pl.multiple_of(i3 * hw + hp * LANES, LANES), LANES)] = v.astype(BF16)

    mid(fc1_p[0])
    mid(fc1_p[1])

    def dh_chunk(s, k):
        rhs = cat([wq_v[i, at512(k), :] for i in range(3)] + [pool[pn.cb + u * nt + k] for u in range(nu)], 1)
        lhs = cat([act[s, :, pl.ds(0, 3 * hw)], buf[pl.ds(s * BK, BK), :]], 1)
        pool[pn.hb + s * nt + k] = mm(lhs, rhs, 1, 1).astype(BF16)

    def step_of(tt, k):
        if k == tt:
            return nt
        return nt - 1 - k + tt if k > tt else k + nt - 1 - tt

    far = [sorted(range(nt), key=lambda k, tt=tt: (step_of(tt, k), k)) for tt in range(nt)]

    def far_chunk(i):
        k = 0
        for tt in range(nt):
            for n in range(nt):
                k = jnp.where((t == tt) & (i == n), far[tt][n], k)
        return k

    def qkv_blocks():
        @pl.loop(0, nt)
        def _(k):
            out = mm(
                cat([pool[pn.xb + k], pool[pn.xb + nt + k]], 1),
                cat([act[0, :, pl.ds(0, 3 * hw)], act[1, :, pl.ds(0, 3 * hw)]], 0),
            ).astype(BF16)
            pool[pn.f2b + k] = out[:, :BK]
            pool[pn.f2b + nt + k // 2, :, at256(lax.rem(k, 2))] = out[:, BK:]

        for i in range(3):
            for p in qkv_p[i]:
                p.start(0)

    told(1)
    arrive("w1r")
    @pl.loop(0, nt)
    def _(i):
        k = far_chunk(i)
        dh_chunk(1, k)
        line_h.pair(k).start()

    arrive("xo")
    line_o.finish()

    @pl.loop(0, BK // 64)
    def _(q):
        rows = pl.ds(pl.multiple_of(q * 64, 64), 64)
        ocol = pl.ds(pl.multiple_of(t * BK, BK), BK)
        v = pool[pn.xo, rows, :].astype(F32) + line_o.value(rows)
        v = v + (obias[pl.ds(0, 1), ocol] + obias[pl.ds(1, 1), ocol])
        block_out[rows, :] = v.astype(BF16)

    line_o.sent()
    @pl.loop(0, nt)
    def _(i):
        k = far_chunk(i)
        dh_chunk(0, k)
        line_h.pair(k).wait()
        pl.when(i < nt - 1)(lambda: line_h.send(i, "end"))

    fin2(2)
    fin2(3)
    for b in range(pn.bits):
        pl.semaphore_signal(credit.at[6 + b], inc=1, device_id=place.over(b), device_id_type=MESH)
    mid(fc1_p[2])
    for b in range(pn.bits):
        pl.semaphore_wait(credit.at[6 + b], 1)
    qkv_blocks()
    mid(fc1_p[3])
    line_h.send(1, "mid")
    fin1(0)
    mid(qkv_p[0])
    line_h.send(2, "mid")
    mid(qkv_p[1])
    mid(qkv_p[2])
    fin1(1)
    fin1(2)
    fin1(3)
    fin_d()
    fin3(0)

    gcol = pl.ds(pl.multiple_of(t * BK, BK), BK)

    def tail(rows):
        dh = line_h.value(rows)
        normed = (pool[pn.xo, rows, :].astype(F32) - mi[0, rows, pl.ds(0, 1)]) * mi[0, rows, pl.ds(1, 1)]
        return dh, normed, dh * gain[:, gcol]

    def s_copy(k, f):
        src = stt.at[:, pl.ds(f * TW, TW)]
        return remote(src, sr.at[t, :, pl.ds(f * TW, TW)], s_s.at[k, f], r_s.at[t, f], (d, lax.rem(t + k, nt)))

    def tail_one(f):
        line_h.finish((f,))

        @pl.loop(0, TW // 64)
        def _(q):
            rows = pl.ds(pl.multiple_of(f * TW + q * 64, 64), 64)
            dh, normed, scaled = tail(rows)
            s1 = jnp.sum(scaled, axis=1, keepdims=True)
            s2 = jnp.sum(scaled * normed, axis=1, keepdims=True)
            stc[rows, :] = jnp.where(first, s1, s2)
            ng[pl.ds(0, 1), :] += jnp.sum(dh * normed, axis=0, keepdims=True)
            ng[pl.ds(1, 1), :] += jnp.sum(dh, axis=0, keepdims=True)

        half = pl.ds(f * TW, TW)
        stt[:, half] = stc[half, :].T[:8]
        sr[t, :, half] = stt[:, half]
        for k in range(1, nt):
            s_copy(k, f).start()

    def tail_two(f):
        half = pl.ds(f * TW, TW)
        for k in range(1, nt):
            s_copy(k, f).wait_send()
            frm = lax.rem(t + k, nt)
            remote(
                stt.at[:, half], sr.at[frm, :, half], s_s.at[k, f], r_s.at[frm, f], place.pair()
            ).wait_recv()
        tot = sr[0, :, half]
        for k in range(1, nt):
            tot = tot + sr[k, :, half]
        stc[half, :] = jnp.concatenate([tot / pn.width, jnp.zeros((LANES - 8, TW), F32)], axis=0).T

        @pl.loop(0, TW // 64)
        def _(q):
            rows = pl.ds(pl.multiple_of(f * TW + q * 64, 64), 64)
            dh, normed, scaled = tail(rows)
            v = mi[0, rows, pl.ds(1, 1)] * (scaled - stc[rows, pl.ds(0, 1)] - normed * stc[rows, pl.ds(1, 1)])
            keep = tab[0, rows, pl.ds(2 * LANES, 1)] >= 0.0
            input_grad[rows, :] = v + jnp.where(keep, pool[pn.co, rows, :].astype(F32), 0.0)

    tail_one(0)
    fin3(1)
    tail_one(1)

    def v_copy(k):
        peer = lax.rem(d + k, nd)
        return remote(sv.at[peer], rv.at[d], s_v.at[k], r_v.at[d], (peer, t))

    cw, hwd = BK // nd, 2 * hw // nd
    sv[...] = jnp.zeros_like(sv)
    for dd in range(nd):
        mine = c == dd % 2
        sv[dd, pl.ds(0, 1), pl.ds(0, ub)] = jnp.where(mine, fb[pl.ds(0, 1), pl.ds((dd // 2) * ub, ub)], 0.0)
        sv[dd, pl.ds(1, 2), pl.ds(0, cw)] = ng[pl.ds(0, 2), pl.ds(dd * cw, cw)]
        sv[dd, pl.ds(3, 1), pl.ds(0, cw)] = ob[pl.ds(0, 1), pl.ds(dd * cw, cw)]
        here = c == (dd * hwd) // hw
        src = pl.ds((dd * hwd) % hw, hwd)
        sv[dd, pl.ds(4, 1), pl.ds(0, hwd)] = jnp.where(here, bias3[0, pl.ds(0, 1), src], 0.0)
        sv[dd, pl.ds(5, 1), pl.ds(0, hwd)] = jnp.where(here, bias3[2, pl.ds(0, 1), src], 0.0)
        for core in range(2):
            sv[dd, pl.ds(6 + core, 1), :] = jnp.where(c == core, bias3[1, pl.ds(0, 1), :], 0.0)
    for k in range(1, nd):
        v_copy(k).start()
    rv[d] = sv[d]
    tail_two(0)
    fin3(2)
    for slot in range(nq + 3):
        send_pair(slot).wait()

        def put(ref, slot=slot):
            ref[pl.ds(0, rb), :] = fr[slot].astype(F32)

        stage_out(put, dst1(slot, 1 - c) if slot < nq else dst3(slot - nq, 1 - c))
    tail_two(1)
    line_h.sent()
    for k in range(1, nd):
        v_copy(k).wait_send()
        frm = lax.rem(d + k, nd)
        remote(sv.at[0], rv.at[frm], s_v.at[k], r_v.at[frm], place.pair()).wait_recv()
    res = rv[0]
    for k in range(1, nd):
        res = res + rv[k]
    fc1b_out[...] = res[0:1, :ub]
    norm_out[...] = res[1:3, :cw]
    outb_out[...] = jnp.concatenate([res[3:4, :cw], res[3:4, :cw]], axis=0)
    qvb_out[...] = res[4:6, :hwd]
    rk = ROT // nd
    turned = pltpu.roll(res, lax.rem(TW - d * rk, TW), 1)
    for core in range(2):
        for h in range(pn.heads):
            stc[pl.ds(core * pn.heads + h, 1), pl.ds(0, rk)] = turned[6 + core : 7 + core, h * HD : h * HD + rk]
    keyb_out[...] = stc[pl.ds(0, LANES), :].T[:rk, : 2 * pn.heads]
    for cp in os_used[-ostage.shape[0] :]:
        cp.wait()

def copy_kernel(n, *refs):
    src, dst, hold, sem = refs[:n], refs[n : 2 * n], refs[2 * n : 3 * n], refs[3 * n]

    def go(i, out):
        a, b = (hold[i], dst[i]) if out else (src[i], hold[i])
        return pltpu.make_async_copy(a, b, sem.at[int(out), i])

    for i in range(n):
        go(i, False).start()
    for i in range(n):
        go(i, False).wait()
        go(i, True).start()
    for i in range(n):
        go(i, True).wait()


def copied(arrays):
    n = len(arrays)
    shapes = [jax.ShapeDtypeStruct(a.shape, a.dtype) for a in arrays]
    return pl.pallas_call(
        functools.partial(copy_kernel, n),
        out_shape=shapes,
        in_specs=[pl.BlockSpec(memory_space=pl.ANY)] * n,
        out_specs=[pl.BlockSpec(memory_space=pl.ANY)] * n,
        scratch_shapes=[pltpu.VMEM(a.shape, a.dtype) for a in arrays] + [pltpu.SemaphoreType.DMA((2, n))],
        compiler_params=pltpu.CompilerParams(vmem_limit_bytes=VMEM_BYTES),
        name="results",
    )(*arrays)


def per_device(
    hidden_in,
    cotangent,
    segment_ids,
    positions,
    norm_gain,
    norm_shift,
    qkv_weight,
    qv_bias,
    key_bias,
    dense_weight,
    fc1_weight,
    fc1_bias,
    fc2_weight,
    out_bias,
):
    nd, nt = lax.axis_size("dp"), lax.axis_size("tensor")
    c = lax.rem(lax.axis_index("dp"), 2)
    nch = nd // 2
    rows, wl = hidden_in.shape
    width = wl * nt
    heads = key_bias.shape[0] // 2
    units = fc1_weight.shape[1] // 2
    ub = units // nch
    pn = Plan(nd, nt, units, heads, ub)
    hw, rb, rd, nq = pn.hw, pn.rb, pn.rd, units // TW
    assert rows == BK and wl == BK and nt == 4 and nq == 4 and hw == TW and rb == ub
    direct = ub == TW

    freq = 10000.0 ** (-(np.arange(LANES) % (ROT // 2)) * (2.0 / ROT))
    freq = jnp.asarray(freq.astype(np.float32)[None, :])

    def pick(w, axis):
        shape = w.shape
        w = w.reshape(*shape[:axis], nch, 2, ub, *shape[axis + 1 :])
        w = lax.dynamic_index_in_dim(w, c, axis + 1, keepdims=False)
        return w.reshape(*shape[:axis], units, *shape[axis + 1 :])

    w1, w2, b1 = fc1_weight, fc2_weight, fc1_bias
    if not direct:
        w1, w2, b1 = pick(w1, 1), pick(w2, 0), pick(b1, 0)
    w1 = w1.reshape(nt, BK, w1.shape[1])
    wq = qkv_weight.transpose(1, 0, 2)
    b1 = b1.reshape(1, -1)

    vm = pl.BlockSpec(memory_space=pltpu.VMEM)
    anyw = pl.BlockSpec(memory_space=pl.ANY)
    shapes = [
        ((rows, wl), BF16, vm),
        ((rows, wl), F32, vm),
        ((2, wl // nd), F32, vm),
        ((3, rb, 2 * hw), F32, anyw),
        ((2, 2 * hw // nd), F32, vm),
        ((ROT // nd, 2 * heads), F32, vm),
        ((rd, width), F32, anyw),
        ((rb, 2 * units), F32, anyw),
        ((1, ub), F32, vm),
        ((ub, width), F32, anyw),
        ((2, wl // nd), F32, vm),
    ]
    dma = pltpu.SemaphoreType.DMA
    nos = 4
    scratch = [
        pltpu.VMEM((pn.blocks, BK, BK), BF16),
        pltpu.VMEM((3, width, hw), BF16),
        pltpu.VMEM((hw, width), BF16),
        pltpu.VMEM((2, rows, 3 * LANES), F32),
        pltpu.VMEM((2, 8, rows), F32),
        pltpu.VMEM((2, rows, units), BF16),
        pltpu.VMEM((units, 2 * rows), BF16),
        pltpu.VMEM((2, rows, units), F32),
        pltpu.VMEM((3, 2, rows, hw), BF16),
        pltpu.VMEM((2, rows, hw), BF16),
        pltpu.VMEM((2, rows, hw), BF16),
        pltpu.VMEM((nch * rd, 2 * rows), BF16),
        pltpu.VMEM((hw, rows), BF16),
        pltpu.VMEM((nch * rd, width), BF16),
        pltpu.VMEM((nt, nch - 1, rd, BK), BF16),
        pltpu.VMEM((pn.n2 + pn.n1, nch - 1, rb, TW), BF16),
        pltpu.VMEM((nq + 3, rb, TW), BF16),
        pltpu.VMEM((nq + 3, rb, TW), BF16),
        pltpu.VMEM((nos, max(rb, rd), TW), F32),
        pltpu.VMEM((2, rows, LANES), F32),
        pltpu.VMEM((3, 8, hw), F32),
        pltpu.VMEM((8, units), F32),
        pltpu.VMEM((8, wl), F32),
        pltpu.VMEM((8, wl), F32),
        pltpu.VMEM((nd, 8, TW), F32),
        pltpu.VMEM((nd, 8, TW), F32),
        pltpu.VMEM((rows, LANES), F32),
        pltpu.VMEM((8, rows), F32),
        pltpu.VMEM((nt, 8, rows), F32),
        pltpu.VMEM((2, nt, 8, rows), F32),
        pltpu.VMEM((8, hw), F32),
        dma((10 + nq * (2 + nt),)),
        dma((2, 2, nt, 2)),
        dma((2, nt, 2)),
        dma((2, nt, 2)),
        dma((2, nt, 2)),
        dma((4,)),
        dma((pn.pieces, nch - 1)),
        dma((pn.pieces, nch - 1)),
        dma((2,)),
        dma((2,)),
        dma((2, nq + 3)),
        dma((nos,)),
        dma((2, 2)),
        dma((nt,)),
        dma((nt,)),
        dma((2, nt, 2)),
        dma((nt + 1, 2)),
        dma((nt,)),
        dma((nt,)),
        dma((2, nt, 2)),
        dma((nt + 1, 2)),
        dma((nd,)),
        dma((nd,)),
        dma((nt, 2)),
        dma((nt, 2)),
        dma((2, nt)),
        dma((2, nt)),
        pltpu.SemaphoreType.REGULAR((6 + pn.bits,)),
    ]
    res = pl.pallas_call(
        functools.partial(block_kernel, pn, direct),
        out_shape=[jax.ShapeDtypeStruct(s, dt) for s, dt, _ in shapes],
        in_specs=[anyw, anyw, vm, vm, vm, vm, vm, anyw, anyw, anyw, anyw, vm, vm, vm, vm],
        out_specs=[sp for _, _, sp in shapes],
        scratch_shapes=scratch,
        compiler_params=pltpu.CompilerParams(
            collective_id=0, has_side_effects=True, vmem_limit_bytes=VMEM_BYTES
        ),
        name="block",
    )(
        hidden_in, cotangent, segment_ids.reshape(1, rows), positions.reshape(1, rows), freq, norm_gain.reshape(1, width), norm_shift.reshape(1, width),
        w1, w2, wq, dense_weight, b1, qv_bias, key_bias, out_bias,
    )
    res = list(copied(res))
    res[3] = res[3].transpose(1, 0, 2)
    res[5] = res[5].T
    if not direct:
        res[7] = res[7].reshape(rb, 2, nch, ub).transpose(0, 2, 1, 3).reshape(rb, 2 * units)
    res[8] = res[8].reshape(ub)
    return tuple(res)


def solution(mesh):
    placed = (
        P("dp", "tensor"),
        P("dp", "tensor"),
        P("dp"),
        P("dp"),
        P(),
        P(),
        P(None, None, "tensor"),
        P(None, "tensor"),
        P("tensor", None),
        P("tensor", None),
        P(None, "tensor"),
        P("tensor"),
        P("tensor", None),
        P(),
    )
    return jax.shard_map(
        per_device,
        mesh=mesh,
        in_specs=placed,
        out_specs=(
            P("dp", "tensor"),
            P("dp", "tensor"),
            P(None, ("tensor", "dp")),
            P("dp", None, "tensor"),
            P(None, ("tensor", "dp")),
            P("tensor", "dp"),
            P(("tensor", "dp"), None),
            P("dp", "tensor"),
            P(("tensor", "dp")),
            P(("tensor", "dp"), None),
            P(None, ("tensor", "dp")),
        ),
        check_vma=False,
    )
```

```python
import functools
import math

import jax
import jax.numpy as jnp
import numpy as np
from jax import lax
from jax.experimental import pallas as pl
from jax.experimental.pallas import tpu as pltpu
from jax.sharding import PartitionSpec as P

HD = 64
ROT = 32
LANES = 128

norm_epsilon = 1e-05
gelu_scale = 0.7978845608028654
gelu_cubic = 0.044715
masked_score = -1e30

MESH = pl.DeviceIdType.MESH
F32 = jnp.float32
BF16 = jnp.bfloat16
VMEM_BYTES = 67043328


def gelu_tanh(u):
    return jnp.tanh(u * (gelu_scale + (gelu_scale * gelu_cubic) * (u * u)))


def gelu_slope(u):
    tanh_val = gelu_tanh(u)
    return 0.5 * (1.0 + tanh_val) + (0.5 * u) * (1.0 - tanh_val * tanh_val) * (
        gelu_scale + (3.0 * gelu_scale * gelu_cubic) * (u * u)
    )


class Place:
    def __init__(self, nd, nt):
        self.nd, self.nt = nd, nt
        self.nch = nd // 2
        self.bits = self.nch.bit_length() - 1
        self.d = lax.axis_index("dp")
        self.t = lax.axis_index("tensor")
        self.c = lax.rem(self.d, 2)
        self.j = self.d // 2

    def pair(self):
        return (self.d + 1 - 2 * self.c, self.t)

    def chip_bit(self, b):
        return lax.rem(self.j // (1 << b), 2)

    def over(self, b):
        step = 2 << b
        return (self.d + step - 2 * step * self.chip_bit(b), self.t)

    def right(self):
        return (self.d, jnp.minimum(self.t + 1, self.nt - 1))

    def left(self):
        return (self.d, jnp.maximum(self.t - 1, 0))


def remote(src, dst, send, recv, device):
    return pltpu.make_async_remote_copy(
        src_ref=src, dst_ref=dst, send_sem=send, recv_sem=recv, device_id=device, device_id_type=MESH
    )


def greet(place):
    barrier = pltpu.get_barrier_semaphore()

    def signal(d, t):
        pl.semaphore_signal(barrier, inc=1, device_id=(d, t), device_id_type=MESH)

    for k in range(1, place.nd):
        signal(lax.rem(place.d + k, place.nd), place.t)
    for k in range(1, place.nt):
        signal(place.d, lax.rem(place.t + k, place.nt))
        signal(place.pair()[0], lax.rem(place.t + k, place.nt))


def greeted(place):
    pl.semaphore_wait(pltpu.get_barrier_semaphore(), place.nd - 1 + 2 * (place.nt - 1))


BK = 512
TW = 256


def mm(a, b, ca=1, cb=0):
    return lax.dot_general(a, b, (((ca,), (cb,)), ((), ())), preferred_element_type=F32)


def cat(parts, axis):
    return jnp.concatenate(parts, axis=axis)


def at512(i):
    return pl.ds(pl.multiple_of(i * BK, BK), BK)


def at256(i):
    return pl.ds(pl.multiple_of(i * TW, TW), TW)


class Plan:
    def __init__(self, nd, nt, units, heads, ub):
        self.nd, self.nt = nd, nt
        self.nch = nd // 2
        self.bits = self.nch.bit_length() - 1
        self.units, self.heads, self.ub = units, heads, ub
        self.hw = heads * HD
        self.nu = units // BK
        self.width = nt * BK
        self.rb = self.width // nd
        self.rd = 2 * self.hw // nd
        n = 0
        for name, size in (
            ("xb", 2 * nt),
            ("cb", 2 * nt),
            ("hb", 2 * nt),
            ("w1b", 2 * nt + 1),
            ("w2b", 2 * nt + 1),
            ("f2b", self.nu * nt),
            ("f1b", self.nu * nt),
            ("xo", 1),
            ("co", 1),
        ):
            setattr(self, name, n)
            n += size
        self.blocks = n
        self.n2 = 2 * nt
        self.n1 = 2 * (units // TW)
        self.n3 = 2 * 3
        self.pieces = self.n2 + self.n1 + self.n3 + nt


class Piece:
    def __init__(self, place, order, view, recv, ss, rs):
        self.p, self.order, self.view, self.r, self.ss, self.rs = place, order, view, recv, ss, rs
        self.off = [0]
        for i in range(len(order)):
            self.off.append(self.off[-1] + (place.nch >> (i + 1)))

    def block(self, i, m, mine):
        j = 0
        for b in self.order[:i]:
            j = j + self.p.chip_bit(b) * (1 << b)
        if i < len(self.order):
            b = self.order[i]
            v = self.p.chip_bit(b)
            j = j + (v if mine else 1 - v) * (1 << b)
            for q, b2 in enumerate(self.order[i + 1 :]):
                j = j + ((m >> q) & 1) * (1 << b2)
        return j

    def held(self, i, m, before):
        idx = 0
        for r in range(before + 1, min(i, len(self.order))):
            idx = idx + self.p.chip_bit(self.order[r]) * (1 << (r - before - 1))
        if i < len(self.order):
            v = self.p.chip_bit(self.order[i])
            idx = idx + (1 - v) * (1 << (i - before - 1)) + m * (1 << (i - before))
        return self.off[before] + idx

    def copy(self, i, m):
        k = self.off[i] + m
        return remote(
            self.view(self.block(i, m, False)),
            self.r.at[k],
            self.ss.at[k],
            self.rs.at[k],
            self.p.over(self.order[i]),
        )

    def total(self, i, m, rows):
        acc = self.view(self.block(i, m, False))[rows, :].astype(F32)
        for before in range(i):
            acc = acc + self.r[self.held(i, m, before), rows, :].astype(F32)
        return acc

    def each(self, do):
        rows = self.view(0).shape[0]
        size = min(rows, 64)

        @pl.loop(0, rows // size)
        def _(q):
            do(pl.ds(pl.multiple_of(q * size, size), size))

    def start(self, i):
        for m in range(self.p.nch >> (i + 1)):
            if i > 0:
                dst = self.view(self.block(i, m, False))

                def put(rows, dst=dst, m=m):
                    dst[rows, :] = self.total(i, m, rows).astype(BF16)

                self.each(put)
            self.copy(i, m).start()

    def wait(self, i):
        for m in range(self.p.nch >> (i + 1)):
            self.copy(i, m).wait()

    def final(self, to):
        def put(rows):
            to[rows, :] = self.total(len(self.order), 0, rows).astype(to.dtype)

        self.each(put)


def block_kernel(pn, direct, *refs):
    (
        x_in, c_in, seg_in, pos_in, freq, gain, shift, w1, w2, wq, wd, b1, qvb, kb, obias,
        block_out, input_grad, norm_out, qkv_out, qvb_out, keyb_out, dense_out, fc1_out, fc1b_out,
        fc2_out, outb_out, other_out,
        pool, wq_v, wd_v, tab, segr, act, buf, pre_v, qkv, attn, attn_p, dl, at_tmp, dg, dr, rp, fs, fr,
        ostage, mi, bias3, fb, ob, ng, sv, rv, stc, stt, sr, st, kbv, stk,
        s_load, s_z, r_z, s_c, r_c, s_tab, s_p, r_p, s_d, r_d, s_f, s_os, s_a, s_oc, r_oc, s_ol, r_ol,
        s_hc, r_hc, s_hl, r_hl, s_v, r_v, s_s, r_s, s_st, r_st, credit,
    ) = refs
    nd, nt, nch, nu = pn.nd, pn.nt, pn.nch, pn.nu
    hw, ub, rb, rd = pn.hw, pn.ub, pn.rb, pn.rd
    place = Place(nd, nt)
    t, c, d = place.t, place.c, place.d
    nq = pn.units // TW

    def load(i, src, dst):
        return pltpu.make_async_copy(src, dst, s_load.at[i])

    loads = {
        "x": [load(0, x_in, pool.at[pn.xb + t])],
        "c": [load(1, c_in, pool.at[pn.cb + t])],
        "wd": [load(4, wd.at[pl.ds(pl.multiple_of(c * hw, hw), hw), :], wd_v)],
        "wq": [
            load(5, wq.at[:, :, pl.ds(pl.multiple_of(c * hw, hw), hw)], wq_v)
        ],
        "xo": [load(8, x_in, pool.at[pn.xo]), load(9, c_in, pool.at[pn.co])],
        "w1": [],
        "w2": [],
        "w1r": [],
    }
    n = 10
    for q in range(nq):
        col = (2 * q + c if direct else q) * TW
        src = w1.at[:, :, pl.ds(pl.multiple_of(col, TW), TW)]
        half = pl.ds((q % 2) * TW, TW)
        loads["w1"].append(load(n, src, pool.at[pl.ds(pn.w1b + (q // 2) * nt, nt), :, half]))
        loads["w1r"].append(load(n + 1, src, pool.at[pl.ds(pn.cb + (q // 2) * nt, nt), :, half]))
        n += 2
        for k in range(nt):
            src = w2.at[pl.ds(pl.multiple_of(col, TW), TW), pl.ds(k * BK, BK)]
            loads["w2"].append(load(n, src, pool.at[pn.w2b + (q // 2) * nt + k, half, :]))
            n += 1

    def begin(*names):
        for name in names:
            for cp in loads[name]:
                cp.start()

    def arrive(*names):
        for name in names:
            for cp in loads[name]:
                cp.wait()

    begin("x")
    greet(place)
    arrive("x")

    first = lax.broadcasted_iota(jnp.int32, (64, LANES), 1) == 0

    @pl.loop(0, BK // 64)
    def _(q):
        rows = pl.ds(pl.multiple_of(q * 64, 64), 64)
        v = pool[pn.xb + t, rows, :].astype(F32)
        m = jnp.sum(v, axis=1, keepdims=True) / BK
        v = v - m
        stc[rows, :] = jnp.where(first, m, jnp.sum(v * v, axis=1, keepdims=True))

    for j in range(4):
        turned = stc[pl.ds(j * LANES, LANES), :].T
        stk[pl.ds(j, 1), :] = turned[0:1]
        stk[pl.ds(4 + j, 1), :] = turned[1:2]

    greeted(place)

    def blk(a, s, k, f):
        return pool.at[a * (pn.cb - pn.xb) + pn.xb + s * nt + k, at256(f), :]

    def z_dev(side):
        return place.right() if side == 0 else place.left()

    def z_copy(a, k, side, f):
        return remote(blk(a, 0, k, f), blk(a, 0, k, f), s_z.at[side, a, k, f], r_z.at[a, k, f], z_dev(side))

    def c_copy(a, k, f):
        return remote(blk(a, 0, k, f), blk(a, 1, k, f), s_c.at[a, k, f], r_c.at[a, k, f], place.pair())

    def own_z(a, side, f):
        src = (x_in, c_in)[a].at[at256(f), :]
        return remote(src, blk(a, 0, t, f), s_z.at[side, a, t, f], r_z.at[a, t, f], z_dev(side))

    def own_c(a, f):
        src = (x_in, c_in)[a].at[at256(f), :]
        return remote(src, blk(a, 1, t, f), s_c.at[a, t, f], r_c.at[a, t, f], place.pair())

    def tab_copies():
        return (
            remote(tab.at[0], tab.at[1], s_tab.at[0], s_tab.at[1], place.pair()),
            remote(segr.at[0], segr.at[1], s_tab.at[2], s_tab.at[3], place.pair()),
        )

    def item(side, who, i):
        if side == 0:
            first = i <= who
            return jnp.where(first, 0, 1), jnp.where(first, who - i, 2 * who + 1 - i)
        m = nt - who
        first = i < m
        return jnp.where(first, 0, 1), jnp.where(first, who + i, who + i - m)

    def progress(step, halves=(0, 1)):
        for f in halves:
            if step >= 1:
                @pl.when((t > 0) & (step - 1 < 2 * t))
                def _():
                    a, k = item(0, t - 1, step - 1)
                    z_copy(a, k, 0, f).wait_recv()
                    c_copy(a, k, f).start()

                @pl.when((t < nt - 1) & (step - 1 < 2 * (nt - 1 - t)))
                def _():
                    a, k = item(1, t + 1, step - 1)
                    z_copy(a, k, 1, f).wait_recv()
                    c_copy(a, k, f).start()

            for side in range(2):
                me = t if side == 0 else nt - 1 - t
                if step == 0:
                    pl.when(me < nt - 1)(lambda side=side: own_z(0, side, f).start())
                else:
                    @pl.when((me < nt - 1) & (step <= me))
                    def _():
                        z_copy(0, me - step if side == 0 else nt - 1 - me + step, side, f).start()

                @pl.when((me < nt - 1) & (step > me) & (step <= 2 * me))
                def _():
                    k = 2 * me - step
                    z_copy(1, k if side == 0 else nt - 1 - k, side, f).start()

        for side in range(2 if 1 in halves else 0):
            me = t if side == 0 else nt - 1 - t

            @pl.when((me < nt - 1) & (step == me))
            def _():
                own_z(1, side, 0).start()
                own_z(1, side, 1).start()

    def z_sent(a):
        for f in range(2):
            for m in range(nt):
                for side in range(2):
                    me = t if side == 0 else nt - 1 - t

                    @pl.when((me < nt - 1) & (m <= me))
                    def _():
                        k = me - m
                        z_copy(a, k if side == 0 else nt - 1 - k, side, f).wait_send()

            for k in range(nt):
                c_copy(a, k, f).wait_send()

    def arrival(tt, k):
        if k == tt:
            return -1
        return 2 * tt - 1 - k if k < tt else (nt - 1 - tt) + (k - tt - 1)

    orders = [sorted(range(nt), key=lambda k, tt=tt: (arrival(tt, k), k)) for tt in range(nt)]
    needed = [max(arrival(tt, orders[tt][i]) for tt in range(nt)) + 1 for i in range(nt)]

    def chunk(i):
        k = orders[0][i]
        for tt in range(1, nt):
            k = jnp.where(t == tt, orders[tt][i], k)
        return k

    def st_copy(s, k):
        peer = lax.rem(t + k, nt)
        dev = (d, peer) if s == 0 else (place.pair()[0], peer)
        return remote(stk, st.at[s, t], s_st.at[s, k], r_st.at[s, t], dev)

    for k in range(nt):
        for s in range(2):
            if k or s:
                st_copy(s, k).start()
    progress(0)
    for f in range(2):
        own_c(0, f).start()
    st[0, t] = stk[...]
    begin("w1", "c")

    def column(row):
        return jnp.broadcast_to(row.astype(F32), (LANES, BK)).T

    lane1 = lax.broadcasted_iota(jnp.int32, (1, LANES), 1)
    dim1 = lax.rem(lane1, HD)
    angles = column(pos_in[...]) * freq[...]
    tab[0, :, pl.ds(0, LANES)] = jnp.where(dim1 < ROT, jnp.cos(angles), 1.0)
    sine = jnp.sin(angles)
    sine = jnp.where(dim1 < ROT // 2, -sine, sine)
    tab[0, :, pl.ds(LANES, LANES)] = jnp.where(dim1 < ROT, sine, 0.0)
    tab[0, :, pl.ds(2 * LANES, LANES)] = column(seg_in[...])
    segr[0] = jnp.broadcast_to(seg_in[...].astype(F32), (8, BK))
    kbv[...] = jnp.zeros_like(kbv)
    for h in range(pn.heads):
        kbv[pl.ds(0, 1), pl.ds(h * HD, ROT)] = kb[pl.ds(c * pn.heads + h, 1), :]
    arrive("c")
    for f in range(2):
        own_c(1, f).start()
    for cp in tab_copies():
        cp.start()
    fb[...] = jnp.zeros_like(fb)
    bias3[...] = jnp.zeros_like(bias3)
    ng[...] = jnp.zeros_like(ng)
    for k in range(nt):
        for s in range(2):
            if k or s:
                frm = lax.rem(t + k, nt)
                st_copy(s, k).wait_send()
                remote(stk, st.at[s, frm], s_st.at[s, k], r_st.at[s, frm], place.pair()).wait_recv()
    for s in range(2):
        mean = sum(st[s, k, pl.ds(0, 4), :] for k in range(nt)) / nt
        dev = 0.0
        for k in range(nt):
            off = st[s, k, pl.ds(0, 4), :] - mean
            dev = dev + st[s, k, pl.ds(4, 4), :] + BK * off * off
        inv = lax.rsqrt(dev / pn.width + norm_epsilon)
        for j in range(4):
            both = cat([mean[j : j + 1], inv[j : j + 1], jnp.zeros((LANES - 2, LANES), F32)], 0)
            mi[s, pl.ds(j * LANES, LANES), :] = both.T
    arrive("w1")

    def live(s):
        return tab[s, :, pl.ds(2 * LANES, 1)] >= 0.0

    def gelu_block(s, u, pre):
        bias = []
        for q in range(2):
            col = (2 * (2 * u + q) + c if direct else 2 * u + q) * TW
            bias.append(b1[:, pl.ds(pl.multiple_of(col, TW), TW)])
        pre = pre + cat(bias, 1)
        val = (0.5 * pre * (1.0 + gelu_tanh(pre))).astype(BF16)
        act[s, :, at512(u)] = val
        val = jnp.where(live(s), val, jnp.zeros_like(val))
        buf[at512(u), at512(s)] = val.T

    def take(k, start, last=False):
        cols = pl.ds(pl.multiple_of(k * BK, BK), BK)

        @pl.loop(0, 2)
        def _(s):
            @pl.when(s == 1)
            def _():
                for f in range(2):
                    c_copy(0, k, f).wait_recv()

            @pl.loop(0, BK // 64)
            def _(q):
                rows = pl.ds(pl.multiple_of(q * 64, 64), 64)
                v = pool[pn.xb + s * nt + k, rows, :].astype(F32)
                v = (v - mi[s, rows, pl.ds(0, 1)]) * mi[s, rows, pl.ds(1, 1)]
                pool[pn.hb + s * nt + k, rows, :] = (v * gain[:, cols] + shift[:, cols]).astype(BF16)

            @pl.loop(0, nu)
            def _(u):
                out = mm(pool[pn.hb + s * nt + k], pool[pn.w1b + u * nt + k])
                if not start:
                    out = out + pre_v[s, :, at512(u)]
                pre_v[s, :, at512(u)] = out
                if last:
                    gelu_block(s, u, out)

    take(t, True)
    begin("wq", "wd", "w2", "xo")
    progress(1)
    pl.when(t >= 1)(lambda: take(t - 1, False))
    progress(2, (0,))
    pl.when(t + 1 < nt)(lambda: take(t + 1, False))
    progress(2, (1,))
    take(jnp.where(t >= 2, t - 2, t + 2), False)
    progress(3)
    for cp in tab_copies():
        cp.wait()

    @pl.when((t == 0) | (t == nt - 1))
    def _():
        take(nt - 1 - t, False, True)

    @pl.when((t > 0) & (t < nt - 1))
    def _():
        @pl.loop(0, 2 * nu)
        def _(i):
            s, u = i // nu, lax.rem(i, nu)
            gelu_block(s, u, pre_v[s, :, at512(u)])


    def biased(s, q):
        col = (2 * q + c if direct else q) * TW
        return pre_v[s, :, at256(q)] + b1[:, pl.ds(pl.multiple_of(col, TW), TW)]

    def tell(i):
        def signal(n, device):
            pl.semaphore_signal(credit.at[3 * i + n], inc=1, device_id=device, device_id_type=MESH)

        signal(0, place.pair())
        pl.when(t > 0)(lambda: signal(2, place.left()))
        pl.when(t < nt - 1)(lambda: signal(1, place.right()))

    def told(i):
        pl.semaphore_wait(credit.at[3 * i], 1)
        pl.when(t > 0)(lambda: pl.semaphore_wait(credit.at[3 * i + 1], 1))
        pl.when(t < nt - 1)(lambda: pl.semaphore_wait(credit.at[3 * i + 2], 1))

    tell(0)

    orders_ab = [list(range(pn.bits)), list(range(pn.bits))[::-1]]

    def piece(index, half, view, recv):
        return Piece(place, orders_ab[half], view, recv, s_p.at[index], r_p.at[index])

    per2 = BK // ub

    def view2(i, h):
        def view(j):
            return pool.at[
                pn.f2b + nu * i + j // per2,
                pl.ds(pl.multiple_of(lax.rem(j, per2) * ub, ub), ub),
                pl.ds(h * TW, TW),
            ]

        return view

    def view1(q, h):
        def view(j):
            r = 2 * j * rb + h * rb
            return pool.at[
                pn.f1b + nu * (r // BK) + q // 2,
                pl.ds(pl.multiple_of(lax.rem(r, BK), rb), rb),
                pl.ds((q % 2) * TW, TW),
            ]

        return view

    def view3(i, h):
        def view(j):
            r = 2 * j * rb + h * rb
            if i < 2:
                b, col = pn.f2b + r // BK, i * TW
            else:
                b, col = pn.f2b + nt + r // (2 * BK), pl.multiple_of(lax.rem(r // BK, 2) * TW, TW)
            return pool.at[b, pl.ds(pl.multiple_of(lax.rem(r, BK), rb), rb), pl.ds(col, TW)]

        return view

    def view_d(i):
        def view(j):
            return dg.at[pl.ds(pl.multiple_of(j * rd, rd), rd), pl.ds(i * BK, BK)]

        return view

    fc2_p = [[piece(2 * i + h, h, view2(i, h), rp.at[2 * i + h]) for h in range(2)] for i in range(nt)]
    fc1_p = [
        [piece(pn.n2 + 2 * q + h, h, view1(q, h), rp.at[pn.n2 + 2 * q + h]) for h in range(2)]
        for q in range(nq)
    ]
    qkv_p = [
        [piece(pn.n2 + pn.n1 + 2 * i + h, h, view3(i, h), rp.at[2 * i + h]) for h in range(2)]
        for i in range(3)
    ]
    den_p = [piece(pn.n2 + pn.n1 + pn.n3 + i, i % 2, view_d(i), dr.at[i]) for i in range(nt)]

    os_used = []

    def stage_out(value_to, dst):
        n = len(os_used)
        slot = n % ostage.shape[0]
        if n >= ostage.shape[0]:
            os_used[n - ostage.shape[0]].wait()
        value_to(ostage.at[slot])
        cp = pltpu.make_async_copy(ostage.at[slot, pl.ds(0, dst.shape[0]), :], dst, s_os.at[slot])
        cp.start()
        os_used.append(cp)

    def fin2(i):
        for h in range(2):
            p = fc2_p[i][h]
            p.wait(pn.bits - 1)

            def put(ref, p=p):
                p.final(ref)

            col = chunk(i) * BK + h * TW
            stage_out(put, fc2_out.at[:, pl.ds(pl.multiple_of(col, TW), TW)])

    def send_pair(slot):
        return remote(fs.at[slot], fr.at[slot], s_f.at[0, slot], s_f.at[1, slot], place.pair())

    def fin_pair(pieces, slot, dst):
        for h in range(2):
            pieces[h].wait(pn.bits - 1)

        def put(ref):
            for h in range(2):
                @pl.when(c == h)
                def _():
                    pieces[h].final(ref)

                @pl.when(c != h)
                def _():
                    pieces[h].final(fs.at[slot])

        stage_out(put, dst)
        send_pair(slot).start()

    def dst1(q):
        return fc1_out.at[:, pl.ds(q * TW, TW)]

    def dst3(i):
        return qkv_out.at[i]

    def fin1(q):
        fin_pair(fc1_p[q], q, dst1(q))

    def fin3(i):
        fin_pair(qkv_p[i], nq + i, dst3(i))

    def fin_d():
        for i in range(nt):
            p = den_p[i]
            p.wait(pn.bits - 1)
            for h in range(2):

                def put(ref, p=p, i=i, h=h):
                    half = pl.ds(h * TW, TW)
                    me = p.block(len(p.order), 0, True)
                    acc = dg[pl.ds(pl.multiple_of(me * rd, rd), rd), pl.ds(i * BK + h * TW, TW)].astype(F32)
                    for before in range(len(p.order)):
                        acc = acc + p.r[p.held(len(p.order), 0, before), :, half].astype(F32)
                    ref[pl.ds(0, rd), :] = acc

                col = chunk(i) * BK + h * TW
                stage_out(put, dense_out.at[:, pl.ds(pl.multiple_of(col, TW), TW)])

    def mids(pieces, i):
        for p in pieces:
            p.wait(i - 1)
            p.start(i)

    def mid(pieces):
        for i in range(1, pn.bits):
            mids(pieces, i)

    def fc2_chunk(i):
        k = chunk(i)
        for f in range(2):
            c_copy(1, k, f).wait_recv()
        for h in range(2):

            half = pl.ds(h * TW, TW)
            out = mm(buf[...], cat([pool[pn.cb + k, :, half], pool[pn.cb + nt + k, :, half]], 0)).astype(BF16)
            for u in range(nu):
                pool[pn.f2b + nu * i + u, :, half] = out[u * BK : (u + 1) * BK]
            fc2_p[i][h].start(0)

    done_steps = [nt - 1]

    def upto(step):
        while done_steps[0] < min(step, 2 * nt - 2):
            done_steps[0] += 1
            progress(done_steps[0])

    fc2_chunk(0)

    arrive("wq")
    lane = lax.broadcasted_iota(jnp.int32, (BK, TW), 1)
    low = lax.rem(lane, ROT) < ROT // 2

    def swap(v):
        return jnp.where(low, pltpu.roll(v, TW - ROT // 2, 1), pltpu.roll(v, ROT // 2, 1))

    def table(s, i):
        v = tab[s, :, pl.ds(i * LANES, LANES)]
        return jnp.concatenate([v, v], axis=1)

    @pl.loop(0, 2)
    def _(s):
        all_v = mm(cat([pool[pn.hb + s * nt + k] for k in range(nt)], 1), cat([wq_v[i] for i in range(3)], 1))
        for i in range(3):
            v = all_v[:, i * hw : (i + 1) * hw]
            cols = pl.ds(pl.multiple_of(c * hw, hw), hw)
            if i == 1:
                v = v + kbv[pl.ds(0, 1), :]
            else:
                v = v + qvb[pl.ds(i // 2, 1), cols]
            if i < 2:
                v = v * table(s, 0) + swap(v) * table(s, 1)
            qkv[i, s] = v.astype(BF16)

    upto(needed[1])
    fc2_chunk(1)
    z_sent(0)

    @pl.loop(0, 2 * nt)
    def _(i):
        for h in range(2):
            pool[pn.xb + i, :, pl.ds(h * TW, TW)] = pool[pn.hb + i, pl.ds(h * TW, TW), :].T


    mid(fc2_p[0])

    heads2 = [lane1 < HD, lane1 >= HD]
    score_scale = HD ** (-0.5)

    def only(v, h):
        return jnp.where(heads2[h], v, jnp.zeros_like(v))

    def bias_of(s, qt):
        nk = (qt + 1) * TW
        col = lax.broadcasted_iota(jnp.int32, (TW, nk), 1)
        row = lax.broadcasted_iota(jnp.int32, (TW, nk), 0) + qt * TW
        same = tab[s, pl.ds(qt * TW, TW), pl.ds(2 * LANES, 1)] == segr[s, pl.ds(0, 1), pl.ds(0, nk)]
        return jnp.where(same & (col <= row), 0.0, masked_score)

    def probs(qh, keys, bias):
        sc = mm(qh, keys, 1, 1) * score_scale + bias
        top = jnp.max(sc, axis=1, keepdims=True)
        ex = jnp.exp(sc - top)
        return ex * (1.0 / jnp.sum(ex, axis=1, keepdims=True))

    npair = hw // LANES

    def attention(s):
        @pl.loop(0, npair)
        def _(hp):
            cols = pl.ds(pl.multiple_of(hp * LANES, LANES), LANES)
            for qt in range(2):
                rows, kr = pl.ds(qt * TW, TW), pl.ds(0, (qt + 1) * TW)
                bias = bias_of(s, qt)
                out = []
                for h in range(2):
                    pb = probs(only(qkv[0, s, rows, cols], h), qkv[1, s, kr, cols], bias).astype(BF16)
                    out.append(mm(pb, qkv[2, s, kr, cols]))
                attn[s, rows, cols] = jnp.where(heads2[0], out[0], out[1]).astype(BF16)

    def attn_copy(s):
        return remote(attn.at[s], attn_p.at[1 - s], s_a.at[0, s], s_a.at[1, s], place.pair())

    attention(0)
    attn_copy(0).start()
    upto(needed[2])
    fc2_chunk(2)
    mid(fc2_p[1])
    attention(1)
    attn_copy(1).start()
    arrive("wd", "w2")

    class Line:
        def __init__(self, part, pr, rbase, sp, rp_, sl, rl):
            self.part, self.pr, self.rbase, self.sp, self.rp, self.sl, self.rl = part, pr, rbase, sp, rp_, sl, rl

        def pair(self, k):
            return remote(
                pool.at[self.part + nt + k], pool.at[self.pr + k], self.sp.at[k], self.rp.at[k], place.pair()
            )

        def copy(self, side, k, f, dev):
            slot = k if side == 0 else jnp.where(k == t - 1, nt, k)
            return remote(
                pool.at[self.part + k, at256(f), :],
                pool.at[self.rbase + slot, at256(f), :],
                self.sl.at[side, k, f],
                self.rl.at[slot, f],
                dev,
            )

        def got(self, slot, f):
            remote(
                pool.at[self.part, at256(f), :],
                pool.at[self.rbase + slot, at256(f), :],
                self.sl.at[0, 0, f],
                self.rl.at[slot, f],
                place.pair(),
            ).wait_recv()

        def each(self, side, step, do, which="all"):
            me = t if side == 0 else nt - 1 - t
            here = {"all": me <= step, "end": me == 0, "far": (me > 1) & (me <= step), "near": me == 1}[which]

            @pl.when(here & (me < nt - 1))
            def _():
                k = nt - 1 - step + me
                do(k if side == 0 else nt - 1 - k)

        def send(self, step, which):
            for side in range(2):

                def do(k, side=side):
                    for f in range(2):
                        if which != "end":
                            self.got(k, f)

                        @pl.loop(0, TW // 64)
                        def _(q):
                            rows = pl.ds(pl.multiple_of(f * TW + q * 64, 64), 64)
                            v = pool[self.part + k, rows, :].astype(F32) + pool[self.pr + k, rows, :].astype(F32)
                            if which != "end":
                                v = v + pool[self.rbase + k, rows, :].astype(F32)
                            pool[self.part + k, rows, :] = v.astype(BF16)

                        self.copy(side, k, f, z_dev(side)).start()

                self.each(side, step, do, which)

        def sent(self):
            for side in range(2):
                for step in range(nt - 1):
                    for f in range(2):
                        self.each(
                            side, step, lambda k, side=side, f=f: self.copy(side, k, f, place.pair()).wait_send()
                        )

        def finish(self, halves=(0, 1)):
            for f in halves:
                pl.when(t > 0)(lambda: self.got(t, f))
                pl.when(t < nt - 1)(lambda: self.got(nt, f))

        def value(self, rows):
            v = pool[self.part + t, rows, :].astype(F32) + pool[self.pr + t, rows, :].astype(F32)
            v = v + jnp.where(t > 0, pool[self.rbase + t, rows, :].astype(F32), 0.0)
            return v + jnp.where(t < nt - 1, pool[self.rbase + nt, rows, :].astype(F32), 0.0)

    line_o = Line(pn.hb, pn.w1b, pn.w1b + nt, s_oc, r_oc, s_ol, r_ol)
    line_h = Line(pn.hb, pn.w2b, pn.w2b + nt, s_hc, r_hc, s_hl, r_hl)
    def out_rows(s):
        @pl.loop(0, nt)
        def _(k):
            rhs = cat([wd_v[:, at512(k)]] + [pool[pn.w2b + u * nt + k] for u in range(nu)], 0)
            pool[pn.hb + s * nt + k] = mm(cat([attn[s], act[s]], 1), rhs).astype(BF16)

    out_rows(1)
    told(0)
    for k in range(nt):
        line_o.pair(k).start()

    for s in range(2):
        attn_copy(s).wait()
    for core in range(2):
        for s in range(2):
            mine = attn if core == 0 else attn_p
            v = jnp.where(live(s), mine[s], jnp.zeros((BK, hw), BF16))
            at_tmp[...] = v.T
            who = c if core == 0 else 1 - c
            for j in range(nch // 2):
                off = lax.rem((2 * j + c) * rd, hw)
                dst = (who * (nch // 2) + j) * rd
                dl[pl.ds(pl.multiple_of(dst, rd), rd), pl.ds(s * BK, BK)] = at_tmp[
                    pl.ds(pl.multiple_of(off, rd), rd), :
                ]

    def dense_chunk(i):
        k = chunk(i)
        out = mm(dl[...], cat([pool[pn.cb + k], pool[pn.cb + nt + k]], 0))
        dg[:, pl.ds(i * BK, BK)] = out.astype(BF16)
        den_p[i].start(0)

    mid(fc2_p[2])
    for i in range(nt - 1):
        dense_chunk(i)
    out_rows(0)
    upto(needed[3])
    for k in range(nt):
        line_o.pair(k).wait()
    @pl.loop(0, nt - 1)
    def _(step):
        line_o.send(step, "end")

    fc2_chunk(3)
    dense_chunk(3)

    def dpre_block(u):
        @pl.loop(0, 2)
        def _(s):
            v = mm(
                cat([pool[pn.cb + s * nt + k] for k in range(nt)], 1),
                cat([pool[pn.w2b + u * nt + k] for k in range(nt)], 1),
                1,
                1,
            )
            for h in range(2):
                q = 2 * u + h
                w = v[:, h * TW : (h + 1) * TW]
                w = jnp.where(live(s), w * gelu_slope(biased(s, q)), 0.0)
                buf[pl.ds(pl.multiple_of(s * BK, BK), BK), pl.ds(q * TW, TW)] = w.astype(BF16)
                fb[pl.ds(0, 1), pl.ds(q * TW, TW)] += jnp.sum(w, axis=0, keepdims=True)

    def fc1_block(u):
        @pl.loop(0, nt)
        def _(k):
            out = mm(cat([pool[pn.xb + k], pool[pn.xb + nt + k]], 1), buf[:, pl.ds(u * BK, BK)])
            pool[pn.f1b + nu * k + u] = out.astype(BF16)

        for q in (2 * u, 2 * u + 1):
            for p in fc1_p[q]:
                p.start(0)

    dpre_block(0)
    fc1_block(0)
    dpre_block(1)
    tell(1)
    fc1_block(1)
    line_o.send(1, "near")
    mid(fc2_p[3])
    mid(den_p)

    def dcols(i):
        return pl.ds(i * hw, hw)

    @pl.loop(0, 2)
    def _(s):
        v = mm(cat([pool[pn.cb + s * nt + k] for k in range(nt)], 1), wd_v[...], 1, 1)
        v = jnp.where(live(s), v, 0.0)
        act[s, :, dcols(3)] = v.astype(BF16)

    ob[...] = jnp.broadcast_to(
        jnp.sum(jnp.where(live(0), pool[pn.cb + t].astype(F32), 0.0), axis=0, keepdims=True), ob.shape
    )
    z_sent(1)
    begin("w1r")
    fin2(0)
    fin2(1)
    @pl.loop(0, 2 * npair)
    def _(i):
        pl.when(i == npair)(lambda: line_o.send(2, "far"))
        s, hp = i // npair, lax.rem(i, npair)
        cols = pl.ds(pl.multiple_of(hp * LANES, LANES), LANES)
        dq, dk, dv = [], [None, None], [None, None]
        for qt in range(2):
            rows, kr, nk = pl.ds(qt * TW, TW), pl.ds(0, (qt + 1) * TW), (qt + 1) * TW
            bias = bias_of(s, qt)
            da = act[s, rows, pl.ds(pl.multiple_of(3 * hw + hp * LANES, LANES), LANES)]
            prod = da.astype(F32) * attn[s, rows, cols].astype(F32)
            qs, ks, vs = qkv[0, s, rows, cols], qkv[1, s, kr, cols], qkv[2, s, kr, cols]
            got = []
            for h in range(2):
                pf = probs(only(qs, h), ks, bias)
                pb = pf.astype(BF16)
                delta = jnp.sum(only(prod, h), axis=1, keepdims=True)
                dp = mm(only(da, h), vs, 1, 1)
                ds = (pf * (dp - delta) * score_scale).astype(BF16)
                got.append((mm(ds, ks), mm(ds, qs, 0, 0), mm(pb, da, 0, 0)))
            pick = [jnp.where(heads2[0], a, b) for a, b in zip(*got)]
            dq.append(pick[0])
            for lst, v in ((dk, pick[1]), (dv, pick[2])):
                lst[0] = v[:TW] if lst[0] is None else lst[0] + v[:TW]
                if qt:
                    lst[1] = v[TW:]
        low1 = lax.rem(lane1, ROT) < ROT // 2
        for i3, parts in enumerate((dq, dk, dv)):
            for qt in range(2):
                rows = pl.ds(qt * TW, TW)
                v = parts[qt]
                if i3 < 2:
                    sw = jnp.where(
                        low1, pltpu.roll(v, LANES - ROT // 2, 1), pltpu.roll(v, ROT // 2, 1)
                    )
                    v = v * tab[s, rows, pl.ds(0, LANES)] - sw * tab[s, rows, pl.ds(LANES, LANES)]
                bias3[i3, pl.ds(0, 1), cols] += jnp.sum(v, axis=0, keepdims=True)
                act[s, rows, pl.ds(pl.multiple_of(i3 * hw + hp * LANES, LANES), LANES)] = v.astype(BF16)

    line_o.send(2, "near")
    mid(fc1_p[0])
    mid(fc1_p[1])

    def dh_chunk(s, k):
        rhs = cat([wq_v[i, at512(k), :] for i in range(3)] + [pool[pn.cb + u * nt + k] for u in range(nu)], 1)
        lhs = cat([act[s, :, pl.ds(0, 3 * hw)], buf[pl.ds(s * BK, BK), :]], 1)
        pool[pn.hb + s * nt + k] = mm(lhs, rhs, 1, 1).astype(BF16)

    def step_of(tt, k):
        if k == tt:
            return nt
        return nt - 1 - k + tt if k > tt else k + nt - 1 - tt

    far = [sorted(range(nt), key=lambda k, tt=tt: (step_of(tt, k), k)) for tt in range(nt)]

    def far_chunk(i):
        k = 0
        for tt in range(nt):
            for n in range(nt):
                k = jnp.where((t == tt) & (i == n), far[tt][n], k)
        return k

    def qkv_blocks():
        @pl.loop(0, nt)
        def _(k):
            out = mm(
                cat([pool[pn.xb + k], pool[pn.xb + nt + k]], 1),
                cat([act[0, :, pl.ds(0, 3 * hw)], act[1, :, pl.ds(0, 3 * hw)]], 0),
            ).astype(BF16)
            pool[pn.f2b + k] = out[:, :BK]
            pool[pn.f2b + nt + k // 2, :, at256(lax.rem(k, 2))] = out[:, BK:]

        for i in range(3):
            for p in qkv_p[i]:
                p.start(0)

    told(1)
    arrive("w1r")
    @pl.loop(0, nt)
    def _(i):
        k = far_chunk(i)
        dh_chunk(1, k)
        line_h.pair(k).start()

    arrive("xo")
    line_o.finish()

    @pl.loop(0, BK // 64)
    def _(q):
        rows = pl.ds(pl.multiple_of(q * 64, 64), 64)
        ocol = pl.ds(pl.multiple_of(t * BK, BK), BK)
        v = pool[pn.xo, rows, :].astype(F32) + line_o.value(rows)
        v = v + (obias[pl.ds(0, 1), ocol] + obias[pl.ds(1, 1), ocol])
        pool[pn.w1b + t, rows, :] = v.astype(BF16)

    def out_copy():
        return pltpu.make_async_copy(pool.at[pn.w1b + t], block_out, s_load.at[2])

    out_copy().start()

    line_o.sent()
    @pl.loop(0, nt)
    def _(i):
        k = far_chunk(i)
        dh_chunk(0, k)
        line_h.pair(k).wait()
        pl.when(i < nt - 1)(lambda: line_h.send(i, "end"))

    fin2(2)
    fin2(3)
    for b in range(pn.bits):
        pl.semaphore_signal(credit.at[6 + b], inc=1, device_id=place.over(b), device_id_type=MESH)
    mid(fc1_p[2])
    for b in range(pn.bits):
        pl.semaphore_wait(credit.at[6 + b], 1)
    qkv_blocks()
    mid(fc1_p[3])
    line_h.send(1, "near")
    fin1(0)
    mid(qkv_p[0])
    line_h.send(2, "far")
    mid(qkv_p[1])
    line_h.send(2, "near")
    mid(qkv_p[2])
    fin1(1)
    fin1(2)

    gcol = pl.ds(pl.multiple_of(t * BK, BK), BK)

    def tail(rows):
        dh = line_h.value(rows)
        normed = (pool[pn.xo, rows, :].astype(F32) - mi[0, rows, pl.ds(0, 1)]) * mi[0, rows, pl.ds(1, 1)]
        return dh, normed, dh * gain[:, gcol]

    def s_copy(k, f):
        src = stt.at[:, pl.ds(f * TW, TW)]
        return remote(src, sr.at[t, :, pl.ds(f * TW, TW)], s_s.at[k, f], r_s.at[t, f], (d, lax.rem(t + k, nt)))

    def tail_one(f):
        line_h.finish((f,))

        @pl.loop(0, TW // 64)
        def _(q):
            rows = pl.ds(pl.multiple_of(f * TW + q * 64, 64), 64)
            dh, normed, scaled = tail(rows)
            s1 = jnp.sum(scaled, axis=1, keepdims=True)
            s2 = jnp.sum(scaled * normed, axis=1, keepdims=True)
            stc[rows, :] = jnp.where(first, s1, s2)
            ng[pl.ds(0, 1), :] += jnp.sum(dh * normed, axis=0, keepdims=True)
            ng[pl.ds(1, 1), :] += jnp.sum(dh, axis=0, keepdims=True)

        half = pl.ds(f * TW, TW)
        stt[:, half] = stc[half, :].T[:8]
        sr[t, :, half] = stt[:, half]
        for k in range(1, nt):
            s_copy(k, f).start()

    def tail_two(f):
        half = pl.ds(f * TW, TW)
        for k in range(1, nt):
            s_copy(k, f).wait_send()
            frm = lax.rem(t + k, nt)
            remote(
                stt.at[:, half], sr.at[frm, :, half], s_s.at[k, f], r_s.at[frm, f], place.pair()
            ).wait_recv()
        tot = sr[0, :, half]
        for k in range(1, nt):
            tot = tot + sr[k, :, half]
        stc[half, :] = jnp.concatenate([tot / pn.width, jnp.zeros((LANES - 8, TW), F32)], axis=0).T

        for h in range(2):

            def put(ref, h=h):
                @pl.loop(0, TW // 64)
                def _(q):
                    rows = pl.ds(pl.multiple_of(f * TW + q * 64, 64), 64)
                    part = slice(h * TW, (h + 1) * TW)
                    _, normed, scaled = (v[:, part] for v in tail(rows))
                    v = scaled - stc[rows, pl.ds(0, 1)] - normed * stc[rows, pl.ds(1, 1)]
                    keep = tab[0, rows, pl.ds(2 * LANES, 1)] >= 0.0
                    own = pool[pn.co, rows, pl.ds(h * TW, TW)].astype(F32)
                    ref[pl.ds(pl.multiple_of(q * 64, 64), 64), :] = v * mi[0, rows, pl.ds(1, 1)] + jnp.where(
                        keep, own, 0.0
                    )

            stage_out(put, input_grad.at[pl.ds(f * TW, TW), pl.ds(h * TW, TW)])

    def pass_on(slot):
        return pltpu.make_async_copy(fr.at[slot], other_out.at[slot], s_f.at[2, slot])

    def pass_all(lo, hi):
        for slot in range(lo, hi):
            send_pair(slot).wait()
            pass_on(slot).start()

    tail_one(0)
    tail_one(1)

    def v_copy(k):
        peer = lax.rem(d + k, nd)
        return remote(sv.at[peer], rv.at[d], s_v.at[k], r_v.at[d], (peer, t))

    cw, hwd = BK // nd, 2 * hw // nd
    sv[...] = jnp.zeros_like(sv)
    for dd in range(nd):
        mine = c == dd % 2
        sv[dd, pl.ds(0, 1), pl.ds(0, ub)] = jnp.where(mine, fb[pl.ds(0, 1), pl.ds((dd // 2) * ub, ub)], 0.0)
        sv[dd, pl.ds(1, 2), pl.ds(0, cw)] = ng[pl.ds(0, 2), pl.ds(dd * cw, cw)]
        sv[dd, pl.ds(3, 1), pl.ds(0, cw)] = ob[pl.ds(0, 1), pl.ds(dd * cw, cw)]
        here = c == (dd * hwd) // hw
        src = pl.ds((dd * hwd) % hw, hwd)
        sv[dd, pl.ds(4, 1), pl.ds(0, hwd)] = jnp.where(here, bias3[0, pl.ds(0, 1), src], 0.0)
        sv[dd, pl.ds(5, 1), pl.ds(0, hwd)] = jnp.where(here, bias3[2, pl.ds(0, 1), src], 0.0)
        for core in range(2):
            sv[dd, pl.ds(6 + core, 1), :] = jnp.where(c == core, bias3[1, pl.ds(0, 1), :], 0.0)
    for k in range(1, nd):
        v_copy(k).start()
    rv[d] = sv[d]
    fin1(3)
    fin_d()
    pass_all(0, nq)
    fin3(0)
    fin3(1)
    tail_two(0)
    fin3(2)
    tail_two(1)
    pass_all(nq, nq + 3)
    line_h.sent()
    for k in range(1, nd):
        v_copy(k).wait_send()
        frm = lax.rem(d + k, nd)
        remote(sv.at[0], rv.at[frm], s_v.at[k], r_v.at[frm], place.pair()).wait_recv()
    res = rv[0]
    for k in range(1, nd):
        res = res + rv[k]
    fc1b_out[...] = res[0:1, :ub]
    norm_out[...] = res[1:3, :cw]
    outb_out[...] = jnp.concatenate([res[3:4, :cw], res[3:4, :cw]], axis=0)
    qvb_out[...] = res[4:6, :hwd]
    rk = ROT // nd
    turned = pltpu.roll(res, lax.rem(TW - d * rk, TW), 1)
    for core in range(2):
        for h in range(pn.heads):
            stc[pl.ds(core * pn.heads + h, 1), pl.ds(0, rk)] = turned[6 + core : 7 + core, h * HD : h * HD + rk]
    keyb_out[...] = stc[pl.ds(0, LANES), :].T[:rk, : 2 * pn.heads]
    for slot in range(nq + 3):
        pass_on(slot).wait()
    out_copy().wait()
    for cp in os_used[-ostage.shape[0] :]:
        cp.wait()

def results_kernel(nq, direct, *refs):
    n = len(refs) // 3 - 1
    src, dst, hold = refs[: n + 1], refs[n + 1 : 2 * n + 1], refs[2 * n + 1 : 3 * n + 2]
    wide, sem, sem_w = refs[3 * n + 2 :]
    c = lax.rem(lax.axis_index("dp"), 2)
    order = sorted(range(n + 1), key=lambda i: -math.prod(src[i].shape))
    order = [n] + [i for i in order if i != n]

    def get(i):
        return pltpu.make_async_copy(src[i], hold[i], sem.at[0, i])

    def parts(i):
        if i not in (3, 7):
            return [(hold[i], dst[i])]
        m = 3 if i == 3 else nq
        out = []
        for k in range(m):
            if i == 3:
                own, at = hold[3].at[k], lambda core, k=k: dst[3].at[k, :, at256(core)]
            else:
                own = hold[7].at[:, pl.ds(k * TW, TW)]
                at = lambda core, k=k: dst[7].at[:, at256(2 * k + core if direct else core * nq + k)]
            out += [(own, at(c)), (wide.at[nq + k if i == 3 else k], at(1 - c))]
        return out

    count = [0]

    def put(i):
        for a, b in parts(i):
            cp = pltpu.make_async_copy(a, b, sem_w.at[count[0]])
            count[0] += 1
            cp.start()
            sent.append(cp)

    sent = []
    for i in order:
        get(i).start()
    for i in order:
        get(i).wait()
        if i == n:
            wide[...] = hold[n][...].astype(F32)
        else:
            put(i)
    for cp in sent:
        cp.wait()


def results(arrays, nq, direct, shapes):
    n = len(shapes)
    anyw = pl.BlockSpec(memory_space=pl.ANY)
    return pl.pallas_call(
        functools.partial(results_kernel, nq, direct),
        out_shape=[jax.ShapeDtypeStruct(s, a.dtype) for s, a in zip(shapes, arrays)],
        in_specs=[anyw] * (n + 1),
        out_specs=[anyw] * n,
        scratch_shapes=[pltpu.VMEM(a.shape, a.dtype) for a in arrays]
        + [
            pltpu.VMEM(arrays[n].shape, F32),
            pltpu.SemaphoreType.DMA((1, n + 1)),
            pltpu.SemaphoreType.DMA((n - 2 + 2 * (nq + 3),)),
        ],
        compiler_params=pltpu.CompilerParams(vmem_limit_bytes=VMEM_BYTES),
        name="results",
    )(*arrays)


def per_device(
    hidden_in,
    cotangent,
    segment_ids,
    positions,
    norm_gain,
    norm_shift,
    qkv_weight,
    qv_bias,
    key_bias,
    dense_weight,
    fc1_weight,
    fc1_bias,
    fc2_weight,
    out_bias,
):
    nd, nt = lax.axis_size("dp"), lax.axis_size("tensor")
    c = lax.rem(lax.axis_index("dp"), 2)
    nch = nd // 2
    rows, wl = hidden_in.shape
    width = wl * nt
    heads = key_bias.shape[0] // 2
    units = fc1_weight.shape[1] // 2
    ub = units // nch
    pn = Plan(nd, nt, units, heads, ub)
    hw, rb, rd, nq = pn.hw, pn.rb, pn.rd, units // TW
    assert rows == BK and wl == BK and nt == 4 and nq == 4 and hw == TW and rb == ub
    direct = ub == TW

    freq = 10000.0 ** (-(np.arange(LANES) % (ROT // 2)) * (2.0 / ROT))
    freq = jnp.asarray(freq.astype(np.float32)[None, :])

    def pick(w, axis):
        shape = w.shape
        w = w.reshape(*shape[:axis], nch, 2, ub, *shape[axis + 1 :])
        w = lax.dynamic_index_in_dim(w, c, axis + 1, keepdims=False)
        return w.reshape(*shape[:axis], units, *shape[axis + 1 :])

    w1, w2, b1 = fc1_weight, fc2_weight, fc1_bias
    if not direct:
        w1, w2, b1 = pick(w1, 1), pick(w2, 0), pick(b1, 0)
    w1 = w1.reshape(nt, BK, w1.shape[1])
    wq = qkv_weight.transpose(1, 0, 2)
    b1 = b1.reshape(1, -1)

    vm = pl.BlockSpec(memory_space=pltpu.VMEM)
    anyw = pl.BlockSpec(memory_space=pl.ANY)
    shapes = [
        ((rows, wl), BF16, anyw),
        ((rows, wl), F32, anyw),
        ((2, wl // nd), F32, vm),
        ((3, rb, hw), F32, anyw),
        ((2, 2 * hw // nd), F32, vm),
        ((ROT // nd, 2 * heads), F32, vm),
        ((rd, width), F32, anyw),
        ((rb, units), F32, anyw),
        ((1, ub), F32, vm),
        ((ub, width), F32, anyw),
        ((2, wl // nd), F32, vm),
        ((nq + 3, rb, TW), BF16, anyw),
    ]
    dma = pltpu.SemaphoreType.DMA
    nos = 4
    scratch = [
        pltpu.VMEM((pn.blocks, BK, BK), BF16),
        pltpu.VMEM((3, width, hw), BF16),
        pltpu.VMEM((hw, width), BF16),
        pltpu.VMEM((2, rows, 3 * LANES), F32),
        pltpu.VMEM((2, 8, rows), F32),
        pltpu.VMEM((2, rows, units), BF16),
        pltpu.VMEM((units, 2 * rows), BF16),
        pltpu.VMEM((2, rows, units), F32),
        pltpu.VMEM((3, 2, rows, hw), BF16),
        pltpu.VMEM((2, rows, hw), BF16),
        pltpu.VMEM((2, rows, hw), BF16),
        pltpu.VMEM((nch * rd, 2 * rows), BF16),
        pltpu.VMEM((hw, rows), BF16),
        pltpu.VMEM((nch * rd, width), BF16),
        pltpu.VMEM((nt, nch - 1, rd, BK), BF16),
        pltpu.VMEM((pn.n2 + pn.n1, nch - 1, rb, TW), BF16),
        pltpu.VMEM((nq + 3, rb, TW), BF16),
        pltpu.VMEM((nq + 3, rb, TW), BF16),
        pltpu.VMEM((nos, TW, TW), F32),
        pltpu.VMEM((2, rows, LANES), F32),
        pltpu.VMEM((3, 8, hw), F32),
        pltpu.VMEM((8, units), F32),
        pltpu.VMEM((8, wl), F32),
        pltpu.VMEM((8, wl), F32),
        pltpu.VMEM((nd, 8, TW), F32),
        pltpu.VMEM((nd, 8, TW), F32),
        pltpu.VMEM((rows, LANES), F32),
        pltpu.VMEM((8, rows), F32),
        pltpu.VMEM((nt, 8, rows), F32),
        pltpu.VMEM((2, nt, 8, LANES), F32),
        pltpu.VMEM((8, hw), F32),
        pltpu.VMEM((8, LANES), F32),
        dma((10 + nq * (2 + nt),)),
        dma((2, 2, nt, 2)),
        dma((2, nt, 2)),
        dma((2, nt, 2)),
        dma((2, nt, 2)),
        dma((4,)),
        dma((pn.pieces, nch - 1)),
        dma((pn.pieces, nch - 1)),
        dma((2,)),
        dma((2,)),
        dma((3, nq + 3)),
        dma((nos,)),
        dma((2, 2)),
        dma((nt,)),
        dma((nt,)),
        dma((2, nt, 2)),
        dma((nt + 1, 2)),
        dma((nt,)),
        dma((nt,)),
        dma((2, nt, 2)),
        dma((nt + 1, 2)),
        dma((nd,)),
        dma((nd,)),
        dma((nt, 2)),
        dma((nt, 2)),
        dma((2, nt)),
        dma((2, nt)),
        pltpu.SemaphoreType.REGULAR((6 + pn.bits,)),
    ]
    res = pl.pallas_call(
        functools.partial(block_kernel, pn, direct),
        out_shape=[jax.ShapeDtypeStruct(s, dt) for s, dt, _ in shapes],
        in_specs=[anyw, anyw, vm, vm, vm, vm, vm, anyw, anyw, anyw, anyw, vm, vm, vm, vm],
        out_specs=[sp for _, _, sp in shapes],
        scratch_shapes=scratch,
        compiler_params=pltpu.CompilerParams(
            collective_id=0, has_side_effects=True, vmem_limit_bytes=VMEM_BYTES
        ),
        name="block",
    )(
        hidden_in, cotangent, segment_ids.reshape(1, rows), positions.reshape(1, rows), freq, norm_gain.reshape(1, width), norm_shift.reshape(1, width),
        w1, w2, wq, dense_weight, b1, qv_bias, key_bias, out_bias,
    )
    whole = [s for s, _, _ in shapes[:-1]]
    whole[3], whole[7] = (3, rb, 2 * hw), (rb, 2 * units)
    res = list(results(res, nq, direct, whole))
    res[3] = res[3].transpose(1, 0, 2)
    res[5] = res[5].T
    if not direct:
        res[7] = res[7].reshape(rb, 2, nch, ub).transpose(0, 2, 1, 3).reshape(rb, 2 * units)
    res[8] = res[8].reshape(ub)
    return tuple(res)


def solution(mesh):
    placed = (
        P("dp", "tensor"),
        P("dp", "tensor"),
        P("dp"),
        P("dp"),
        P(),
        P(),
        P(None, None, "tensor"),
        P(None, "tensor"),
        P("tensor", None),
        P("tensor", None),
        P(None, "tensor"),
        P("tensor"),
        P("tensor", None),
        P(),
    )
    return jax.shard_map(
        per_device,
        mesh=mesh,
        in_specs=placed,
        out_specs=(
            P("dp", "tensor"),
            P("dp", "tensor"),
            P(None, ("tensor", "dp")),
            P("dp", None, "tensor"),
            P(None, ("tensor", "dp")),
            P("tensor", "dp"),
            P(("tensor", "dp"), None),
            P("dp", "tensor"),
            P(("tensor", "dp")),
            P(("tensor", "dp"), None),
            P(None, ("tensor", "dp")),
        ),
        check_vma=False,
    )
```

```python
import functools
import math

import jax
import jax.numpy as jnp
import numpy as np
from jax import lax
from jax.experimental import pallas as pl
from jax.experimental.pallas import tpu as pltpu
from jax.sharding import PartitionSpec as P

HD = 64
ROT = 32
LANES = 128

norm_epsilon = 1e-05
gelu_scale = 0.7978845608028654
gelu_cubic = 0.044715
masked_score = -1e30

MESH = pl.DeviceIdType.MESH
F32 = jnp.float32
BF16 = jnp.bfloat16
VMEM_BYTES = 67043328


def gelu_tanh(u):
    return jnp.tanh(u * (gelu_scale + (gelu_scale * gelu_cubic) * (u * u)))


def gelu_slope(u):
    tanh_val = gelu_tanh(u)
    return 0.5 * (1.0 + tanh_val) + (0.5 * u) * (1.0 - tanh_val * tanh_val) * (
        gelu_scale + (3.0 * gelu_scale * gelu_cubic) * (u * u)
    )


class Place:
    def __init__(self, nd, nt):
        self.nd, self.nt = nd, nt
        self.nch = nd // 2
        self.bits = self.nch.bit_length() - 1
        self.d = lax.axis_index("dp")
        self.t = lax.axis_index("tensor")
        self.c = lax.rem(self.d, 2)
        self.j = self.d // 2

    def pair(self):
        return (self.d + 1 - 2 * self.c, self.t)

    def chip_bit(self, b):
        return lax.rem(self.j // (1 << b), 2)

    def over(self, b):
        step = 2 << b
        return (self.d + step - 2 * step * self.chip_bit(b), self.t)

    def right(self):
        return (self.d, jnp.minimum(self.t + 1, self.nt - 1))

    def left(self):
        return (self.d, jnp.maximum(self.t - 1, 0))


def remote(src, dst, send, recv, device):
    return pltpu.make_async_remote_copy(
        src_ref=src, dst_ref=dst, send_sem=send, recv_sem=recv, device_id=device, device_id_type=MESH
    )


def greet(place):
    barrier = pltpu.get_barrier_semaphore()

    def signal(d, t):
        pl.semaphore_signal(barrier, inc=1, device_id=(d, t), device_id_type=MESH)

    for k in range(1, place.nd):
        signal(lax.rem(place.d + k, place.nd), place.t)
    for k in range(1, place.nt):
        signal(place.d, lax.rem(place.t + k, place.nt))
        signal(place.pair()[0], lax.rem(place.t + k, place.nt))


def greeted(place):
    pl.semaphore_wait(pltpu.get_barrier_semaphore(), place.nd - 1 + 2 * (place.nt - 1))


BK = 512
TW = 256


def mm(a, b, ca=1, cb=0):
    return lax.dot_general(a, b, (((ca,), (cb,)), ((), ())), preferred_element_type=F32)


def cat(parts, axis):
    return jnp.concatenate(parts, axis=axis)


def at512(i):
    return pl.ds(pl.multiple_of(i * BK, BK), BK)


def at256(i):
    return pl.ds(pl.multiple_of(i * TW, TW), TW)


class Plan:
    def __init__(self, nd, nt, units, heads, ub):
        self.nd, self.nt = nd, nt
        self.nch = nd // 2
        self.bits = self.nch.bit_length() - 1
        self.units, self.heads, self.ub = units, heads, ub
        self.hw = heads * HD
        self.nu = units // BK
        self.width = nt * BK
        self.rb = self.width // nd
        self.rd = 2 * self.hw // nd
        n = 0
        for name, size in (
            ("xb", 2 * nt),
            ("cb", 2 * nt),
            ("hb", 2 * nt),
            ("w1b", 2 * nt + 1),
            ("w2b", 2 * nt + 1),
            ("f2b", self.nu * nt),
            ("f1b", self.nu * nt),
            ("xo", 1),
            ("co", 1),
        ):
            setattr(self, name, n)
            n += size
        self.blocks = n
        self.n2 = 2 * nt
        self.n1 = 2 * (units // TW)
        self.n3 = 2 * 3
        self.pieces = self.n2 + self.n1 + self.n3 + nt


class Piece:
    def __init__(self, place, order, view, recv, ss, rs):
        self.p, self.order, self.view, self.r, self.ss, self.rs = place, order, view, recv, ss, rs
        self.off = [0]
        for i in range(len(order)):
            self.off.append(self.off[-1] + (place.nch >> (i + 1)))

    def block(self, i, m, mine):
        j = 0
        for b in self.order[:i]:
            j = j + self.p.chip_bit(b) * (1 << b)
        if i < len(self.order):
            b = self.order[i]
            v = self.p.chip_bit(b)
            j = j + (v if mine else 1 - v) * (1 << b)
            for q, b2 in enumerate(self.order[i + 1 :]):
                j = j + ((m >> q) & 1) * (1 << b2)
        return j

    def held(self, i, m, before):
        idx = 0
        for r in range(before + 1, min(i, len(self.order))):
            idx = idx + self.p.chip_bit(self.order[r]) * (1 << (r - before - 1))
        if i < len(self.order):
            v = self.p.chip_bit(self.order[i])
            idx = idx + (1 - v) * (1 << (i - before - 1)) + m * (1 << (i - before))
        return self.off[before] + idx

    def copy(self, i, m):
        k = self.off[i] + m
        return remote(
            self.view(self.block(i, m, False)),
            self.r.at[k],
            self.ss.at[k],
            self.rs.at[k],
            self.p.over(self.order[i]),
        )

    def total(self, i, m, rows):
        acc = self.view(self.block(i, m, False))[rows, :].astype(F32)
        for before in range(i):
            acc = acc + self.r[self.held(i, m, before), rows, :].astype(F32)
        return acc

    def each(self, do):
        rows = self.view(0).shape[0]
        size = min(rows, 64)

        @pl.loop(0, rows // size)
        def _(q):
            do(pl.ds(pl.multiple_of(q * size, size), size))

    def start(self, i):
        for m in range(self.p.nch >> (i + 1)):
            if i > 0:
                dst = self.view(self.block(i, m, False))

                def put(rows, dst=dst, m=m):
                    dst[rows, :] = self.total(i, m, rows).astype(BF16)

                self.each(put)
            self.copy(i, m).start()

    def wait(self, i):
        for m in range(self.p.nch >> (i + 1)):
            self.copy(i, m).wait()

    def final(self, to):
        def put(rows):
            to[rows, :] = self.total(len(self.order), 0, rows).astype(to.dtype)

        self.each(put)


def block_kernel(pn, direct, *refs):
    (
        x_in, c_in, seg_in, pos_in, freq, gain, shift, w1, w2, wq, wd, b1, qvb, kb, obias,
        block_out, input_grad, norm_out, qkv_out, qvb_out, keyb_out, dense_out, fc1_out, fc1b_out,
        fc2_out, outb_out, other_out,
        pool, wq_v, wd_v, tab, segr, act, buf, pre_v, qkv, attn, attn_p, dl, at_tmp, dg, dr, rp, fs, fr,
        ostage, mi, bias3, fb, ob, ng, sv, rv, stc, stt, sr, st, kbv, stk,
        s_load, s_z, r_z, s_c, r_c, s_tab, s_p, r_p, s_d, r_d, s_f, s_os, s_a, s_oc, r_oc, s_ol, r_ol,
        s_hc, r_hc, s_hl, r_hl, s_v, r_v, s_s, r_s, s_st, r_st, credit,
    ) = refs
    nd, nt, nch, nu = pn.nd, pn.nt, pn.nch, pn.nu
    hw, ub, rb, rd = pn.hw, pn.ub, pn.rb, pn.rd
    place = Place(nd, nt)
    t, c, d = place.t, place.c, place.d
    nq = pn.units // TW

    def load(i, src, dst):
        return pltpu.make_async_copy(src, dst, s_load.at[i])

    loads = {
        "x": [load(0, x_in, pool.at[pn.xb + t])],
        "c": [load(1, c_in, pool.at[pn.cb + t])],
        "wd": [load(4, wd.at[pl.ds(pl.multiple_of(c * hw, hw), hw), :], wd_v)],
        "wq": [
            load(5, wq.at[:, :, pl.ds(pl.multiple_of(c * hw, hw), hw)], wq_v)
        ],
        "xo": [load(8, x_in, pool.at[pn.xo]), load(9, c_in, pool.at[pn.co])],
        "w1": [],
        "w2": [],
        "w1r": [],
    }
    n = 10
    for q in range(nq):
        col = (2 * q + c if direct else q) * TW
        src = w1.at[:, :, pl.ds(pl.multiple_of(col, TW), TW)]
        half = pl.ds((q % 2) * TW, TW)
        loads["w1"].append(load(n, src, pool.at[pl.ds(pn.w1b + (q // 2) * nt, nt), :, half]))
        loads["w1r"].append(load(n + 1, src, pool.at[pl.ds(pn.cb + (q // 2) * nt, nt), :, half]))
        n += 2
        for k in range(nt):
            src = w2.at[pl.ds(pl.multiple_of(col, TW), TW), pl.ds(k * BK, BK)]
            loads["w2"].append(load(n, src, pool.at[pn.w2b + (q // 2) * nt + k, half, :]))
            n += 1

    def begin(*names):
        for name in names:
            for cp in loads[name]:
                cp.start()

    def arrive(*names):
        for name in names:
            for cp in loads[name]:
                cp.wait()

    begin("x")
    greet(place)
    arrive("x")

    first = lax.broadcasted_iota(jnp.int32, (64, LANES), 1) == 0

    @pl.loop(0, BK // 64)
    def _(q):
        rows = pl.ds(pl.multiple_of(q * 64, 64), 64)
        v = pool[pn.xb + t, rows, :].astype(F32)
        m = jnp.sum(v, axis=1, keepdims=True) / BK
        v = v - m
        stc[rows, :] = jnp.where(first, m, jnp.sum(v * v, axis=1, keepdims=True))

    for j in range(4):
        turned = stc[pl.ds(j * LANES, LANES), :].T
        stk[pl.ds(j, 1), :] = turned[0:1]
        stk[pl.ds(4 + j, 1), :] = turned[1:2]

    greeted(place)

    def blk(a, s, k, f):
        return pool.at[a * (pn.cb - pn.xb) + pn.xb + s * nt + k, at256(f), :]

    def z_dev(side):
        return place.right() if side == 0 else place.left()

    def z_copy(a, k, side, f):
        return remote(blk(a, 0, k, f), blk(a, 0, k, f), s_z.at[side, a, k, f], r_z.at[a, k, f], z_dev(side))

    def c_copy(a, k, f):
        return remote(blk(a, 0, k, f), blk(a, 1, k, f), s_c.at[a, k, f], r_c.at[a, k, f], place.pair())

    def own_z(a, side, f):
        src = (x_in, c_in)[a].at[at256(f), :]
        return remote(src, blk(a, 0, t, f), s_z.at[side, a, t, f], r_z.at[a, t, f], z_dev(side))

    def own_c(a, f):
        src = (x_in, c_in)[a].at[at256(f), :]
        return remote(src, blk(a, 1, t, f), s_c.at[a, t, f], r_c.at[a, t, f], place.pair())

    def tab_copies():
        return (
            remote(tab.at[0], tab.at[1], s_tab.at[0], s_tab.at[1], place.pair()),
            remote(segr.at[0], segr.at[1], s_tab.at[2], s_tab.at[3], place.pair()),
        )

    def item(side, who, i):
        if side == 0:
            first = i <= who
            return jnp.where(first, 0, 1), jnp.where(first, who - i, 2 * who + 1 - i)
        m = nt - who
        first = i < m
        return jnp.where(first, 0, 1), jnp.where(first, who + i, who + i - m)

    def progress(step, halves=(0, 1)):
        for f in halves:
            if step >= 1:
                @pl.when((t > 0) & (step - 1 < 2 * t))
                def _():
                    a, k = item(0, t - 1, step - 1)
                    z_copy(a, k, 0, f).wait_recv()
                    c_copy(a, k, f).start()

                @pl.when((t < nt - 1) & (step - 1 < 2 * (nt - 1 - t)))
                def _():
                    a, k = item(1, t + 1, step - 1)
                    z_copy(a, k, 1, f).wait_recv()
                    c_copy(a, k, f).start()

            for side in range(2):
                me = t if side == 0 else nt - 1 - t
                if step == 0:
                    pl.when(me < nt - 1)(lambda side=side: own_z(0, side, f).start())
                else:
                    @pl.when((me < nt - 1) & (step <= me))
                    def _():
                        z_copy(0, me - step if side == 0 else nt - 1 - me + step, side, f).start()

                @pl.when((me < nt - 1) & (step > me) & (step <= 2 * me))
                def _():
                    k = 2 * me - step
                    z_copy(1, k if side == 0 else nt - 1 - k, side, f).start()

        for side in range(2 if 1 in halves else 0):
            me = t if side == 0 else nt - 1 - t

            @pl.when((me < nt - 1) & (step == me))
            def _():
                own_z(1, side, 0).start()
                own_z(1, side, 1).start()

    def z_sent(a):
        for f in range(2):
            for m in range(nt):
                for side in range(2):
                    me = t if side == 0 else nt - 1 - t

                    @pl.when((me < nt - 1) & (m <= me))
                    def _():
                        k = me - m
                        z_copy(a, k if side == 0 else nt - 1 - k, side, f).wait_send()

            for k in range(nt):
                c_copy(a, k, f).wait_send()

    def arrival(tt, k):
        if k == tt:
            return -1
        return 2 * tt - 1 - k if k < tt else (nt - 1 - tt) + (k - tt - 1)

    orders = [sorted(range(nt), key=lambda k, tt=tt: (arrival(tt, k), k)) for tt in range(nt)]
    needed = [max(arrival(tt, orders[tt][i]) for tt in range(nt)) + 1 for i in range(nt)]

    def chunk(i):
        k = orders[0][i]
        for tt in range(1, nt):
            k = jnp.where(t == tt, orders[tt][i], k)
        return k

    def st_copy(s, k):
        peer = lax.rem(t + k, nt)
        dev = (d, peer) if s == 0 else (place.pair()[0], peer)
        return remote(stk, st.at[s, t], s_st.at[s, k], r_st.at[s, t], dev)

    for k in range(nt):
        for s in range(2):
            if k or s:
                st_copy(s, k).start()
    progress(0)
    for f in range(2):
        own_c(0, f).start()
    st[0, t] = stk[...]
    begin("w1", "c")

    def column(row):
        return jnp.broadcast_to(row.astype(F32), (LANES, BK)).T

    lane1 = lax.broadcasted_iota(jnp.int32, (1, LANES), 1)
    dim1 = lax.rem(lane1, HD)
    angles = column(pos_in[...]) * freq[...]
    tab[0, :, pl.ds(0, LANES)] = jnp.where(dim1 < ROT, jnp.cos(angles), 1.0)
    sine = jnp.sin(angles)
    sine = jnp.where(dim1 < ROT // 2, -sine, sine)
    tab[0, :, pl.ds(LANES, LANES)] = jnp.where(dim1 < ROT, sine, 0.0)
    tab[0, :, pl.ds(2 * LANES, LANES)] = column(seg_in[...])
    segr[0] = jnp.broadcast_to(seg_in[...].astype(F32), (8, BK))
    kbv[...] = jnp.zeros_like(kbv)
    for h in range(pn.heads):
        kbv[pl.ds(0, 1), pl.ds(h * HD, ROT)] = kb[pl.ds(c * pn.heads + h, 1), :]
    arrive("c")
    for f in range(2):
        own_c(1, f).start()
    for cp in tab_copies():
        cp.start()
    fb[...] = jnp.zeros_like(fb)
    bias3[...] = jnp.zeros_like(bias3)
    ng[...] = jnp.zeros_like(ng)
    for k in range(nt):
        for s in range(2):
            if k or s:
                frm = lax.rem(t + k, nt)
                st_copy(s, k).wait_send()
                remote(stk, st.at[s, frm], s_st.at[s, k], r_st.at[s, frm], place.pair()).wait_recv()
    for s in range(2):
        mean = sum(st[s, k, pl.ds(0, 4), :] for k in range(nt)) / nt
        dev = 0.0
        for k in range(nt):
            off = st[s, k, pl.ds(0, 4), :] - mean
            dev = dev + st[s, k, pl.ds(4, 4), :] + BK * off * off
        inv = lax.rsqrt(dev / pn.width + norm_epsilon)
        for j in range(4):
            both = cat([mean[j : j + 1], inv[j : j + 1], jnp.zeros((LANES - 2, LANES), F32)], 0)
            mi[s, pl.ds(j * LANES, LANES), :] = both.T
    arrive("w1")

    def live(s):
        return tab[s, :, pl.ds(2 * LANES, 1)] >= 0.0

    def gelu_block(s, u, pre):
        bias = []
        for q in range(2):
            col = (2 * (2 * u + q) + c if direct else 2 * u + q) * TW
            bias.append(b1[:, pl.ds(pl.multiple_of(col, TW), TW)])
        pre = pre + cat(bias, 1)
        val = (0.5 * pre * (1.0 + gelu_tanh(pre))).astype(BF16)
        act[s, :, at512(u)] = val
        val = jnp.where(live(s), val, jnp.zeros_like(val))
        buf[at512(u), at512(s)] = val.T

    def take(k, start, last=False):
        cols = pl.ds(pl.multiple_of(k * BK, BK), BK)

        @pl.loop(0, 2)
        def _(s):
            @pl.when(s == 1)
            def _():
                for f in range(2):
                    c_copy(0, k, f).wait_recv()

            @pl.loop(0, BK // 64)
            def _(q):
                rows = pl.ds(pl.multiple_of(q * 64, 64), 64)
                v = pool[pn.xb + s * nt + k, rows, :].astype(F32)
                v = (v - mi[s, rows, pl.ds(0, 1)]) * mi[s, rows, pl.ds(1, 1)]
                pool[pn.hb + s * nt + k, rows, :] = (v * gain[:, cols] + shift[:, cols]).astype(BF16)

            @pl.loop(0, nu)
            def _(u):
                out = mm(pool[pn.hb + s * nt + k], pool[pn.w1b + u * nt + k])
                if not start:
                    out = out + pre_v[s, :, at512(u)]
                pre_v[s, :, at512(u)] = out
                if last:
                    gelu_block(s, u, out)

    take(t, True)
    begin("wq", "wd", "w2", "xo")
    progress(1)
    pl.when(t >= 1)(lambda: take(t - 1, False))
    progress(2, (0,))
    pl.when(t + 1 < nt)(lambda: take(t + 1, False))
    progress(2, (1,))
    take(jnp.where(t >= 2, t - 2, t + 2), False)
    progress(3)
    for cp in tab_copies():
        cp.wait()

    @pl.when((t == 0) | (t == nt - 1))
    def _():
        take(nt - 1 - t, False, True)

    @pl.when((t > 0) & (t < nt - 1))
    def _():
        @pl.loop(0, 2 * nu)
        def _(i):
            s, u = i // nu, lax.rem(i, nu)
            gelu_block(s, u, pre_v[s, :, at512(u)])


    def biased(s, q):
        col = (2 * q + c if direct else q) * TW
        return pre_v[s, :, at256(q)] + b1[:, pl.ds(pl.multiple_of(col, TW), TW)]

    def tell(i):
        def signal(n, device):
            pl.semaphore_signal(credit.at[3 * i + n], inc=1, device_id=device, device_id_type=MESH)

        signal(0, place.pair())
        pl.when(t > 0)(lambda: signal(2, place.left()))
        pl.when(t < nt - 1)(lambda: signal(1, place.right()))

    def told(i):
        pl.semaphore_wait(credit.at[3 * i], 1)
        pl.when(t > 0)(lambda: pl.semaphore_wait(credit.at[3 * i + 1], 1))
        pl.when(t < nt - 1)(lambda: pl.semaphore_wait(credit.at[3 * i + 2], 1))

    tell(0)

    orders_ab = [list(range(pn.bits)), list(range(pn.bits))[::-1]]

    def piece(index, half, view, recv):
        return Piece(place, orders_ab[half], view, recv, s_p.at[index], r_p.at[index])

    per2 = BK // ub

    def view2(i, h):
        def view(j):
            return pool.at[
                pn.f2b + nu * i + j // per2,
                pl.ds(pl.multiple_of(lax.rem(j, per2) * ub, ub), ub),
                pl.ds(h * TW, TW),
            ]

        return view

    def view1(q, h):
        def view(j):
            r = 2 * j * rb + h * rb
            return pool.at[
                pn.f1b + nu * (r // BK) + q // 2,
                pl.ds(pl.multiple_of(lax.rem(r, BK), rb), rb),
                pl.ds((q % 2) * TW, TW),
            ]

        return view

    def view3(i, h):
        def view(j):
            r = 2 * j * rb + h * rb
            if i < 2:
                b, col = pn.f2b + r // BK, i * TW
            else:
                b, col = pn.f2b + nt + r // (2 * BK), pl.multiple_of(lax.rem(r // BK, 2) * TW, TW)
            return pool.at[b, pl.ds(pl.multiple_of(lax.rem(r, BK), rb), rb), pl.ds(col, TW)]

        return view

    def view_d(i):
        def view(j):
            return dg.at[pl.ds(pl.multiple_of(j * rd, rd), rd), pl.ds(i * BK, BK)]

        return view

    fc2_p = [[piece(2 * i + h, h, view2(i, h), rp.at[2 * i + h]) for h in range(2)] for i in range(nt)]
    fc1_p = [
        [piece(pn.n2 + 2 * q + h, h, view1(q, h), rp.at[pn.n2 + 2 * q + h]) for h in range(2)]
        for q in range(nq)
    ]
    qkv_p = [
        [piece(pn.n2 + pn.n1 + 2 * i + h, h, view3(i, h), rp.at[2 * i + h]) for h in range(2)]
        for i in range(3)
    ]
    den_p = [piece(pn.n2 + pn.n1 + pn.n3 + i, i % 2, view_d(i), dr.at[i]) for i in range(nt)]

    os_used = []

    def stage_out(value_to, dst):
        n = len(os_used)
        slot = n % ostage.shape[0]
        if n >= ostage.shape[0]:
            os_used[n - ostage.shape[0]].wait()
        value_to(ostage.at[slot])
        cp = pltpu.make_async_copy(ostage.at[slot, pl.ds(0, dst.shape[0]), :], dst, s_os.at[slot])
        cp.start()
        os_used.append(cp)

    def fin2(i):
        for h in range(2):
            p = fc2_p[i][h]
            p.wait(pn.bits - 1)

            def put(ref, p=p):
                p.final(ref)

            col = chunk(i) * BK + h * TW
            stage_out(put, fc2_out.at[:, pl.ds(pl.multiple_of(col, TW), TW)])

    def send_pair(slot):
        return remote(fs.at[slot], fr.at[slot], s_f.at[0, slot], s_f.at[1, slot], place.pair())

    def fin_pair(pieces, slot, dst):
        for h in range(2):
            pieces[h].wait(pn.bits - 1)

        def put(ref):
            for h in range(2):
                @pl.when(c == h)
                def _():
                    pieces[h].final(ref)

                @pl.when(c != h)
                def _():
                    pieces[h].final(fs.at[slot])

        stage_out(put, dst)
        send_pair(slot).start()

    def dst1(q):
        return fc1_out.at[:, pl.ds(q * TW, TW)]

    def dst3(i):
        return qkv_out.at[i]

    def fin1(q):
        fin_pair(fc1_p[q], q, dst1(q))

    def fin3(i):
        fin_pair(qkv_p[i], nq + i, dst3(i))

    def fin_d():
        for i in range(nt):
            p = den_p[i]
            p.wait(pn.bits - 1)
            for h in range(2):

                def put(ref, p=p, i=i, h=h):
                    half = pl.ds(h * TW, TW)
                    me = p.block(len(p.order), 0, True)
                    acc = dg[pl.ds(pl.multiple_of(me * rd, rd), rd), pl.ds(i * BK + h * TW, TW)].astype(F32)
                    for before in range(len(p.order)):
                        acc = acc + p.r[p.held(len(p.order), 0, before), :, half].astype(F32)
                    ref[pl.ds(0, rd), :] = acc

                col = chunk(i) * BK + h * TW
                stage_out(put, dense_out.at[:, pl.ds(pl.multiple_of(col, TW), TW)])

    def mids(pieces, i):
        for p in pieces:
            p.wait(i - 1)
            p.start(i)

    def mid(pieces):
        for i in range(1, pn.bits):
            mids(pieces, i)

    def fc2_chunk(i):
        k = chunk(i)
        for f in range(2):
            c_copy(1, k, f).wait_recv()
        for h in range(2):

            half = pl.ds(h * TW, TW)
            out = mm(buf[...], cat([pool[pn.cb + k, :, half], pool[pn.cb + nt + k, :, half]], 0)).astype(BF16)
            for u in range(nu):
                pool[pn.f2b + nu * i + u, :, half] = out[u * BK : (u + 1) * BK]
            fc2_p[i][h].start(0)

    done_steps = [nt - 1]

    def upto(step):
        while done_steps[0] < min(step, 2 * nt - 2):
            done_steps[0] += 1
            progress(done_steps[0])

    fc2_chunk(0)

    arrive("wq")
    lane = lax.broadcasted_iota(jnp.int32, (BK, TW), 1)
    low = lax.rem(lane, ROT) < ROT // 2

    def swap(v):
        return jnp.where(low, pltpu.roll(v, TW - ROT // 2, 1), pltpu.roll(v, ROT // 2, 1))

    def table(s, i):
        v = tab[s, :, pl.ds(i * LANES, LANES)]
        return jnp.concatenate([v, v], axis=1)

    @pl.loop(0, 2)
    def _(s):
        all_v = mm(cat([pool[pn.hb + s * nt + k] for k in range(nt)], 1), cat([wq_v[i] for i in range(3)], 1))
        for i in range(3):
            v = all_v[:, i * hw : (i + 1) * hw]
            cols = pl.ds(pl.multiple_of(c * hw, hw), hw)
            if i == 1:
                v = v + kbv[pl.ds(0, 1), :]
            else:
                v = v + qvb[pl.ds(i // 2, 1), cols]
            if i < 2:
                v = v * table(s, 0) + swap(v) * table(s, 1)
            qkv[i, s] = v.astype(BF16)

    upto(needed[1])
    fc2_chunk(1)
    z_sent(0)

    @pl.loop(0, 2 * nt)
    def _(i):
        for h in range(2):
            pool[pn.xb + i, :, pl.ds(h * TW, TW)] = pool[pn.hb + i, pl.ds(h * TW, TW), :].T


    mid(fc2_p[0])

    heads2 = [lane1 < HD, lane1 >= HD]
    score_scale = HD ** (-0.5)

    def only(v, h):
        return jnp.where(heads2[h], v, jnp.zeros_like(v))

    def bias_of(s, qt):
        nk = (qt + 1) * TW
        col = lax.broadcasted_iota(jnp.int32, (TW, nk), 1)
        row = lax.broadcasted_iota(jnp.int32, (TW, nk), 0) + qt * TW
        same = tab[s, pl.ds(qt * TW, TW), pl.ds(2 * LANES, 1)] == segr[s, pl.ds(0, 1), pl.ds(0, nk)]
        return jnp.where(same & (col <= row), 0.0, masked_score)

    def probs(qh, keys, bias):
        sc = mm(qh, keys, 1, 1) * score_scale + bias
        top = jnp.max(sc, axis=1, keepdims=True)
        ex = jnp.exp(sc - top)
        return ex * (1.0 / jnp.sum(ex, axis=1, keepdims=True))

    npair = hw // LANES

    def attention(s):
        @pl.loop(0, npair)
        def _(hp):
            cols = pl.ds(pl.multiple_of(hp * LANES, LANES), LANES)
            for qt in range(2):
                rows, kr = pl.ds(qt * TW, TW), pl.ds(0, (qt + 1) * TW)
                bias = bias_of(s, qt)
                out = []
                for h in range(2):
                    pb = probs(only(qkv[0, s, rows, cols], h), qkv[1, s, kr, cols], bias).astype(BF16)
                    out.append(mm(pb, qkv[2, s, kr, cols]))
                attn[s, rows, cols] = jnp.where(heads2[0], out[0], out[1]).astype(BF16)

    def attn_copy(s):
        return remote(attn.at[s], attn_p.at[1 - s], s_a.at[0, s], s_a.at[1, s], place.pair())

    attention(0)
    attn_copy(0).start()
    attention(1)
    attn_copy(1).start()
    upto(needed[2])
    fc2_chunk(2)
    mid(fc2_p[1])
    arrive("wd", "w2")

    class Line:
        def __init__(self, part, pr, rbase, sp, rp_, sl, rl):
            self.part, self.pr, self.rbase, self.sp, self.rp, self.sl, self.rl = part, pr, rbase, sp, rp_, sl, rl

        def pair(self, k):
            return remote(
                pool.at[self.part + nt + k], pool.at[self.pr + k], self.sp.at[k], self.rp.at[k], place.pair()
            )

        def copy(self, side, k, f, dev):
            slot = k if side == 0 else jnp.where(k == t - 1, nt, k)
            return remote(
                pool.at[self.part + k, at256(f), :],
                pool.at[self.rbase + slot, at256(f), :],
                self.sl.at[side, k, f],
                self.rl.at[slot, f],
                dev,
            )

        def got(self, slot, f):
            remote(
                pool.at[self.part, at256(f), :],
                pool.at[self.rbase + slot, at256(f), :],
                self.sl.at[0, 0, f],
                self.rl.at[slot, f],
                place.pair(),
            ).wait_recv()

        def each(self, side, step, do, which="all"):
            me = t if side == 0 else nt - 1 - t
            here = {"all": me <= step, "end": me == 0, "far": (me > 1) & (me <= step), "near": me == 1}[which]

            @pl.when(here & (me < nt - 1))
            def _():
                k = nt - 1 - step + me
                do(k if side == 0 else nt - 1 - k)

        def send(self, step, which):
            for side in range(2):

                def do(k, side=side):
                    for f in range(2):
                        if which != "end":
                            self.got(k, f)

                        @pl.loop(0, TW // 64)
                        def _(q):
                            rows = pl.ds(pl.multiple_of(f * TW + q * 64, 64), 64)
                            v = pool[self.part + k, rows, :].astype(F32) + pool[self.pr + k, rows, :].astype(F32)
                            if which != "end":
                                v = v + pool[self.rbase + k, rows, :].astype(F32)
                            pool[self.part + k, rows, :] = v.astype(BF16)

                        self.copy(side, k, f, z_dev(side)).start()

                self.each(side, step, do, which)

        def sent(self):
            for side in range(2):
                for step in range(nt - 1):
                    for f in range(2):
                        self.each(
                            side, step, lambda k, side=side, f=f: self.copy(side, k, f, place.pair()).wait_send()
                        )

        def finish(self, halves=(0, 1)):
            for f in halves:
                pl.when(t > 0)(lambda: self.got(t, f))
                pl.when(t < nt - 1)(lambda: self.got(nt, f))

        def value(self, rows):
            v = pool[self.part + t, rows, :].astype(F32) + pool[self.pr + t, rows, :].astype(F32)
            v = v + jnp.where(t > 0, pool[self.rbase + t, rows, :].astype(F32), 0.0)
            return v + jnp.where(t < nt - 1, pool[self.rbase + nt, rows, :].astype(F32), 0.0)

    line_o = Line(pn.hb, pn.w1b, pn.w1b + nt, s_oc, r_oc, s_ol, r_ol)
    line_h = Line(pn.hb, pn.w2b, pn.w2b + nt, s_hc, r_hc, s_hl, r_hl)
    def out_rows(s):
        @pl.loop(0, nt)
        def _(k):
            rhs = cat([wd_v[:, at512(k)]] + [pool[pn.w2b + u * nt + k] for u in range(nu)], 0)
            pool[pn.hb + s * nt + k] = mm(cat([attn[s], act[s]], 1), rhs).astype(BF16)

    out_rows(1)
    told(0)
    for k in range(nt):
        line_o.pair(k).start()

    for s in range(2):
        attn_copy(s).wait()
    for core in range(2):
        for s in range(2):
            mine = attn if core == 0 else attn_p
            v = jnp.where(live(s), mine[s], jnp.zeros((BK, hw), BF16))
            at_tmp[...] = v.T
            who = c if core == 0 else 1 - c
            for j in range(nch // 2):
                off = lax.rem((2 * j + c) * rd, hw)
                dst = (who * (nch // 2) + j) * rd
                dl[pl.ds(pl.multiple_of(dst, rd), rd), pl.ds(s * BK, BK)] = at_tmp[
                    pl.ds(pl.multiple_of(off, rd), rd), :
                ]

    def dense_chunk(i):
        k = chunk(i)
        out = mm(dl[...], cat([pool[pn.cb + k], pool[pn.cb + nt + k]], 0))
        dg[:, pl.ds(i * BK, BK)] = out.astype(BF16)
        den_p[i].start(0)

    for i in range(nt - 1):
        dense_chunk(i)
    out_rows(0)
    upto(needed[3])
    mid(fc2_p[2])
    for k in range(nt):
        line_o.pair(k).wait()
    @pl.loop(0, nt - 1)
    def _(step):
        line_o.send(step, "end")

    fc2_chunk(3)
    dense_chunk(3)

    def dpre_block(u):
        @pl.loop(0, 2)
        def _(s):
            v = mm(
                cat([pool[pn.cb + s * nt + k] for k in range(nt)], 1),
                cat([pool[pn.w2b + u * nt + k] for k in range(nt)], 1),
                1,
                1,
            )
            for h in range(2):
                q = 2 * u + h
                w = v[:, h * TW : (h + 1) * TW]
                w = jnp.where(live(s), w * gelu_slope(biased(s, q)), 0.0)
                buf[pl.ds(pl.multiple_of(s * BK, BK), BK), pl.ds(q * TW, TW)] = w.astype(BF16)
                fb[pl.ds(0, 1), pl.ds(q * TW, TW)] += jnp.sum(w, axis=0, keepdims=True)

    def fc1_block(u):
        @pl.loop(0, nt)
        def _(k):
            out = mm(cat([pool[pn.xb + k], pool[pn.xb + nt + k]], 1), buf[:, pl.ds(u * BK, BK)])
            pool[pn.f1b + nu * k + u] = out.astype(BF16)

        for q in (2 * u, 2 * u + 1):
            for p in fc1_p[q]:
                p.start(0)

    dpre_block(0)
    fc1_block(0)
    dpre_block(1)
    tell(1)
    fc1_block(1)
    line_o.send(1, "near")
    mid(fc2_p[3])
    mid(den_p)

    def dcols(i):
        return pl.ds(i * hw, hw)

    @pl.loop(0, 2)
    def _(s):
        v = mm(cat([pool[pn.cb + s * nt + k] for k in range(nt)], 1), wd_v[...], 1, 1)
        v = jnp.where(live(s), v, 0.0)
        act[s, :, dcols(3)] = v.astype(BF16)

    ob[...] = jnp.broadcast_to(
        jnp.sum(jnp.where(live(0), pool[pn.cb + t].astype(F32), 0.0), axis=0, keepdims=True), ob.shape
    )
    z_sent(1)
    begin("w1r")
    fin2(0)
    fin2(1)
    @pl.loop(0, 2 * npair)
    def _(i):
        pl.when(i == npair)(lambda: line_o.send(2, "far"))
        s, hp = i // npair, lax.rem(i, npair)
        cols = pl.ds(pl.multiple_of(hp * LANES, LANES), LANES)
        dq, dk, dv = [], [None, None], [None, None]
        for qt in range(2):
            rows, kr, nk = pl.ds(qt * TW, TW), pl.ds(0, (qt + 1) * TW), (qt + 1) * TW
            bias = bias_of(s, qt)
            da = act[s, rows, pl.ds(pl.multiple_of(3 * hw + hp * LANES, LANES), LANES)]
            prod = da.astype(F32) * attn[s, rows, cols].astype(F32)
            qs, ks, vs = qkv[0, s, rows, cols], qkv[1, s, kr, cols], qkv[2, s, kr, cols]
            got = []
            for h in range(2):
                pf = probs(only(qs, h), ks, bias)
                pb = pf.astype(BF16)
                delta = jnp.sum(only(prod, h), axis=1, keepdims=True)
                dp = mm(only(da, h), vs, 1, 1)
                ds = (pf * (dp - delta) * score_scale).astype(BF16)
                got.append((mm(ds, ks), mm(ds, qs, 0, 0), mm(pb, da, 0, 0)))
            pick = [jnp.where(heads2[0], a, b) for a, b in zip(*got)]
            dq.append(pick[0])
            for lst, v in ((dk, pick[1]), (dv, pick[2])):
                lst[0] = v[:TW] if lst[0] is None else lst[0] + v[:TW]
                if qt:
                    lst[1] = v[TW:]
        low1 = lax.rem(lane1, ROT) < ROT // 2
        for i3, parts in enumerate((dq, dk, dv)):
            for qt in range(2):
                rows = pl.ds(qt * TW, TW)
                v = parts[qt]
                if i3 < 2:
                    sw = jnp.where(
                        low1, pltpu.roll(v, LANES - ROT // 2, 1), pltpu.roll(v, ROT // 2, 1)
                    )
                    v = v * tab[s, rows, pl.ds(0, LANES)] - sw * tab[s, rows, pl.ds(LANES, LANES)]
                bias3[i3, pl.ds(0, 1), cols] += jnp.sum(v, axis=0, keepdims=True)
                act[s, rows, pl.ds(pl.multiple_of(i3 * hw + hp * LANES, LANES), LANES)] = v.astype(BF16)

    line_o.send(2, "near")
    mid(fc1_p[0])
    mid(fc1_p[1])

    def dh_chunk(s, k):
        rhs = cat([wq_v[i, at512(k), :] for i in range(3)] + [pool[pn.cb + u * nt + k] for u in range(nu)], 1)
        lhs = cat([act[s, :, pl.ds(0, 3 * hw)], buf[pl.ds(s * BK, BK), :]], 1)
        pool[pn.hb + s * nt + k] = mm(lhs, rhs, 1, 1).astype(BF16)

    def step_of(tt, k):
        if k == tt:
            return nt
        return nt - 1 - k + tt if k > tt else k + nt - 1 - tt

    far = [sorted(range(nt), key=lambda k, tt=tt: (step_of(tt, k), k)) for tt in range(nt)]

    def far_chunk(i):
        k = 0
        for tt in range(nt):
            for n in range(nt):
                k = jnp.where((t == tt) & (i == n), far[tt][n], k)
        return k

    def qkv_blocks():
        @pl.loop(0, nt)
        def _(k):
            out = mm(
                cat([pool[pn.xb + k], pool[pn.xb + nt + k]], 1),
                cat([act[0, :, pl.ds(0, 3 * hw)], act[1, :, pl.ds(0, 3 * hw)]], 0),
            ).astype(BF16)
            pool[pn.f2b + k] = out[:, :BK]
            pool[pn.f2b + nt + k // 2, :, at256(lax.rem(k, 2))] = out[:, BK:]

        for i in range(3):
            for p in qkv_p[i]:
                p.start(0)

    told(1)
    arrive("w1r")
    @pl.loop(0, nt)
    def _(i):
        k = far_chunk(i)
        dh_chunk(1, k)
        line_h.pair(k).start()

    arrive("xo")
    line_o.finish()

    @pl.loop(0, BK // 64)
    def _(q):
        rows = pl.ds(pl.multiple_of(q * 64, 64), 64)
        ocol = pl.ds(pl.multiple_of(t * BK, BK), BK)
        v = pool[pn.xo, rows, :].astype(F32) + line_o.value(rows)
        v = v + (obias[pl.ds(0, 1), ocol] + obias[pl.ds(1, 1), ocol])
        pool[pn.w1b + t, rows, :] = v.astype(BF16)

    def out_copy():
        return pltpu.make_async_copy(pool.at[pn.w1b + t], block_out, s_load.at[2])

    out_copy().start()

    line_o.sent()
    @pl.loop(0, nt)
    def _(i):
        k = far_chunk(i)
        dh_chunk(0, k)
        line_h.pair(k).wait()
        pl.when(i < nt - 1)(lambda: line_h.send(i, "end"))

    fin2(2)
    fin2(3)
    for b in range(pn.bits):
        pl.semaphore_signal(credit.at[6 + b], inc=1, device_id=place.over(b), device_id_type=MESH)
    mid(fc1_p[2])
    for b in range(pn.bits):
        pl.semaphore_wait(credit.at[6 + b], 1)
    qkv_blocks()
    mid(fc1_p[3])
    line_h.send(1, "near")
    fin1(0)
    mid(qkv_p[0])
    line_h.send(2, "far")
    mid(qkv_p[1])
    line_h.send(2, "near")
    mid(qkv_p[2])
    fin1(1)
    fin1(2)

    gcol = pl.ds(pl.multiple_of(t * BK, BK), BK)

    def tail(rows):
        dh = line_h.value(rows)
        normed = (pool[pn.xo, rows, :].astype(F32) - mi[0, rows, pl.ds(0, 1)]) * mi[0, rows, pl.ds(1, 1)]
        return dh, normed, dh * gain[:, gcol]

    def s_copy(k, f):
        src = stt.at[:, pl.ds(f * TW, TW)]
        return remote(src, sr.at[t, :, pl.ds(f * TW, TW)], s_s.at[k, f], r_s.at[t, f], (d, lax.rem(t + k, nt)))

    def tail_one(f):
        line_h.finish((f,))

        @pl.loop(0, TW // 64)
        def _(q):
            rows = pl.ds(pl.multiple_of(f * TW + q * 64, 64), 64)
            dh, normed, scaled = tail(rows)
            s1 = jnp.sum(scaled, axis=1, keepdims=True)
            s2 = jnp.sum(scaled * normed, axis=1, keepdims=True)
            stc[rows, :] = jnp.where(first, s1, s2)
            ng[pl.ds(0, 1), :] += jnp.sum(dh * normed, axis=0, keepdims=True)
            ng[pl.ds(1, 1), :] += jnp.sum(dh, axis=0, keepdims=True)

        half = pl.ds(f * TW, TW)
        stt[:, half] = stc[half, :].T[:8]
        sr[t, :, half] = stt[:, half]
        for k in range(1, nt):
            s_copy(k, f).start()

    def tail_two(f):
        half = pl.ds(f * TW, TW)
        for k in range(1, nt):
            s_copy(k, f).wait_send()
            frm = lax.rem(t + k, nt)
            remote(
                stt.at[:, half], sr.at[frm, :, half], s_s.at[k, f], r_s.at[frm, f], place.pair()
            ).wait_recv()
        tot = sr[0, :, half]
        for k in range(1, nt):
            tot = tot + sr[k, :, half]
        stc[half, :] = jnp.concatenate([tot / pn.width, jnp.zeros((LANES - 8, TW), F32)], axis=0).T

        for h in range(2):

            def put(ref, h=h):
                @pl.loop(0, TW // 64)
                def _(q):
                    rows = pl.ds(pl.multiple_of(f * TW + q * 64, 64), 64)
                    part = slice(h * TW, (h + 1) * TW)
                    _, normed, scaled = (v[:, part] for v in tail(rows))
                    v = scaled - stc[rows, pl.ds(0, 1)] - normed * stc[rows, pl.ds(1, 1)]
                    keep = tab[0, rows, pl.ds(2 * LANES, 1)] >= 0.0
                    own = pool[pn.co, rows, pl.ds(h * TW, TW)].astype(F32)
                    ref[pl.ds(pl.multiple_of(q * 64, 64), 64), :] = v * mi[0, rows, pl.ds(1, 1)] + jnp.where(
                        keep, own, 0.0
                    )

            stage_out(put, input_grad.at[pl.ds(f * TW, TW), pl.ds(h * TW, TW)])

    def pass_on(slot):
        return pltpu.make_async_copy(fr.at[slot], other_out.at[slot], s_f.at[2, slot])

    def pass_all(lo, hi):
        for slot in range(lo, hi):
            send_pair(slot).wait()
            pass_on(slot).start()

    tail_one(0)
    tail_one(1)

    def v_copy(k):
        peer = lax.rem(d + k, nd)
        return remote(sv.at[peer], rv.at[d], s_v.at[k], r_v.at[d], (peer, t))

    cw, hwd = BK // nd, 2 * hw // nd
    sv[...] = jnp.zeros_like(sv)
    for dd in range(nd):
        mine = c == dd % 2
        sv[dd, pl.ds(0, 1), pl.ds(0, ub)] = jnp.where(mine, fb[pl.ds(0, 1), pl.ds((dd // 2) * ub, ub)], 0.0)
        sv[dd, pl.ds(1, 2), pl.ds(0, cw)] = ng[pl.ds(0, 2), pl.ds(dd * cw, cw)]
        sv[dd, pl.ds(3, 1), pl.ds(0, cw)] = ob[pl.ds(0, 1), pl.ds(dd * cw, cw)]
        here = c == (dd * hwd) // hw
        src = pl.ds((dd * hwd) % hw, hwd)
        sv[dd, pl.ds(4, 1), pl.ds(0, hwd)] = jnp.where(here, bias3[0, pl.ds(0, 1), src], 0.0)
        sv[dd, pl.ds(5, 1), pl.ds(0, hwd)] = jnp.where(here, bias3[2, pl.ds(0, 1), src], 0.0)
        for core in range(2):
            sv[dd, pl.ds(6 + core, 1), :] = jnp.where(c == core, bias3[1, pl.ds(0, 1), :], 0.0)
    for k in range(1, nd):
        v_copy(k).start()
    rv[d] = sv[d]
    fin1(3)
    fin_d()
    pass_all(0, nq)
    fin3(0)
    fin3(1)
    tail_two(0)
    fin3(2)
    tail_two(1)
    pass_all(nq, nq + 3)
    line_h.sent()
    for k in range(1, nd):
        v_copy(k).wait_send()
        frm = lax.rem(d + k, nd)
        remote(sv.at[0], rv.at[frm], s_v.at[k], r_v.at[frm], place.pair()).wait_recv()
    res = rv[0]
    for k in range(1, nd):
        res = res + rv[k]
    fc1b_out[...] = res[0:1, :ub]
    norm_out[...] = res[1:3, :cw]
    outb_out[...] = jnp.concatenate([res[3:4, :cw], res[3:4, :cw]], axis=0)
    qvb_out[...] = res[4:6, :hwd]
    rk = ROT // nd
    turned = pltpu.roll(res, lax.rem(TW - d * rk, TW), 1)
    for core in range(2):
        for h in range(pn.heads):
            stc[pl.ds(core * pn.heads + h, 1), pl.ds(0, rk)] = turned[6 + core : 7 + core, h * HD : h * HD + rk]
    keyb_out[...] = stc[pl.ds(0, LANES), :].T[:rk, : 2 * pn.heads]
    for slot in range(nq + 3):
        pass_on(slot).wait()
    out_copy().wait()
    for cp in os_used[-ostage.shape[0] :]:
        cp.wait()

def results_kernel(nq, direct, *refs):
    n = len(refs) // 3 - 1
    src, dst, hold = refs[: n + 1], refs[n + 1 : 2 * n + 1], refs[2 * n + 1 : 3 * n + 2]
    wide, sem, sem_w = refs[3 * n + 2 :]
    c = lax.rem(lax.axis_index("dp"), 2)
    order = sorted(range(n + 1), key=lambda i: -math.prod(src[i].shape))
    order = [n] + [i for i in order if i != n]

    def get(i):
        return pltpu.make_async_copy(src[i], hold[i], sem.at[0, i])

    def parts(i):
        if i not in (3, 7):
            return [(hold[i], dst[i])]
        m = 3 if i == 3 else nq
        out = []
        for k in range(m):
            if i == 3:
                own, at = hold[3].at[k], lambda core, k=k: dst[3].at[k, :, at256(core)]
            else:
                own = hold[7].at[:, pl.ds(k * TW, TW)]
                at = lambda core, k=k: dst[7].at[:, at256(2 * k + core if direct else core * nq + k)]
            out += [(own, at(c)), (wide.at[nq + k if i == 3 else k], at(1 - c))]
        return out

    count = [0]

    def put(i):
        for a, b in parts(i):
            cp = pltpu.make_async_copy(a, b, sem_w.at[count[0]])
            count[0] += 1
            cp.start()
            sent.append(cp)

    sent = []
    for i in order:
        get(i).start()
    for i in order:
        get(i).wait()
        if i == n:
            wide[...] = hold[n][...].astype(F32)
        else:
            put(i)
    for cp in sent:
        cp.wait()


def results(arrays, nq, direct, shapes):
    n = len(shapes)
    anyw = pl.BlockSpec(memory_space=pl.ANY)
    return pl.pallas_call(
        functools.partial(results_kernel, nq, direct),
        out_shape=[jax.ShapeDtypeStruct(s, a.dtype) for s, a in zip(shapes, arrays)],
        in_specs=[anyw] * (n + 1),
        out_specs=[anyw] * n,
        scratch_shapes=[pltpu.VMEM(a.shape, a.dtype) for a in arrays]
        + [
            pltpu.VMEM(arrays[n].shape, F32),
            pltpu.SemaphoreType.DMA((1, n + 1)),
            pltpu.SemaphoreType.DMA((n - 2 + 2 * (nq + 3),)),
        ],
        compiler_params=pltpu.CompilerParams(vmem_limit_bytes=VMEM_BYTES),
        name="results",
    )(*arrays)


def per_device(
    hidden_in,
    cotangent,
    segment_ids,
    positions,
    norm_gain,
    norm_shift,
    qkv_weight,
    qv_bias,
    key_bias,
    dense_weight,
    fc1_weight,
    fc1_bias,
    fc2_weight,
    out_bias,
):
    nd, nt = lax.axis_size("dp"), lax.axis_size("tensor")
    c = lax.rem(lax.axis_index("dp"), 2)
    nch = nd // 2
    rows, wl = hidden_in.shape
    width = wl * nt
    heads = key_bias.shape[0] // 2
    units = fc1_weight.shape[1] // 2
    ub = units // nch
    pn = Plan(nd, nt, units, heads, ub)
    hw, rb, rd, nq = pn.hw, pn.rb, pn.rd, units // TW
    assert rows == BK and wl == BK and nt == 4 and nq == 4 and hw == TW and rb == ub
    direct = ub == TW

    freq = 10000.0 ** (-(np.arange(LANES) % (ROT // 2)) * (2.0 / ROT))
    freq = jnp.asarray(freq.astype(np.float32)[None, :])

    def pick(w, axis):
        shape = w.shape
        w = w.reshape(*shape[:axis], nch, 2, ub, *shape[axis + 1 :])
        w = lax.dynamic_index_in_dim(w, c, axis + 1, keepdims=False)
        return w.reshape(*shape[:axis], units, *shape[axis + 1 :])

    w1, w2, b1 = fc1_weight, fc2_weight, fc1_bias
    if not direct:
        w1, w2, b1 = pick(w1, 1), pick(w2, 0), pick(b1, 0)
    w1 = w1.reshape(nt, BK, w1.shape[1])
    wq = qkv_weight.transpose(1, 0, 2)
    b1 = b1.reshape(1, -1)

    vm = pl.BlockSpec(memory_space=pltpu.VMEM)
    anyw = pl.BlockSpec(memory_space=pl.ANY)
    shapes = [
        ((rows, wl), BF16, anyw),
        ((rows, wl), F32, anyw),
        ((2, wl // nd), F32, vm),
        ((3, rb, hw), F32, anyw),
        ((2, 2 * hw // nd), F32, vm),
        ((ROT // nd, 2 * heads), F32, vm),
        ((rd, width), F32, anyw),
        ((rb, units), F32, anyw),
        ((1, ub), F32, vm),
        ((ub, width), F32, anyw),
        ((2, wl // nd), F32, vm),
        ((nq + 3, rb, TW), BF16, anyw),
    ]
    dma = pltpu.SemaphoreType.DMA
    nos = 4
    scratch = [
        pltpu.VMEM((pn.blocks, BK, BK), BF16),
        pltpu.VMEM((3, width, hw), BF16),
        pltpu.VMEM((hw, width), BF16),
        pltpu.VMEM((2, rows, 3 * LANES), F32),
        pltpu.VMEM((2, 8, rows), F32),
        pltpu.VMEM((2, rows, units), BF16),
        pltpu.VMEM((units, 2 * rows), BF16),
        pltpu.VMEM((2, rows, units), F32),
        pltpu.VMEM((3, 2, rows, hw), BF16),
        pltpu.VMEM((2, rows, hw), BF16),
        pltpu.VMEM((2, rows, hw), BF16),
        pltpu.VMEM((nch * rd, 2 * rows), BF16),
        pltpu.VMEM((hw, rows), BF16),
        pltpu.VMEM((nch * rd, width), BF16),
        pltpu.VMEM((nt, nch - 1, rd, BK), BF16),
        pltpu.VMEM((pn.n2 + pn.n1, nch - 1, rb, TW), BF16),
        pltpu.VMEM((nq + 3, rb, TW), BF16),
        pltpu.VMEM((nq + 3, rb, TW), BF16),
        pltpu.VMEM((nos, TW, TW), F32),
        pltpu.VMEM((2, rows, LANES), F32),
        pltpu.VMEM((3, 8, hw), F32),
        pltpu.VMEM((8, units), F32),
        pltpu.VMEM((8, wl), F32),
        pltpu.VMEM((8, wl), F32),
        pltpu.VMEM((nd, 8, TW), F32),
        pltpu.VMEM((nd, 8, TW), F32),
        pltpu.VMEM((rows, LANES), F32),
        pltpu.VMEM((8, rows), F32),
        pltpu.VMEM((nt, 8, rows), F32),
        pltpu.VMEM((2, nt, 8, LANES), F32),
        pltpu.VMEM((8, hw), F32),
        pltpu.VMEM((8, LANES), F32),
        dma((10 + nq * (2 + nt),)),
        dma((2, 2, nt, 2)),
        dma((2, nt, 2)),
        dma((2, nt, 2)),
        dma((2, nt, 2)),
        dma((4,)),
        dma((pn.pieces, nch - 1)),
        dma((pn.pieces, nch - 1)),
        dma((2,)),
        dma((2,)),
        dma((3, nq + 3)),
        dma((nos,)),
        dma((2, 2)),
        dma((nt,)),
        dma((nt,)),
        dma((2, nt, 2)),
        dma((nt + 1, 2)),
        dma((nt,)),
        dma((nt,)),
        dma((2, nt, 2)),
        dma((nt + 1, 2)),
        dma((nd,)),
        dma((nd,)),
        dma((nt, 2)),
        dma((nt, 2)),
        dma((2, nt)),
        dma((2, nt)),
        pltpu.SemaphoreType.REGULAR((6 + pn.bits,)),
    ]
    res = pl.pallas_call(
        functools.partial(block_kernel, pn, direct),
        out_shape=[jax.ShapeDtypeStruct(s, dt) for s, dt, _ in shapes],
        in_specs=[anyw, anyw, vm, vm, vm, vm, vm, anyw, anyw, anyw, anyw, vm, vm, vm, vm],
        out_specs=[sp for _, _, sp in shapes],
        scratch_shapes=scratch,
        compiler_params=pltpu.CompilerParams(
            collective_id=0, has_side_effects=True, vmem_limit_bytes=VMEM_BYTES
        ),
        name="block",
    )(
        hidden_in, cotangent, segment_ids.reshape(1, rows), positions.reshape(1, rows), freq, norm_gain.reshape(1, width), norm_shift.reshape(1, width),
        w1, w2, wq, dense_weight, b1, qv_bias, key_bias, out_bias,
    )
    whole = [s for s, _, _ in shapes[:-1]]
    whole[3], whole[7] = (3, rb, 2 * hw), (rb, 2 * units)
    res = list(results(res, nq, direct, whole))
    res[3] = res[3].transpose(1, 0, 2)
    res[5] = res[5].T
    if not direct:
        res[7] = res[7].reshape(rb, 2, nch, ub).transpose(0, 2, 1, 3).reshape(rb, 2 * units)
    res[8] = res[8].reshape(ub)
    return tuple(res)


def solution(mesh):
    placed = (
        P("dp", "tensor"),
        P("dp", "tensor"),
        P("dp"),
        P("dp"),
        P(),
        P(),
        P(None, None, "tensor"),
        P(None, "tensor"),
        P("tensor", None),
        P("tensor", None),
        P(None, "tensor"),
        P("tensor"),
        P("tensor", None),
        P(),
    )
    return jax.shard_map(
        per_device,
        mesh=mesh,
        in_specs=placed,
        out_specs=(
            P("dp", "tensor"),
            P("dp", "tensor"),
            P(None, ("tensor", "dp")),
            P("dp", None, "tensor"),
            P(None, ("tensor", "dp")),
            P("tensor", "dp"),
            P(("tensor", "dp"), None),
            P("dp", "tensor"),
            P(("tensor", "dp")),
            P(("tensor", "dp"), None),
            P(None, ("tensor", "dp")),
        ),
        check_vma=False,
    )
```
